256 devices in a mesh: lat: 4 (over y), lon: 64 (over x, z, core).
Axes of the slice: x: 4, y: 4, z: 8, core: 2. Of those that a mesh axis runs over, the one named last changes fastest.
Arguments:
- right_side: float32 [512, 8192], P('lat', 'lon'), may hold values from -8 to 8
- surface_term: float32 [512, 8192], P('lat', 'lon'), may hold values from 0.0002 to 0.002
- east_coupling: float32 [512, 8192], P('lat', 'lon'), may hold values from 0.3 to 3
- north_coupling: float32 [512, 8192], P('lat', 'lon'), may hold values from 0.3 to 3
- neast_coupling: float32 [512, 8192], P('lat', 'lon'), may hold values from 0.1 to 0.5
- nwest_coupling: float32 [512, 8192], P('lat', 'lon'), may hold values from 0.1 to 0.5
- land_sea: int32 [512, 8192], P('lat', 'lon'), may hold values from 0 to 1, as said below
- fold_map: int32 [8192], P('lon'), may hold values from 0 to 8191, as said below
Outputs:
- solution: float32 [512, 8192], P('lat', 'lon')
- residual: float32 [512, 8192], P('lat', 'lon')
The draws below stay inside these ranges and needn't reach their ends.
Inputs may be any that keep to these rules, and one draw needn't show every extreme that they name: fold_map[j] = (c - j) mod 8192 for one odd c: an involution of the columns with no fixed point. land_sea is 0 or 1; land lies in bands of 8 columns, each over one range of rows.
All inputs are finite; a program needn't handle non-finite values.
Results may differ from the reference program's by a relative error of at most 0.0015.
Values sent between devices are 32-bit elements.
No kernel may reach another device: no remote copies, remote signals or barrier semaphores. Data moves between devices by JAX's collectives and lax.ppermute only.
A program may use at most 64 MiB of HBM per device.

```python
import math
import jax
import jax.numpy as jnp
from jax import lax

ITERS = 8
NLAT = 512
NLON = 8192


def draw_right_side(key, part):
    noise_key, scale_key = jax.random.split(jax.random.fold_in(key, 11))
    row_block = jnp.arange(NLAT) // 150
    col_block = jnp.arange(NLON) // 64
    block_scales = jnp.exp(jax.random.uniform(scale_key, (NLAT // 150 + 1, NLON // 64 + 1), jnp.float32, math.log(0.1), math.log(3.0)))
    cell_scale = block_scales[row_block[:, None], col_block[None, :]]
    noise_values = jax.random.normal(noise_key, (NLAT, NLON), jnp.float32)
    return jnp.clip(noise_values * cell_scale, -8.0, 8.0)


def draw_land_sea(key, part):
    first_key, second_key, third_key = jax.random.split(jax.random.fold_in(key, 37), 3)
    band_count = NLON // 8
    continent = (jax.random.randint(first_key, (band_count,), 0, 3, jnp.int32) == 0) | (jnp.arange(band_count) == 0)
    start_row = jax.random.randint(second_key, (band_count,), 0, NLAT // 2, jnp.int32)
    extent = jax.random.randint(third_key, (band_count,), NLAT // 8 + 1, NLAT // 2 + 1, jnp.int32)
    band_of = jnp.arange(NLON, dtype=jnp.int32) // 8
    rows = jnp.arange(NLAT, dtype=jnp.int32)[:, None]
    land = continent[band_of][None, :] & (rows >= start_row[band_of][None, :]) & (rows < (start_row + extent)[band_of][None, :])
    return jnp.where(land, 0, 1).astype(jnp.int32)


def draw_fold_map(key, part):
    offset = 2 * jax.random.randint(jax.random.fold_in(key, 23), (), 0, NLON // 2, jnp.int32) + 1
    return (offset - jnp.arange(NLON, dtype=jnp.int32)) % NLON


def levels(rng, shape, cuts, low, top_value):
    factor_of = 1.0
    for dim, parts in cuts:
        draws = jax.random.uniform(jax.random.fold_in(jax.random.fold_in(rng, 6), dim), (parts,), jnp.float32, low / len(cuts), top_value / len(cuts))
        factor_of = factor_of * jnp.repeat(jnp.exp(draws), shape[dim] // parts).reshape((-1,) + (1,) * (len(shape) - 1 - dim))
    return factor_of


def setup_inputs(seed: int = 0) -> dict:
    keys = jax.random.split(jax.random.key(seed), 9)
    return {
        "right_side": draw_right_side(jax.random.fold_in(keys[8], 71), 0),
        "surface_term": jnp.clip(jnp.exp(math.log(0.002) - 2.3025852 * jax.random.uniform(keys[1], (NLAT, NLON), jnp.float32) ** levels(keys[1], (NLAT, NLON), ((0, 4), (1, 64)), -0.2, 0.2)), 0.0002, 0.002),
        "east_coupling": jnp.clip(jnp.exp(math.log(3.0) - 2.3025851 * jax.random.uniform(keys[2], (NLAT, NLON), jnp.float32) ** levels(keys[2], (NLAT, NLON), ((0, 4), (1, 64)), -0.2, 0.2)), 0.3, 3.0),
        "north_coupling": jnp.clip(jnp.exp(math.log(3.0) - 2.3025851 * jax.random.uniform(keys[3], (NLAT, NLON), jnp.float32) ** levels(keys[3], (NLAT, NLON), ((0, 4), (1, 64)), -0.2, 0.2)), 0.3, 3.0),
        "neast_coupling": jnp.clip(jnp.exp(math.log(0.5) - 1.609438 * jax.random.uniform(keys[4], (NLAT, NLON), jnp.float32) ** levels(keys[4], (NLAT, NLON), ((0, 4), (1, 64)), -0.2, 0.2)), 0.1, 0.5),
        "nwest_coupling": jnp.clip(jnp.exp(math.log(0.5) - 1.609438 * jax.random.uniform(keys[5], (NLAT, NLON), jnp.float32) ** levels(keys[5], (NLAT, NLON), ((0, 4), (1, 64)), -0.2, 0.2)), 0.1, 0.5),
        "land_sea": draw_land_sea(jax.random.fold_in(keys[8], 71), 0),
        "fold_map": draw_fold_map(jax.random.fold_in(keys[8], 71), 0),
    }


OFFSETS = ((0, 1), (0, -1), (1, 0), (-1, 0), (1, 1), (-1, -1), (1, -1), (-1, 1))
COUPLINGS = ((1, 0, 0), (1, 0, -1), (2, 0, 0), (2, -1, 0), (3, 0, 0), (3, -1, -1), (4, 0, 0), (4, -1, 1))

def interior(padded, row_step, col_step):
    row_count = padded.shape[-2] - 2
    col_count = padded.shape[-1] - 2
    return padded[..., 1 + row_step:1 + row_step + row_count, 1 + col_step:1 + col_step + col_count]

def stencil_weights(padded):
    ocean_pad = padded[0]
    centre = interior(ocean_pad, 0, 0)
    weight_list = []
    open_sum = jnp.zeros_like(centre)
    for (layer_index, row_step, col_step), (row_off, col_off) in zip(COUPLINGS, OFFSETS):
        edge_value = interior(padded[layer_index], row_step, col_step)
        weight_list.append(edge_value * centre * interior(ocean_pad, row_off, col_off))
        open_sum = open_sum + edge_value
    return (jnp.stack(weight_list), open_sum)

def neighbour_sum(weights, padded_field):
    accumulated = jnp.zeros_like(weights[0])
    for position, (row_off, col_off) in enumerate(OFFSETS):
        accumulated = accumulated + weights[position] * interior(padded_field, row_off, col_off)
    return accumulated

def pad_grid(values):
    wrapped = jnp.concatenate([values[..., -1:], values, values[..., :1]], axis=-1)
    zero_row = jnp.zeros_like(wrapped[..., :1, :])
    return jnp.concatenate([zero_row, wrapped, zero_row], axis=-2)

def line_solve(lower_band, middle_band, upper_band, values):
    solved = lax.linalg.tridiagonal_solve(lower_band.T, middle_band.T, upper_band.T, values.T[:, :, None])
    return solved[:, :, 0].T

def reference(right_side, surface_term, east_coupling, north_coupling, neast_coupling, nwest_coupling, land_sea, fold_map):
    ocean = land_sea.astype(jnp.float32)
    row_ids = lax.broadcasted_iota(jnp.int32, ocean.shape, 0)
    top_row = jnp.where(row_ids == ocean.shape[0] - 1, 1.0, 0.0).astype(jnp.float32)
    open_rows = 1.0 - top_row
    stacked = jnp.stack([ocean, east_coupling, north_coupling * open_rows, neast_coupling * open_rows, nwest_coupling * open_rows])
    weights, open_sum = stencil_weights(pad_grid(stacked))
    top_north = north_coupling[-1]
    fold_open = 0.5 * (top_north + jnp.take(top_north, fold_map))
    fold_weight = fold_open * ocean[-1] * jnp.take(ocean[-1], fold_map)
    diagonal = ocean * (surface_term + open_sum + top_row * fold_open[None]) + (1.0 - ocean)
    line_diagonal = ocean * (surface_term + weights[2] + weights[3]) + (1.0 - ocean)
    lower_band = -weights[3]
    upper_band = -weights[2]

    def operate(field):
        fold_term = fold_weight * jnp.take(field[-1], fold_map)
        return diagonal * field - neighbour_sum(weights, pad_grid(field)) - top_row * fold_term[None]
    residual = ocean * right_side
    solution = jnp.zeros_like(residual)
    precond = line_solve(lower_band, line_diagonal, upper_band, residual)
    direction = precond
    product_now = jnp.sum(residual * precond)
    for iteration in range(ITERS):
        image_field = operate(direction)
        step_length = product_now / jnp.sum(direction * image_field)
        solution = solution + step_length * direction
        residual = residual - step_length * image_field
        if iteration + 1 < ITERS:
            precond = line_solve(lower_band, line_diagonal, upper_band, residual)
            product_next = jnp.sum(residual * precond)
            direction = precond + product_next / product_now * direction
            product_now = product_next
    return (solution, residual)
```

```python
import functools

import jax
import jax.numpy as jnp
from jax import lax
from jax.experimental import pallas as pl
from jax.experimental.pallas import tpu as pltpu
from jax.sharding import Mesh
from jax.sharding import PartitionSpec as P

LON = ("x", "z", "core")
NLON = 8192
COLS = 128
OWN = 32
GHOST = 8
WIDE = OWN + 2 * GHOST
PAD = COLS + 2 * GHOST
STEPS = 64
HALF = 4
TOTAL = 2 * HALF
SCALE = 1.0e-4
F32 = jnp.float32
HIGHEST = lax.Precision.HIGHEST
E, W, N, S, NE, SW, NW, SE, DIAG = range(9)
MULT, IPIV, LOWER, UPPER = range(4)


def params():
    return pltpu.CompilerParams(vmem_limit_bytes=48 * 1024 * 1024)


def two_sum(a, b):
    s = a + b
    bb = s - a
    return s, (a - (s - bb)) + (b - bb)


def split(a):
    t = a * 4097.0
    hi = t - (t - a)
    return hi, a - hi


def two_prod(a, b):
    p = a * b
    ah, al = split(a)
    bh, bl = split(b)
    return p, ((ah * bh - p) + ah * bl + al * bh) + al * bl


def renorm(s, e):
    hi = s + e
    return hi, e - (hi - s)


def pair_sub(a, b):
    s, e = two_sum(a[0], -b[0])
    return renorm(s, e + (a[1] - b[1]))


def pair_mul(a, b):
    p, e = two_prod(a[0], b[0])
    return renorm(p, e + (a[0] * b[1] + a[1] * b[0]))


def pair_div(a, b):
    first = a[0] / b[0]
    zero = jnp.zeros_like(first)
    rest = pair_sub(a, pair_mul((first, zero), b))
    return renorm(first, rest[0] / b[0])


def sum_rows(values):
    s = values[0:8]
    e = jnp.zeros_like(s)
    for start in range(8, values.shape[0], 8):
        s, err = two_sum(s, values[start : start + 8])
        e = e + err
    for shift in (4, 2, 1):
        s_other = pltpu.roll(s, shift, 0)
        e_other = pltpu.roll(e, shift, 0)
        s, err = two_sum(s, s_other)
        e = e + e_other + err
    hi, lo = renorm(s, e)
    return hi[0:1], lo[0:1]


def small_solve(hi_row, lo_row, order):
    row = lax.broadcasted_iota(jnp.int32, (8, 128), 0)
    lane = lax.broadcasted_iota(jnp.int32, (8, 128), 1)

    def matrix(values):
        wide = jnp.broadcast_to(values, (8, 128))
        out = jnp.zeros((8, 128), F32)
        for i in range(order):
            turned = wide if i == 0 else pltpu.roll(wide, 128 - 16 * i, 1)
            out = jnp.where(row == i, turned, out)
        return jnp.where(lane < 16, out, 0.0)

    hi, lo = matrix(hi_row), matrix(lo_row)
    ratio = hi[3:4, 3:4] / hi[3:4, 2:3]
    start = jnp.sum(jnp.where(row == lane, hi, 0.0), axis=1, keepdims=True)
    unit = jnp.where(row == lane, 1.0, 0.0)
    live = jnp.ones((8, 128), F32)
    for k in range(order):
        col = tuple(jnp.broadcast_to(v[:, k : k + 1], (8, 128)) for v in (hi, lo))
        piv_row = tuple(jnp.broadcast_to(v[k : k + 1, :], (8, 128)) for v in (hi, lo))
        piv = tuple(jnp.broadcast_to(v[k : k + 1, k : k + 1], (8, 128)) for v in (hi, lo))
        good = piv[0] > 1e-11 * jnp.broadcast_to(start[k : k + 1, :], (8, 128))
        piv = (jnp.where(good, piv[0], 1.0), jnp.where(good, piv[1], 0.0))
        factor = pair_div(col, piv)
        new = pair_sub((hi, lo), pair_mul(factor, piv_row))
        change = good & (row != k)
        hi = jnp.where(change, new[0], hi)
        lo = jnp.where(change, new[1], lo)
        live = jnp.where((row == k) & ~good, 0.0, live)
    diag = jnp.sum(jnp.where(row == lane, hi, 0.0), axis=1, keepdims=True)
    diag = jnp.where((diag != 0.0) & (live[:, 0:1] > 0.0), diag, 1.0)
    y = jnp.broadcast_to(hi[:, 8:9] / diag, (8, 128)) * live
    y = jnp.where(row < order, y, 0.0)
    del unit
    return y, jnp.broadcast_to(ratio, (8, 128))


def pack_body(rhs, surface, east, north, neast, nwest, land, out):
    for place, ref in enumerate((rhs, surface, east, north, neast, nwest)):
        out[place] = ref[...].T
    out[6] = land[...].astype(F32).T


def select_body(offset, ghosted, first, second, out):
    rho = offset[0, 0]
    same = offset[0, 1]
    i = lax.broadcasted_iota(jnp.int32, (PAD, 2 * 136), 0)
    u = lax.broadcasted_iota(jnp.int32, (PAD, 2 * 136), 1)
    plain = jnp.where(u == rho + PAD - i, 1.0, 0.0)
    moved = jnp.where(u == rho + PAD - 1 - i, 1.0, 0.0)
    for place, source in enumerate((0, 1, 2, 3, 5, 4, 6)):
        x, y = first[source], second[source]
        low = jnp.where(same == 0, y, x)
        high = jnp.where(same == 0, x, y)
        both = jnp.concatenate([low[0:136], high[8:PAD]], axis=0)
        facing = jnp.dot(moved if source == 2 else plain, both, precision=HIGHEST, preferred_element_type=F32)
        for part in range(4):
            out[part, place, 0:WIDE, :] = ghosted[place, OWN * part : OWN * part + WIDE, :]
            out[part, place, WIDE : 2 * WIDE, :] = facing[OWN * part : OWN * part + WIDE, :]


def east_of(v):
    return pltpu.roll(v, 127, v.ndim - 1)


def west_of(v):
    return pltpu.roll(v, 1, v.ndim - 1)


def facing_of(v):
    return pltpu.roll(v, 64, v.ndim - 1)


def row_before(v):
    s = lax.broadcasted_iota(jnp.int32, (8, 128), 0)
    return jnp.where(s == 0, 0.0, pltpu.roll(v, 1, 0))


def row_after(v):
    s = lax.broadcasted_iota(jnp.int32, (8, 128), 0)
    return jnp.where(s == 7, 0.0, pltpu.roll(v, 7, 0))


def line_solve(load, lines, below_mat, above_mat, y_buf, g_buf, finish):
    zero = jnp.zeros((8, 128), F32)

    def forward(t, y):
        y = load(t) + lines[MULT, t] * y
        y_buf[t] = y
        return y

    lax.fori_loop(0, STEPS, forward, zero, unroll=8)

    def backward(k, x):
        t = STEPS - 1 - k
        x = y_buf[t] * lines[IPIV, t] + lines[MULT, t + 1] * x
        g_buf[t] = x
        return x

    lax.fori_loop(0, STEPS, backward, zero, unroll=8)
    first, last = g_buf[0], g_buf[STEPS - 1]
    below, above = zero, zero
    for k in range(8):
        for base, ends in ((0, first), (8, last)):
            end = jnp.broadcast_to(ends[k : k + 1, :], (8, 128))
            below = below + below_mat[base + k] * end
            above = above + above_mat[base + k] * end

    def combine(c, _):
        t0 = c * 8
        g = g_buf[pl.ds(t0, 8)] + lines[LOWER, pl.ds(t0, 8)] * below + lines[UPPER, pl.ds(t0, 8)] * above
        finish(t0, g)
        return 0

    lax.fori_loop(0, STEPS // 8, combine, 0, unroll=2)


def operate(v_ref, place, w_ref, coef, fold, vp, ve, vw):
    for t, v in ((0, row_before(v_ref[place, STEPS - 1])), (STEPS + 1, row_after(v_ref[place, 0]))):
        vp[t] = v
        ve[t] = east_of(v)
        vw[t] = west_of(v)

    def step(c, _):
        t = c * 4
        here, up, down = pl.ds(t + 1, 4), pl.ds(t + 2, 4), pl.ds(t, 4)
        at = pl.ds(t, 4)
        out = coef[DIAG, at] * vp[here]
        side = coef[E, at] * ve[here] + coef[W, at] * vw[here]
        north = coef[N, at] * vp[up] + coef[NE, at] * ve[up] + coef[NW, at] * vw[up]
        south = coef[S, at] * vp[down] + coef[SW, at] * vw[down] + coef[SE, at] * ve[down]
        w_ref[place, at] = out - (side + north + south)
        return 0

    lax.fori_loop(0, STEPS // 4, step, 0, unroll=2)
    w_ref[place, STEPS - 1] = w_ref[place, STEPS - 1] - fold[...] * facing_of(v_ref[place, STEPS - 1])


def store_field(v_ref, place, vp, ve, vw):
    def finish_with(value_of):
        def finish(t0, g):
            v = value_of(t0, g)
            v_ref[place, pl.ds(t0, 8)] = v
            vp[pl.ds(t0 + 1, 8)] = v
            ve[pl.ds(t0 + 1, 8)] = east_of(v)
            vw[pl.ds(t0 + 1, 8)] = west_of(v)

        return finish

    return finish_with


def gram_row(entries, rows, out):
    lane = lax.broadcasted_iota(jnp.int32, (8, 128), 1)
    own = (lane >= GHOST) & (lane < GHOST + OWN)
    rows[...] = jnp.zeros((128, 128), F32)
    group = 16
    for start in range(0, len(entries), group):
        part = entries[start : start + group]

        def add(t, sums, part=part):
            return tuple(s + left(t) * right(t) for s, (left, right, _) in zip(sums, part))

        sums = lax.fori_loop(0, STEPS, add, tuple(jnp.zeros((8, 128), F32) for _ in part), unroll=2)
        for total, (_, _, places) in zip(sums, part):
            line = jnp.sum(jnp.where(own, total, 0.0), axis=0, keepdims=True)
            for place in places:
                rows[place : place + 1, :] = line
    summed = lax.dot_general(
        jnp.ones((8, 128), F32), rows[...], (((1,), (1,)), ((), ())), precision=HIGHEST, preferred_element_type=F32
    )
    out[...] = jnp.concatenate([summed] * 4, axis=0)


def at(ref, *index):
    return lambda t: ref[(*index, t)]


def first_body(recv, coef, lines, below_mat, above_mat, fold, r0, v_ref, w_ref, gram, raw, grid, y_buf, g_buf, vp, ve, vw, rows):
    s_id = lax.broadcasted_iota(jnp.int32, (8, 128), 0)
    zero = jnp.zeros((8, 128), F32)
    gap = jnp.zeros((64 - WIDE, 128), F32)
    for place in range(7):
        for source in range(4):
            both = recv[source, place]
            full = jnp.concatenate([both[0:WIDE], gap, both[WIDE : 2 * WIDE], gap], axis=0)
            raw[place, 128 * source : 128 * source + 128, :] = full.T
        for t in range(STEPS):
            grid[place, t + 1] = raw[place, pl.ds(t, 8, stride=STEPS), :]
    top_north = grid[3, STEPS]
    top_ocean = grid[6, STEPS]
    last = s_id == 7
    fold_open = jnp.where(last, 0.5 * (top_north + facing_of(top_north)), 0.0)
    fold[...] = fold_open * top_ocean * facing_of(top_ocean)
    for place in (3, 4, 5):
        grid[place, STEPS] = jnp.where(last, 0.0, grid[place, STEPS])
    for place in (3, 4, 5, 6):
        grid[place, 0] = row_before(grid[place, STEPS])
        grid[place, STEPS + 1] = row_after(grid[place, 1])

    def weigh(t, _):
        o, o_up, o_down = grid[6, t + 1], grid[6, t + 2], grid[6, t]
        east = grid[2, t + 1]
        north, neast, nwest = grid[3, t + 1], grid[4, t + 1], grid[5, t + 1]
        south, s_neast, s_nwest = grid[3, t], grid[4, t], grid[5, t]
        open_sum = zero
        parts = (
            (E, east, east_of(o)),
            (W, west_of(east), west_of(o)),
            (N, north, o_up),
            (S, south, o_down),
            (NE, neast, east_of(o_up)),
            (SW, west_of(s_neast), west_of(o_down)),
            (NW, nwest, west_of(o_up)),
            (SE, east_of(s_nwest), east_of(o_down)),
        )
        for place, edge, other in parts:
            coef[place, t] = edge * o * other
            open_sum = open_sum + edge
        surface = grid[1, t + 1]
        coef[DIAG, t] = o * (surface + open_sum) + (1.0 - o)
        r0[t] = o * grid[0, t + 1]
        y_buf[t] = o * (surface + north * o * o_up + south * o * o_down) + (1.0 - o)
        return 0

    lax.fori_loop(0, STEPS, weigh, 0, unroll=2)
    surface = grid[1, STEPS]
    o = top_ocean
    coef[DIAG, STEPS - 1] = coef[DIAG, STEPS - 1] + o * fold_open

    def pivots(t, carry):
        before, response = carry
        south = jnp.where(t == 0, zero, coef[S, t])
        mult = south * before
        inverse = 1.0 / (y_buf[t] - south * mult)
        lines[MULT, t] = mult
        lines[IPIV, t] = inverse
        response = jnp.where(t == 0, coef[S, 0], mult * response)
        g_buf[t] = response
        return inverse, response

    lax.fori_loop(0, STEPS, pivots, (zero, zero), unroll=4)
    for t in range(STEPS, lines.shape[1]):
        lines[MULT, t] = zero

    def respond(k, carry):
        low, up = carry
        t = STEPS - 1 - k
        factor = lines[MULT, t + 1]
        low = g_buf[t] * lines[IPIV, t] + factor * low
        up = jnp.where(k == 0, coef[N, STEPS - 1] * lines[IPIV, t], factor * up)
        lines[LOWER, t] = low
        lines[UPPER, t] = up
        return low, up

    lax.fori_loop(0, STEPS, respond, (zero, zero), unroll=4)
    unit = lax.broadcasted_iota(jnp.int32, (16, 128), 0)
    low_first, low_last = lines[LOWER, 0], lines[LOWER, STEPS - 1]
    up_first, up_last = lines[UPPER, 0], lines[UPPER, STEPS - 1]

    def spread(v, s):
        return jnp.broadcast_to(v[s : s + 1, :], (16, 128))

    alphas, betas, dens = [jnp.zeros((16, 128), F32)], [jnp.zeros((16, 128), F32)], []
    for s in range(8):
        alpha, beta = alphas[-1], betas[-1]
        g_first = jnp.where(unit == s, 1.0, 0.0)
        g_last = jnp.where(unit == 8 + s, 1.0, 0.0)
        lf, ll, uf, ul = (spread(v, s) for v in (low_first, low_last, up_first, up_last))
        den = 1.0 / (1.0 - lf * beta)
        dens.append(den)
        alphas.append(g_last + ll * (alpha + beta * den * (g_first + lf * alpha)))
        betas.append(ul + ll * beta * den * uf)
    above = jnp.zeros((16, 128), F32)
    for s in range(7, -1, -1):
        alpha, beta = alphas[s], betas[s]
        above_mat[:, s, :] = above
        lf, uf = spread(low_first, s), spread(up_first, s)
        g_first = jnp.where(unit == s, 1.0, 0.0)
        above = dens[s] * (g_first + lf * alpha + uf * above)
        below_mat[:, s, :] = alpha + beta * above
    finish_with = functools.partial(store_field, v_ref)
    for i in range(HALF):
        load = (lambda t: r0[t]) if i == 0 else (lambda t, i=i: w_ref[i - 1, t])
        value = (lambda t0, g: g) if i == 0 else (lambda t0, g: g * SCALE)
        line_solve(load, lines, below_mat, above_mat, y_buf, g_buf, finish_with(i, vp, ve, vw)(value))
        operate(v_ref, i, w_ref, coef, fold, vp, ve, vw)
    entries = []
    for i in range(HALF):
        for j in range(i, HALF):
            entries.append((at(v_ref, i), at(w_ref, j), sorted({16 * i + j, 16 * j + i})))
        entries.append((at(v_ref, i), lambda t: r0[t], [16 * i + 8]))
    gram_row(entries, rows, gram)


def second_body(sums, coef, lines, below_mat, above_mat, fold, r0, v1, w1, r_ref, y_out, v_ref, w_ref, gram, y_buf, g_buf, vp, ve, vw, rows):
    y, ratio = small_solve(*sum_rows(sums[...]), HALF)
    y_out[...] = y
    bound = ratio * (1.6 / SCALE)
    step = 2.0 / bound
    weights = [jnp.broadcast_to(y[i : i + 1, :], (8, 128)) for i in range(HALF)]

    def renew(t, _):
        r = r0[t]
        for i in range(HALF):
            r = r - weights[i] * w1[i, t]
        r_ref[t] = r
        return 0

    lax.fori_loop(0, STEPS, renew, 0, unroll=4)
    finish_with = functools.partial(store_field, v_ref)
    for i in range(HALF):
        load = (lambda t: r_ref[t]) if i == 0 else (lambda t, i=i: w_ref[i - 1, t])
        if i == 0:
            value = lambda t0, g: g
        elif i == 1:
            value = lambda t0, g: v_ref[0, pl.ds(t0, 8)] - step * g
        else:
            value = lambda t0, g, i=i: 2.0 * (v_ref[i - 1, pl.ds(t0, 8)] - step * g) - v_ref[i - 2, pl.ds(t0, 8)]
        line_solve(load, lines, below_mat, above_mat, y_buf, g_buf, finish_with(i, vp, ve, vw)(value))
        operate(v_ref, i, w_ref, coef, fold, vp, ve, vw)
    entries = []
    for i in range(TOTAL):
        left = at(v1, i) if i < HALF else at(v_ref, i - HALF)
        for j in range(i, TOTAL):
            right = at(w1, j) if j < HALF else at(w_ref, j - HALF)
            entries.append((left, right, sorted({16 * i + j, 16 * j + i})))
        entries.append((left, lambda t: r_ref[t], [16 * i + 8]))
    gram_row(entries, rows, gram)


def middle_body(values, out):
    hi, lo = sum_rows(values[...])
    row = lax.broadcasted_iota(jnp.int32, (16, 128), 0)
    even = (row & 1) == 0
    out[...] = jnp.where(even, jnp.broadcast_to(hi, (16, 128)), jnp.broadcast_to(lo, (16, 128)))


def last_body(sums, y1, r_ref, v1, w1, v2, w2, out, x_rows, r_rows):
    y, _ = small_solve(*sum_rows(sums[...]), TOTAL)
    w_weights = [jnp.broadcast_to(y[i : i + 1, :], (8, 128)) for i in range(TOTAL)]
    v_weights = [w + (y1[i : i + 1, :] if i < HALF else 0.0) for i, w in enumerate(w_weights)]
    for t in range(STEPS):
        x = jnp.zeros((8, 128), F32)
        r = r_ref[t]
        for i in range(HALF):
            x = x + v_weights[i] * v1[i, t]
            r = r - w_weights[i] * w1[i, t]
        for i in range(HALF):
            x = x + v_weights[HALF + i] * v2[i, t]
            r = r - w_weights[HALF + i] * w2[i, t]
        x_rows[pl.ds(t, 8, stride=STEPS), :] = x
        r_rows[pl.ds(t, 8, stride=STEPS), :] = r
    for place, rows in enumerate((x_rows, r_rows)):
        for part in range(4):
            out[part, place] = rows[128 * part : 128 * part + 128, :].T[GHOST : GHOST + OWN, :]


def unpack_body(recv, x, r):
    for place, ref in enumerate((x, r)):
        ref[...] = jnp.concatenate([recv[part, place] for part in range(4)], axis=0).T


def shape(*dims):
    return jax.ShapeDtypeStruct(dims, F32)


def vmem(*dims):
    return pltpu.VMEM(dims, F32)


FIELD = (STEPS, 8, 128)
SCRATCH = [vmem(*FIELD), vmem(*FIELD), vmem(STEPS + 2, 8, 128), vmem(STEPS + 2, 8, 128), vmem(STEPS + 2, 8, 128), vmem(128, 128)]


def all_sums(gram):
    near = lax.all_to_all(gram, ("lat", "x", "core"), split_axis=0, concat_axis=0, tiled=True)
    part = pl.pallas_call(middle_body, out_shape=shape(16, 128), name="add_near")(near)
    return lax.all_to_all(part, "z", split_axis=0, concat_axis=0, tiled=True)


def reflect_switch(block, half):
    def branch(q):
        return lambda b: lax.ppermute(b, LON, [(d, (2 * q - d) % 64) for d in range(64)])

    return lax.switch(half, [branch(q) for q in range(32)], block)


def shards(right_side, surface_term, east, north, neast, nwest, land_sea, fold_map):
    place = lax.axis_index(LON)
    offset = (fold_map[0] + COLS * place) % NLON
    block_offset = offset // COLS
    rho = offset % COLS
    odd = block_offset % 2
    packed = pl.pallas_call(pack_body, out_shape=shape(7, COLS, 128), name="pack")(
        right_side, surface_term, east, north, neast, nwest, land_sea
    )
    up = [(d, (d + 1) % 64) for d in range(64)]
    down = [(d, (d - 1) % 64) for d in range(64)]
    before = lax.ppermute(packed[:, COLS - GHOST :], LON, up)
    after = lax.ppermute(packed[:, :GHOST], LON, down)
    ghosted = jnp.concatenate([before, packed, after], axis=1)
    first = reflect_switch(ghosted, block_offset // 2)
    second = lax.cond(
        odd == 0, lambda b: lax.ppermute(b, LON, down), lambda b: lax.ppermute(b, LON, up), first
    )
    scalars = jnp.stack([rho, odd]).reshape(1, 2)
    windows = pl.pallas_call(
        select_body,
        in_specs=[pl.BlockSpec(memory_space=pltpu.SMEM)] + [pl.BlockSpec(memory_space=pltpu.VMEM)] * 3,
        out_shape=shape(4, 7, 2 * WIDE, 128),
        name="select",
        compiler_params=params(),
    )(scalars, ghosted, first, second)
    lines_in = lax.all_to_all(windows, "lat", split_axis=0, concat_axis=0, tiled=True)
    coef, lines, below_mat, above_mat, fold, r0, v1, w1, gram = pl.pallas_call(
        first_body,
        out_shape=(
            shape(9, *FIELD),
            shape(4, STEPS + 8, 8, 128),
            shape(16, 8, 128),
            shape(16, 8, 128),
            shape(8, 128),
            shape(*FIELD),
            shape(HALF, *FIELD),
            shape(HALF, *FIELD),
            shape(32, 128),
        ),
        scratch_shapes=[vmem(7, 512, 128), vmem(7, STEPS + 2, 8, 128), *SCRATCH],
        name="phase_one",
        compiler_params=params(),
    )(lines_in)
    sums = all_sums(gram)
    r4, y1, v2, w2, gram = pl.pallas_call(
        second_body,
        out_shape=(
            shape(*FIELD),
            shape(8, 128),
            shape(HALF, *FIELD),
            shape(HALF, *FIELD),
            shape(32, 128),
        ),
        scratch_shapes=SCRATCH,
        name="phase_two",
        compiler_params=params(),
    )(sums, coef, lines, below_mat, above_mat, fold, r0, v1, w1)
    sums = all_sums(gram)
    pieces = pl.pallas_call(
        last_body,
        out_shape=shape(4, 2, OWN, 128),
        scratch_shapes=[vmem(512, 128), vmem(512, 128)],
        name="combine",
        compiler_params=params(),
    )(sums, y1, r4, v1, w1, v2, w2)
    columns = lax.all_to_all(pieces, "lat", split_axis=0, concat_axis=0, tiled=True)
    return pl.pallas_call(unpack_body, out_shape=(shape(128, COLS), shape(128, COLS)), name="unpack")(columns)


def solution(mesh):
    finer = Mesh(mesh.devices.reshape(mesh.shape["lat"], 4, 8, 2), ("lat", *LON))
    field = P("lat", LON)
    return jax.shard_map(
        shards,
        mesh=finer,
        in_specs=(field,) * 7 + (P(LON),),
        out_specs=(field, field),
        check_vma=False,
    )
```

```python
import functools

import jax
import jax.numpy as jnp
from jax import lax
from jax.experimental import pallas as pl
from jax.experimental.pallas import tpu as pltpu
from jax.sharding import Mesh
from jax.sharding import PartitionSpec as P

LON = ("x", "z", "core")
NLON = 8192
COLS = 128
OWN = 32
GHOST = 8
WIDE = OWN + 2 * GHOST
PAD = COLS + 2 * GHOST
STEPS = 64
HALF = 4
TOTAL = 2 * HALF
SCALE = 1.0e-4
F32 = jnp.float32
HIGHEST = lax.Precision.HIGHEST
E, W, N, S, NE, SW, NW, SE, DIAG = range(9)
MULT, IPIV, LOWER, UPPER = range(4)


SIDE = 72


def params(mib=24):
    return pltpu.CompilerParams(vmem_limit_bytes=mib * 1024 * 1024)


def two_sum(a, b):
    s = a + b
    bb = s - a
    return s, (a - (s - bb)) + (b - bb)


def split(a):
    t = a * 4097.0
    hi = t - (t - a)
    return hi, a - hi


def two_prod(a, b):
    p = a * b
    ah, al = split(a)
    bh, bl = split(b)
    return p, ((ah * bh - p) + ah * bl + al * bh) + al * bl


def renorm(s, e):
    hi = s + e
    return hi, e - (hi - s)


def pair_sub(a, b):
    s, e = two_sum(a[0], -b[0])
    return renorm(s, e + (a[1] - b[1]))


def pair_mul(a, b):
    p, e = two_prod(a[0], b[0])
    return renorm(p, e + (a[0] * b[1] + a[1] * b[0]))


def pair_div(a, b):
    first = a[0] / b[0]
    zero = jnp.zeros_like(first)
    rest = pair_sub(a, pair_mul((first, zero), b))
    return renorm(first, rest[0] / b[0])


def sum_rows(values):
    s = values[0:8]
    e = jnp.zeros_like(s)
    for start in range(8, values.shape[0], 8):
        s, err = two_sum(s, values[start : start + 8])
        e = e + err
    for shift in (4, 2, 1):
        s_other = pltpu.roll(s, shift, 0)
        e_other = pltpu.roll(e, shift, 0)
        s, err = two_sum(s, s_other)
        e = e + e_other + err
    hi, lo = renorm(s, e)
    return hi[0:1], lo[0:1]


def small_solve(hi_row, lo_row, order):
    row = lax.broadcasted_iota(jnp.int32, (8, 128), 0)
    lane = lax.broadcasted_iota(jnp.int32, (8, 128), 1)

    def matrix(values):
        wide = jnp.broadcast_to(values, (8, 128))
        out = jnp.zeros((8, 128), F32)
        for i in range(order):
            turned = wide if i == 0 else pltpu.roll(wide, 128 - 16 * i, 1)
            out = jnp.where(row == i, turned, out)
        return jnp.where(lane < 16, out, 0.0)

    hi, lo = matrix(hi_row), matrix(lo_row)
    ratio = hi[3:4, 3:4] / hi[3:4, 2:3]
    start = jnp.sum(jnp.where(row == lane, hi, 0.0), axis=1, keepdims=True)
    live = jnp.ones((8, 128), F32)
    for k in range(order):
        col = tuple(jnp.broadcast_to(v[:, k : k + 1], (8, 128)) for v in (hi, lo))
        piv_row = tuple(jnp.broadcast_to(v[k : k + 1, :], (8, 128)) for v in (hi, lo))
        piv = tuple(jnp.broadcast_to(v[k : k + 1, k : k + 1], (8, 128)) for v in (hi, lo))
        good = piv[0] > 1e-11 * jnp.broadcast_to(start[k : k + 1, :], (8, 128))
        piv = (jnp.where(good, piv[0], 1.0), jnp.where(good, piv[1], 0.0))
        factor = pair_div(col, piv)
        new = pair_sub((hi, lo), pair_mul(factor, piv_row))
        change = good & (row != k)
        hi = jnp.where(change, new[0], hi)
        lo = jnp.where(change, new[1], lo)
        live = jnp.where((row == k) & ~good, 0.0, live)
    diag = jnp.sum(jnp.where(row == lane, hi, 0.0), axis=1, keepdims=True)
    diag = jnp.where((diag != 0.0) & (live[:, 0:1] > 0.0), diag, 1.0)
    y = jnp.broadcast_to(hi[:, 8:9] / diag, (8, 128)) * live
    y = jnp.where(row < order, y, 0.0)
    return y, jnp.broadcast_to(ratio, (8, 128))


def pack_body(place, rhs, surface, east, north, neast, nwest, land, out, *chunks):
    for k, ref in enumerate((rhs, surface, east, north, neast, nwest)):
        out[k] = ref[...].T
    out[6] = land[...].astype(F32).T
    for step, chunk in enumerate(chunks):
        start = pl.multiple_of(OWN * ((place[0] + step) & 3), OWN)
        chunk[...] = out[:, pl.ds(start, OWN), :]


def select_body(shift, low, main, high, out):
    i = lax.broadcasted_iota(jnp.int32, (PAD, COLS + 2 * SIDE), 0)
    u = lax.broadcasted_iota(jnp.int32, (PAD, COLS + 2 * SIDE), 1)
    reach = shift[0] + GHOST + SIDE
    plain = jnp.where(u == reach - i, 1.0, 0.0)
    moved = jnp.where(u == reach - 1 - i, 1.0, 0.0)
    for place, source in enumerate((0, 1, 2, 3, 5, 4, 6)):
        both = jnp.concatenate([low[source], main[source], high[source]], axis=0)
        facing = jnp.dot(moved if source == 2 else plain, both, precision=HIGHEST, preferred_element_type=F32)
        for part in range(4):
            out[part, place] = facing[OWN * part : OWN * part + WIDE, :]


def east_of(v):
    return pltpu.roll(v, 127, v.ndim - 1)


def west_of(v):
    return pltpu.roll(v, 1, v.ndim - 1)


def facing_of(v):
    return pltpu.roll(v, 64, v.ndim - 1)


def row_before(v):
    s = lax.broadcasted_iota(jnp.int32, (8, 128), 0)
    return jnp.where(s == 0, 0.0, pltpu.roll(v, 1, 0))


def row_after(v):
    s = lax.broadcasted_iota(jnp.int32, (8, 128), 0)
    return jnp.where(s == 7, 0.0, pltpu.roll(v, 7, 0))


def line_solve(load, lines, below_mat, above_mat, y_buf, g_buf, finish):
    zero = jnp.zeros((8, 128), F32)

    def forward(t, y):
        y = load(t) + lines[MULT, t] * y
        y_buf[t] = y
        return y

    lax.fori_loop(0, STEPS, forward, zero, unroll=8)

    def backward(k, x):
        t = STEPS - 1 - k
        x = y_buf[t] * lines[IPIV, t] + lines[MULT, t + 1] * x
        g_buf[t] = x
        return x

    lax.fori_loop(0, STEPS, backward, zero, unroll=8)
    first, last = g_buf[0], g_buf[STEPS - 1]
    below, above = zero, zero
    for k in range(8):
        for base, ends in ((0, first), (8, last)):
            end = jnp.broadcast_to(ends[k : k + 1, :], (8, 128))
            below = below + below_mat[base + k] * end
            above = above + above_mat[base + k] * end

    def combine(c, _):
        t0 = c * 8
        g = g_buf[pl.ds(t0, 8)] + lines[LOWER, pl.ds(t0, 8)] * below + lines[UPPER, pl.ds(t0, 8)] * above
        finish(t0, g)
        return 0

    lax.fori_loop(0, STEPS // 8, combine, 0, unroll=2)


def operate(v_ref, place, w_ref, coef, fold, vp, ve, vw):
    for t, v in ((0, row_before(v_ref[place, STEPS - 1])), (STEPS + 1, row_after(v_ref[place, 0]))):
        vp[t] = v
        ve[t] = east_of(v)
        vw[t] = west_of(v)

    def step(c, _):
        t = c * 4
        here, up, down = pl.ds(t + 1, 4), pl.ds(t + 2, 4), pl.ds(t, 4)
        at = pl.ds(t, 4)
        out = coef[DIAG, at] * vp[here]
        side = coef[E, at] * ve[here] + coef[W, at] * vw[here]
        north = coef[N, at] * vp[up] + coef[NE, at] * ve[up] + coef[NW, at] * vw[up]
        south = coef[S, at] * vp[down] + coef[SW, at] * vw[down] + coef[SE, at] * ve[down]
        w_ref[place, at] = out - (side + north + south)
        return 0

    lax.fori_loop(0, STEPS // 4, step, 0, unroll=2)
    w_ref[place, STEPS - 1] = w_ref[place, STEPS - 1] - fold[...] * facing_of(v_ref[place, STEPS - 1])


def store_field(v_ref, place, vp, ve, vw):
    def finish_with(value_of):
        def finish(t0, g):
            v = value_of(t0, g)
            v_ref[place, pl.ds(t0, 8)] = v
            vp[pl.ds(t0 + 1, 8)] = v
            ve[pl.ds(t0 + 1, 8)] = east_of(v)
            vw[pl.ds(t0 + 1, 8)] = west_of(v)

        return finish

    return finish_with


def gram_row(lefts, rights, pairs, exact, highs, lows, out):
    highs[...] = jnp.zeros(highs.shape, F32)
    lows[...] = jnp.zeros(lows.shape, F32)
    start = 0
    while start < len(pairs):
        end = start
        while end < len(pairs) and (pairs[end][0] == pairs[start][0] or end - start < 12) and end - start < 17:
            end += 1
        part = pairs[start:end]
        start = end

        def add(t, sums, part=part):
            left = {i: lefts[i](t) for i in sorted({i for i, _, _ in part})}
            right = {j: rights[j](t) for j in sorted({j for _, j, _ in part})}
            if not exact:
                return tuple((s + left[i] * right[j], e) for (s, e), (i, j, _) in zip(sums, part))
            left_halves = {i: split(v) for i, v in left.items()}
            right_halves = {j: split(v) for j, v in right.items()}
            out = []
            for (s, e), (i, j, _) in zip(sums, part):
                ah, al = left_halves[i]
                bh, bl = right_halves[j]
                s, err = two_sum(s, ah * bh)
                out.append((s, e + (err + (ah * bl + al * right[j]))))
            return tuple(out)

        zero = jnp.zeros((8, 128), F32)
        sums = lax.fori_loop(0, STEPS, add, tuple((zero, zero) for _ in part), unroll=1 if exact else 2)
        for (s, e), (_, _, lanes) in zip(sums, part):
            for lane in lanes:
                highs[pl.ds(lane, 8, stride=128), :] = s
                lows[pl.ds(lane, 8, stride=128), :] = e
    s, e = highs[0:128], lows[0:128]
    for k in range(1, 8):
        s, err = two_sum(s, highs[128 * k : 128 * k + 128])
        e = e + (err + lows[128 * k : 128 * k + 128])
    s, e = s.T, e.T
    hi, lo = sum_rows(jnp.concatenate([s[GHOST : GHOST + OWN], e[GHOST : GHOST + OWN]], axis=0))
    row = lax.broadcasted_iota(jnp.int32, (8, 128), 0)
    both = jnp.where((row & 1) == 0, jnp.broadcast_to(hi, (8, 128)), jnp.broadcast_to(lo, (8, 128)))
    out[...] = jnp.concatenate([both] * (out.shape[0] // 8), axis=0)


def gram_pairs(count):
    out = []
    for i in range(count):
        out += [(i, j, sorted({16 * i + j, 16 * j + i})) for j in range(i, count)]
        out.append((i, count, [16 * i + 8]))
    return out


def at(ref, *index):
    return lambda t: ref[(*index, t)]


def first_body(lat, c0, c1, c2, c3, lefts, rights, facing, coef, lines, below_mat, above_mat, fold, r0, v_ref, w_ref, gram, raw, grid, y_buf, g_buf, vp, ve, vw, highs, lows):
    s_id = lax.broadcasted_iota(jnp.int32, (8, 128), 0)
    zero = jnp.zeros((8, 128), F32)
    gap = jnp.zeros((64 - WIDE, 128), F32)
    for place in range(7):
        for step, chunk in enumerate((c0, c1, c2, c3)):
            source = (lat[0] - step) & 3
            left, right = lefts[(step - 1) % 4, place], rights[(step + 1) % 4, place]
            full = jnp.concatenate([left, chunk[place], right, gap, facing[source, place], gap], axis=0)
            raw[place, pl.ds(pl.multiple_of(128 * source, 128), 128), :] = full.T
        for t in range(STEPS):
            grid[place, t + 1] = raw[place, pl.ds(t, 8, stride=STEPS), :]
    top_north = grid[3, STEPS]
    top_ocean = grid[6, STEPS]
    last = s_id == 7
    fold_open = jnp.where(last, 0.5 * (top_north + facing_of(top_north)), 0.0)
    fold[...] = fold_open * top_ocean * facing_of(top_ocean)
    for place in (3, 4, 5):
        grid[place, STEPS] = jnp.where(last, 0.0, grid[place, STEPS])
    for place in (3, 4, 5, 6):
        grid[place, 0] = row_before(grid[place, STEPS])
        grid[place, STEPS + 1] = row_after(grid[place, 1])

    def weigh(t, _):
        o, o_up, o_down = grid[6, t + 1], grid[6, t + 2], grid[6, t]
        east = grid[2, t + 1]
        north, neast, nwest = grid[3, t + 1], grid[4, t + 1], grid[5, t + 1]
        south, s_neast, s_nwest = grid[3, t], grid[4, t], grid[5, t]
        open_sum = zero
        parts = (
            (E, east, east_of(o)),
            (W, west_of(east), west_of(o)),
            (N, north, o_up),
            (S, south, o_down),
            (NE, neast, east_of(o_up)),
            (SW, west_of(s_neast), west_of(o_down)),
            (NW, nwest, west_of(o_up)),
            (SE, east_of(s_nwest), east_of(o_down)),
        )
        for place, edge, other in parts:
            coef[place, t] = edge * o * other
            open_sum = open_sum + edge
        surface = grid[1, t + 1]
        coef[DIAG, t] = o * (surface + open_sum) + (1.0 - o)
        r0[t] = o * grid[0, t + 1]
        vw[t] = o * (surface + coef[N, t] + coef[S, t]) + (1.0 - o)
        return 0

    lax.fori_loop(0, STEPS, weigh, 0, unroll=2)
    surface = grid[1, STEPS]
    o = top_ocean
    coef[DIAG, STEPS - 1] = coef[DIAG, STEPS - 1] + o * fold_open

    def eliminate(t, carry):
        ratio, beyond = carry
        north = coef[N, t]
        pivot = vw[t] - coef[S, t] * ratio
        more, err = two_sum(pivot, -north)
        more = more + err
        y_buf[t] = more - ratio * beyond
        guess = north / pivot
        prod, err = two_prod(guess, pivot)
        return guess + ((north - prod) - err) / pivot, more

    ends = lax.fori_loop(0, STEPS, eliminate, (zero, zero), unroll=2)
    lax.fori_loop(0, STEPS, eliminate, tuple(row_before(v) for v in ends), unroll=2)

    def pivots(t, carry):
        before, beyond, response, source = carry
        rest = y_buf[t]
        mult = jnp.where(t == 0, zero, coef[S, t] * before)
        beyond = rest + jnp.where(t == 0, coef[S, 0], mult * beyond)
        inverse = 1.0 / (coef[N, t] + beyond)
        lines[MULT, t] = mult
        lines[IPIV, t] = inverse
        response = jnp.where(t == 0, coef[S, 0], mult * response)
        source = rest + mult * source
        g_buf[t] = response
        vp[t] = source
        return inverse, beyond, response, source

    lax.fori_loop(0, STEPS, pivots, (zero,) * 4, unroll=4)
    for t in range(STEPS, lines.shape[1]):
        lines[MULT, t] = zero

    def respond(k, carry):
        low, up, source = carry
        t = STEPS - 1 - k
        factor = lines[MULT, t + 1]
        inverse = lines[IPIV, t]
        low = g_buf[t] * inverse + factor * low
        up = jnp.where(k == 0, coef[N, STEPS - 1] * inverse, factor * up)
        source = vp[t] * inverse + factor * source
        lines[LOWER, t] = low
        lines[UPPER, t] = up
        ve[t] = source
        return low, up, source

    lax.fori_loop(0, STEPS, respond, (zero,) * 3, unroll=4)
    unit = lax.broadcasted_iota(jnp.int32, (16, 128), 0)
    low_first, low_last = lines[LOWER, 0], lines[LOWER, STEPS - 1]
    up_first, up_last = lines[UPPER, 0], lines[UPPER, STEPS - 1]

    def spread(v, s):
        return jnp.broadcast_to(v[s : s + 1, :], (16, 128))

    source_first, source_last = ve[0], ve[STEPS - 1]
    alphas, betas, dens = [jnp.zeros((16, 128), F32)], [jnp.zeros((16, 128), F32)], []
    short = jnp.ones((16, 128), F32)
    for s in range(8):
        alpha, beta = alphas[-1], betas[-1]
        g_first = jnp.where(unit == s, 1.0, 0.0)
        g_last = jnp.where(unit == 8 + s, 1.0, 0.0)
        lf, ll, uf, ul = (spread(v, s) for v in (low_first, low_last, up_first, up_last))
        sf, sl = spread(source_first, s), spread(source_last, s)
        den = 1.0 / (sf + uf + short * lf)
        dens.append(den)
        alphas.append(g_last + ll * (alpha + beta * den * (g_first + lf * alpha)))
        betas.append(ul + ll * beta * den * uf)
        short = sl + ll * (short + beta * den * (sf + lf * short))
    above = jnp.zeros((16, 128), F32)
    for s in range(7, -1, -1):
        alpha, beta = alphas[s], betas[s]
        above_mat[:, s, :] = above
        lf, uf = spread(low_first, s), spread(up_first, s)
        g_first = jnp.where(unit == s, 1.0, 0.0)
        above = dens[s] * (g_first + lf * alpha + uf * above)
        below_mat[:, s, :] = alpha + beta * above
    finish_with = functools.partial(store_field, v_ref)
    for i in range(HALF):
        load = (lambda t: r0[t]) if i == 0 else (lambda t, i=i: w_ref[i - 1, t])
        value = (lambda t0, g: g) if i == 0 else (lambda t0, g: g * SCALE)
        line_solve(load, lines, below_mat, above_mat, y_buf, g_buf, finish_with(i, vp, ve, vw)(value))
        operate(v_ref, i, w_ref, coef, fold, vp, ve, vw)
    lefts = [at(v_ref, i) for i in range(HALF)]
    rights = [at(w_ref, j) for j in range(HALF)] + [at(r0)]
    gram_row(lefts, rights, gram_pairs(HALF), False, highs, lows, gram)


def second_body(sums, coef, lines, below_mat, above_mat, fold, r0, v1, w1, r_ref, y_out, v_ref, w_ref, gram, y_buf, g_buf, vp, ve, vw, highs, lows):
    y, ratio = small_solve(*sum_rows(sums[...]), HALF)
    y_out[...] = y
    bound = ratio * (2.0 / SCALE)
    step = 2.0 / bound
    weights = [jnp.broadcast_to(y[i : i + 1, :], (8, 128)) for i in range(HALF)]

    def renew(t, _):
        r = r0[t]
        for i in range(HALF):
            r = r - weights[i] * w1[i, t]
        r_ref[t] = r
        return 0

    lax.fori_loop(0, STEPS, renew, 0, unroll=4)
    finish_with = functools.partial(store_field, v_ref)
    for i in range(HALF):
        load = (lambda t: r_ref[t]) if i == 0 else (lambda t, i=i: w_ref[i - 1, t])
        if i == 0:
            value = lambda t0, g: g
        elif i == 1:
            value = lambda t0, g: v_ref[0, pl.ds(t0, 8)] - step * g
        else:
            value = lambda t0, g, i=i: 2.0 * (v_ref[i - 1, pl.ds(t0, 8)] - step * g) - v_ref[i - 2, pl.ds(t0, 8)]
        line_solve(load, lines, below_mat, above_mat, y_buf, g_buf, finish_with(i, vp, ve, vw)(value))
        operate(v_ref, i, w_ref, coef, fold, vp, ve, vw)
    lefts = [at(ref, i) for ref in (v1, v_ref) for i in range(HALF)]
    rights = [at(ref, j) for ref in (w1, w_ref) for j in range(HALF)] + [at(r_ref)]
    gram_row(lefts, rights, gram_pairs(TOTAL), True, highs, lows, gram)


def last_body(sums, y1, r_ref, v1, w1, v2, w2, out, x_rows, r_rows):
    y, _ = small_solve(*sum_rows(sums[...]), TOTAL)
    w_weights = [jnp.broadcast_to(y[i : i + 1, :], (8, 128)) for i in range(TOTAL)]
    v_weights = [w + (y1[i : i + 1, :] if i < HALF else 0.0) for i, w in enumerate(w_weights)]
    for t in range(STEPS):
        x = jnp.zeros((8, 128), F32)
        r = r_ref[t]
        for i in range(HALF):
            x = x + v_weights[i] * v1[i, t]
            r = r - w_weights[i] * w1[i, t]
        for i in range(HALF):
            x = x + v_weights[HALF + i] * v2[i, t]
            r = r - w_weights[HALF + i] * w2[i, t]
        x_rows[pl.ds(t, 8, stride=STEPS), :] = x
        r_rows[pl.ds(t, 8, stride=STEPS), :] = r
    for place, rows in enumerate((x_rows, r_rows)):
        for part in range(4):
            out[part, place] = rows[128 * part : 128 * part + 128, :].T[GHOST : GHOST + OWN, :]


def unpack_body(recv, x, r):
    for place, ref in enumerate((x, r)):
        ref[...] = jnp.concatenate([recv[part, place] for part in range(4)], axis=0).T


def shape(*dims):
    return jax.ShapeDtypeStruct(dims, F32)


def vmem(*dims):
    return pltpu.VMEM(dims, F32)


FIELD = (STEPS, 8, 128)
SCRATCH = [vmem(*FIELD), vmem(*FIELD), vmem(STEPS + 2, 8, 128), vmem(STEPS + 2, 8, 128), vmem(STEPS + 2, 8, 128), vmem(1024, 128), vmem(1024, 128)]


def all_sums(gram):
    return lax.all_to_all(gram, ("lat", *LON), split_axis=0, concat_axis=0, tiled=True)


def reflect(block, centre):
    def branch(q):
        return lambda b: lax.ppermute(b, LON, [(d, (q - d) % 64) for d in range(64)])

    return lax.switch(centre, [branch(q) for q in range(64)], block)


def shards(right_side, surface_term, east, north, neast, nwest, land_sea, fold_map):
    lat = lax.axis_index("lat").reshape(1)
    offset = (fold_map[0] + COLS * lax.axis_index(LON)) % NLON
    centre = ((offset - COLS // 2) % NLON) // COLS
    shift = (offset - COLS // 2) % COLS + COLS // 2
    smem = pl.BlockSpec(memory_space=pltpu.SMEM)
    whole = pl.BlockSpec(memory_space=pltpu.VMEM)
    packed, *chunks = pl.pallas_call(
        pack_body,
        in_specs=[smem] + [whole] * 7,
        out_shape=(shape(7, COLS, 128),) + (shape(7, OWN, 128),) * 4,
        name="pack",
        compiler_params=params(),
    )(lat, right_side, surface_term, east, north, neast, nwest, land_sea)
    for step in range(1, 4):
        chunks[step] = lax.ppermute(chunks[step], "lat", [(i, (i + step) % 4) for i in range(4)])
    up = [(d, (d + 1) % 64) for d in range(64)]
    down = [(d, (d - 1) % 64) for d in range(64)]
    main = reflect(packed, centre)
    low = lax.ppermute(main[:, COLS - SIDE :], LON, down)
    high = lax.ppermute(main[:, :SIDE], LON, up)
    where = [64 * (k % 4) + k // 4 for k in range(256)]
    lefts = jnp.stack([c[:, OWN - GHOST :] for c in chunks])
    rights = jnp.stack([c[:, :GHOST] for c in chunks])
    lefts = lax.ppermute(lefts, ("lat", *LON), [(where[k], where[(k + 1) % 256]) for k in range(256)])
    rights = lax.ppermute(rights, ("lat", *LON), [(where[k], where[k - 1]) for k in range(256)])
    windows = pl.pallas_call(
        select_body,
        in_specs=[smem] + [whole] * 3,
        out_shape=shape(4, 7, WIDE, 128),
        name="select",
        compiler_params=params(),
    )(shift.reshape(1), low, main, high)
    facing = lax.all_to_all(windows, "lat", split_axis=0, concat_axis=0, tiled=True)
    coef, lines, below_mat, above_mat, fold, r0, v1, w1, gram = pl.pallas_call(
        first_body,
        out_shape=(
            shape(9, *FIELD),
            shape(4, STEPS + 8, 8, 128),
            shape(16, 8, 128),
            shape(16, 8, 128),
            shape(8, 128),
            shape(*FIELD),
            shape(HALF, *FIELD),
            shape(HALF, *FIELD),
            shape(512, 128),
        ),
        scratch_shapes=[vmem(7, 512, 128), vmem(7, STEPS + 2, 8, 128), *SCRATCH],
        in_specs=[smem] + [whole] * 7,
        name="phase_one",
        compiler_params=params(),
    )(lat, *chunks, lefts, rights, facing)
    sums = all_sums(gram)
    r4, y1, v2, w2, gram = pl.pallas_call(
        second_body,
        out_shape=(
            shape(*FIELD),
            shape(8, 128),
            shape(HALF, *FIELD),
            shape(HALF, *FIELD),
            shape(512, 128),
        ),
        scratch_shapes=SCRATCH,
        name="phase_two",
        compiler_params=params(),
    )(sums, coef, lines, below_mat, above_mat, fold, r0, v1, w1)
    sums = all_sums(gram)
    pieces = pl.pallas_call(
        last_body,
        out_shape=shape(4, 2, OWN, 128),
        scratch_shapes=[vmem(512, 128), vmem(512, 128)],
        name="combine",
        compiler_params=params(),
    )(sums, y1, r4, v1, w1, v2, w2)
    columns = lax.all_to_all(pieces, "lat", split_axis=0, concat_axis=0, tiled=True)
    return pl.pallas_call(unpack_body, out_shape=(shape(128, COLS), shape(128, COLS)), name="unpack")(columns)


def solution(mesh):
    finer = Mesh(mesh.devices.reshape(mesh.shape["lat"], 4, 8, 2), ("lat", *LON))
    field = P("lat", LON)
    return jax.shard_map(
        shards,
        mesh=finer,
        in_specs=(field,) * 7 + (P(LON),),
        out_specs=(field, field),
        check_vma=False,
    )
```

```python
import functools

import jax
import jax.numpy as jnp
from jax import lax
from jax.experimental import pallas as pl
from jax.experimental.pallas import tpu as pltpu
from jax.sharding import Mesh
from jax.sharding import PartitionSpec as P

LON = ("x", "z", "core")
NLON = 8192
COLS = 128
OWN = 32
GHOST = 8
WIDE = OWN + 2 * GHOST
PAD = COLS + 2 * GHOST
STEPS = 64
HALF = 4
TOTAL = 2 * HALF
SCALE = 1.0e-4
F32 = jnp.float32
HIGHEST = lax.Precision.HIGHEST
E, W, N, S, NE, SW, NW, SE, DIAG = range(9)
MULT, IPIV, LOWER, UPPER = range(4)


SIDE = 72


def params(mib=24):
    return pltpu.CompilerParams(vmem_limit_bytes=mib * 1024 * 1024)


def two_sum(a, b):
    s = a + b
    bb = s - a
    return s, (a - (s - bb)) + (b - bb)


def split(a):
    t = a * 4097.0
    hi = t - (t - a)
    return hi, a - hi


def two_prod(a, b):
    p = a * b
    ah, al = split(a)
    bh, bl = split(b)
    return p, ((ah * bh - p) + ah * bl + al * bh) + al * bl


def renorm(s, e):
    hi = s + e
    return hi, e - (hi - s)


def pair_sub(a, b):
    s, e = two_sum(a[0], -b[0])
    return renorm(s, e + (a[1] - b[1]))


def pair_mul(a, b):
    p, e = two_prod(a[0], b[0])
    return renorm(p, e + (a[0] * b[1] + a[1] * b[0]))


def pair_div(a, b):
    first = a[0] / b[0]
    zero = jnp.zeros_like(first)
    rest = pair_sub(a, pair_mul((first, zero), b))
    return renorm(first, rest[0] / b[0])


def sum_rows(values):
    s = values[0:8]
    e = jnp.zeros_like(s)
    for start in range(8, values.shape[0], 8):
        s, err = two_sum(s, values[start : start + 8])
        e = e + err
    for shift in (4, 2, 1):
        s_other = pltpu.roll(s, shift, 0)
        e_other = pltpu.roll(e, shift, 0)
        s, err = two_sum(s, s_other)
        e = e + e_other + err
    hi, lo = renorm(s, e)
    return hi[0:1], lo[0:1]


def small_solve(hi_row, lo_row, order):
    row = lax.broadcasted_iota(jnp.int32, (8, 128), 0)
    lane = lax.broadcasted_iota(jnp.int32, (8, 128), 1)

    def matrix(values):
        wide = jnp.broadcast_to(values, (8, 128))
        out = jnp.zeros((8, 128), F32)
        for i in range(order):
            turned = wide if i == 0 else pltpu.roll(wide, 128 - 16 * i, 1)
            out = jnp.where(row == i, turned, out)
        return jnp.where(lane < 16, out, 0.0)

    hi, lo = matrix(hi_row), matrix(lo_row)
    ratio = hi[3:4, 3:4] / hi[3:4, 2:3]
    start = jnp.sum(jnp.where(row == lane, hi, 0.0), axis=1, keepdims=True)
    live = jnp.ones((8, 128), F32)
    for k in range(order):
        col = tuple(jnp.broadcast_to(v[:, k : k + 1], (8, 128)) for v in (hi, lo))
        piv_row = tuple(jnp.broadcast_to(v[k : k + 1, :], (8, 128)) for v in (hi, lo))
        piv = tuple(jnp.broadcast_to(v[k : k + 1, k : k + 1], (8, 128)) for v in (hi, lo))
        good = piv[0] > 1e-11 * jnp.broadcast_to(start[k : k + 1, :], (8, 128))
        piv = (jnp.where(good, piv[0], 1.0), jnp.where(good, piv[1], 0.0))
        factor = pair_div(col, piv)
        new = pair_sub((hi, lo), pair_mul(factor, piv_row))
        change = good & (row != k)
        hi = jnp.where(change, new[0], hi)
        lo = jnp.where(change, new[1], lo)
        live = jnp.where((row == k) & ~good, 0.0, live)
    diag = jnp.sum(jnp.where(row == lane, hi, 0.0), axis=1, keepdims=True)
    diag = jnp.where((diag != 0.0) & (live[:, 0:1] > 0.0), diag, 1.0)
    y = jnp.broadcast_to(hi[:, 8:9] / diag, (8, 128)) * live
    y = jnp.where(row < order, y, 0.0)
    return y, jnp.broadcast_to(ratio, (8, 128))


def pack_body(place, rhs, surface, east, north, neast, nwest, land, out, *chunks):
    for k, ref in enumerate((rhs, surface, east, north, neast, nwest)):
        out[k] = ref[...].T
    out[6] = land[...].astype(F32).T
    for step, chunk in enumerate(chunks):
        start = pl.multiple_of(OWN * ((place[0] + step) & 3), OWN)
        chunk[...] = out[:, pl.ds(start, OWN), :]


def select_body(shift, low, main, high, out):
    i = lax.broadcasted_iota(jnp.int32, (PAD, COLS + 2 * SIDE), 0)
    u = lax.broadcasted_iota(jnp.int32, (PAD, COLS + 2 * SIDE), 1)
    reach = shift[0] + GHOST + SIDE
    plain = jnp.where(u == reach - i, 1.0, 0.0)
    moved = jnp.where(u == reach - 1 - i, 1.0, 0.0)
    for place, source in enumerate((0, 1, 2, 3, 5, 4, 6)):
        both = jnp.concatenate([low[source], main[source], high[source]], axis=0)
        facing = jnp.dot(moved if source == 2 else plain, both, precision=HIGHEST, preferred_element_type=F32)
        for part in range(4):
            out[part, place] = facing[OWN * part : OWN * part + WIDE, :]


def east_of(v):
    return pltpu.roll(v, 127, v.ndim - 1)


def west_of(v):
    return pltpu.roll(v, 1, v.ndim - 1)


def facing_of(v):
    return pltpu.roll(v, 64, v.ndim - 1)


def row_before(v):
    s = lax.broadcasted_iota(jnp.int32, (8, 128), 0)
    return jnp.where(s == 0, 0.0, pltpu.roll(v, 1, 0))


def row_after(v):
    s = lax.broadcasted_iota(jnp.int32, (8, 128), 0)
    return jnp.where(s == 7, 0.0, pltpu.roll(v, 7, 0))


def line_solve(load, lines, below_mat, above_mat, y_buf, g_buf, finish):
    zero = jnp.zeros((8, 128), F32)

    def forward(t, y):
        y = load(t) + lines[MULT, t] * y
        y_buf[t] = y
        return y

    lax.fori_loop(0, STEPS, forward, zero, unroll=8)

    def backward(k, x):
        t = STEPS - 1 - k
        x = y_buf[t] * lines[IPIV, t] + lines[MULT, t + 1] * x
        g_buf[t] = x
        return x

    lax.fori_loop(0, STEPS, backward, zero, unroll=8)
    first, last = g_buf[0], g_buf[STEPS - 1]
    below, above = zero, zero
    for k in range(8):
        for base, ends in ((0, first), (8, last)):
            end = jnp.broadcast_to(ends[k : k + 1, :], (8, 128))
            below = below + below_mat[base + k] * end
            above = above + above_mat[base + k] * end

    def combine(c, _):
        t0 = c * 8
        g = g_buf[pl.ds(t0, 8)] + lines[LOWER, pl.ds(t0, 8)] * below + lines[UPPER, pl.ds(t0, 8)] * above
        finish(t0, g)
        return 0

    lax.fori_loop(0, STEPS // 8, combine, 0, unroll=2)


def operate(v_ref, place, w_ref, coef, fold, vp, ve, vw):
    for t, v in ((0, row_before(v_ref[place, STEPS - 1])), (STEPS + 1, row_after(v_ref[place, 0]))):
        vp[t] = v
        ve[t] = east_of(v)
        vw[t] = west_of(v)

    def step(c, _):
        t = c * 4
        here, up, down = pl.ds(t + 1, 4), pl.ds(t + 2, 4), pl.ds(t, 4)
        at = pl.ds(t, 4)
        out = coef[DIAG, at] * vp[here]
        side = coef[E, at] * ve[here] + coef[W, at] * vw[here]
        north = coef[N, at] * vp[up] + coef[NE, at] * ve[up] + coef[NW, at] * vw[up]
        south = coef[S, at] * vp[down] + coef[SW, at] * vw[down] + coef[SE, at] * ve[down]
        w_ref[place, at] = out - (side + north + south)
        return 0

    lax.fori_loop(0, STEPS // 4, step, 0, unroll=2)
    w_ref[place, STEPS - 1] = w_ref[place, STEPS - 1] - fold[...] * facing_of(v_ref[place, STEPS - 1])


def store_field(v_ref, place, vp, ve, vw):
    def finish_with(value_of):
        def finish(t0, g):
            v = value_of(t0, g)
            v_ref[place, pl.ds(t0, 8)] = v
            vp[pl.ds(t0 + 1, 8)] = v
            ve[pl.ds(t0 + 1, 8)] = east_of(v)
            vw[pl.ds(t0 + 1, 8)] = west_of(v)

        return finish

    return finish_with


def gram_row(lefts, rights, pairs, exact, highs, lows, out):
    highs[...] = jnp.zeros(highs.shape, F32)
    lows[...] = jnp.zeros(lows.shape, F32)
    start = 0
    while start < len(pairs):
        end = start
        while end < len(pairs) and (pairs[end][0] == pairs[start][0] or end - start < 12) and end - start < 17:
            end += 1
        part = pairs[start:end]
        start = end

        def add(t, sums, part=part):
            left = {i: lefts[i](t) for i in sorted({i for i, _, _ in part})}
            right = {j: rights[j](t) for j in sorted({j for _, j, _ in part})}
            if not exact:
                return tuple((s + left[i] * right[j], e) for (s, e), (i, j, _) in zip(sums, part))
            left_halves = {i: split(v) for i, v in left.items()}
            right_halves = {j: split(v) for j, v in right.items()}
            out = []
            for (s, e), (i, j, _) in zip(sums, part):
                ah, al = left_halves[i]
                bh, bl = right_halves[j]
                s, err = two_sum(s, ah * bh)
                out.append((s, e + (err + (ah * bl + al * right[j]))))
            return tuple(out)

        zero = jnp.zeros((8, 128), F32)
        sums = lax.fori_loop(0, STEPS, add, tuple((zero, zero) for _ in part), unroll=1 if exact else 2)
        for (s, e), (_, _, lanes) in zip(sums, part):
            for lane in lanes:
                highs[pl.ds(lane, 8, stride=128), :] = s
                lows[pl.ds(lane, 8, stride=128), :] = e
    s, e = highs[0:128], lows[0:128]
    for k in range(1, 8):
        s, err = two_sum(s, highs[128 * k : 128 * k + 128])
        e = e + (err + lows[128 * k : 128 * k + 128])
    s, e = s.T, e.T
    hi, lo = sum_rows(jnp.concatenate([s[GHOST : GHOST + OWN], e[GHOST : GHOST + OWN]], axis=0))
    row = lax.broadcasted_iota(jnp.int32, (8, 128), 0)
    both = jnp.where((row & 1) == 0, jnp.broadcast_to(hi, (8, 128)), jnp.broadcast_to(lo, (8, 128)))
    out[...] = jnp.concatenate([both] * (out.shape[0] // 8), axis=0)


def gram_pairs(count):
    out = []
    for i in range(count):
        out += [(i, j, sorted({16 * i + j, 16 * j + i})) for j in range(i, count)]
        out.append((i, count, [16 * i + 8]))
    return out


def at(ref, *index):
    return lambda t: ref[(*index, t)]


def first_body(lat, c0, c1, c2, c3, lefts, rights, facing, coef, lines, below_mat, above_mat, fold, r0, v_ref, w_ref, gram, raw, grid, y_buf, g_buf, vp, ve, vw, highs, lows):
    s_id = lax.broadcasted_iota(jnp.int32, (8, 128), 0)
    zero = jnp.zeros((8, 128), F32)
    gap = jnp.zeros((64 - WIDE, 128), F32)
    for place in range(7):
        for step, chunk in enumerate((c0, c1, c2, c3)):
            source = (lat[0] - step) & 3
            left, right = lefts[(step - 1) % 4, place], rights[(step + 1) % 4, place]
            full = jnp.concatenate([left, chunk[place], right, gap, facing[source, place], gap], axis=0)
            raw[place, pl.ds(pl.multiple_of(128 * source, 128), 128), :] = full.T
        for t in range(STEPS):
            grid[place, t + 1] = raw[place, pl.ds(t, 8, stride=STEPS), :]
    top_north = grid[3, STEPS]
    top_ocean = grid[6, STEPS]
    last = s_id == 7
    fold_open = jnp.where(last, 0.5 * (top_north + facing_of(top_north)), 0.0)
    fold[...] = fold_open * top_ocean * facing_of(top_ocean)
    for place in (3, 4, 5):
        grid[place, STEPS] = jnp.where(last, 0.0, grid[place, STEPS])
    for place in (3, 4, 5, 6):
        grid[place, 0] = row_before(grid[place, STEPS])
        grid[place, STEPS + 1] = row_after(grid[place, 1])

    def weigh(t, _):
        o, o_up, o_down = grid[6, t + 1], grid[6, t + 2], grid[6, t]
        east = grid[2, t + 1]
        north, neast, nwest = grid[3, t + 1], grid[4, t + 1], grid[5, t + 1]
        south, s_neast, s_nwest = grid[3, t], grid[4, t], grid[5, t]
        open_sum = zero
        parts = (
            (E, east, east_of(o)),
            (W, west_of(east), west_of(o)),
            (N, north, o_up),
            (S, south, o_down),
            (NE, neast, east_of(o_up)),
            (SW, west_of(s_neast), west_of(o_down)),
            (NW, nwest, west_of(o_up)),
            (SE, east_of(s_nwest), east_of(o_down)),
        )
        for place, edge, other in parts:
            coef[place, t] = edge * o * other
            open_sum = open_sum + edge
        surface = grid[1, t + 1]
        coef[DIAG, t] = o * (surface + open_sum) + (1.0 - o)
        r0[t] = o * grid[0, t + 1]
        vw[t] = o * (surface + coef[N, t] + coef[S, t]) + (1.0 - o)
        return 0

    lax.fori_loop(0, STEPS, weigh, 0, unroll=2)
    surface = grid[1, STEPS]
    o = top_ocean
    coef[DIAG, STEPS - 1] = coef[DIAG, STEPS - 1] + o * fold_open

    def eliminate(t, carry):
        ratio, beyond = carry
        north = coef[N, t]
        pivot = vw[t] - coef[S, t] * ratio
        more, err = two_sum(pivot, -north)
        more = more + err
        y_buf[t] = more - ratio * beyond
        guess = north / pivot
        prod, err = two_prod(guess, pivot)
        return guess + ((north - prod) - err) / pivot, more

    ends = lax.fori_loop(0, STEPS, eliminate, (zero, zero), unroll=2)
    lax.fori_loop(0, STEPS, eliminate, tuple(row_before(v) for v in ends), unroll=2)

    def pivots(t, carry):
        before, beyond, response, source = carry
        rest = y_buf[t]
        mult = jnp.where(t == 0, zero, coef[S, t] * before)
        beyond = rest + jnp.where(t == 0, coef[S, 0], mult * beyond)
        inverse = 1.0 / (coef[N, t] + beyond)
        lines[MULT, t] = mult
        lines[IPIV, t] = inverse
        response = jnp.where(t == 0, coef[S, 0], mult * response)
        source = rest + mult * source
        g_buf[t] = response
        vp[t] = source
        return inverse, beyond, response, source

    lax.fori_loop(0, STEPS, pivots, (zero,) * 4, unroll=4)
    for t in range(STEPS, lines.shape[1]):
        lines[MULT, t] = zero

    def respond(k, carry):
        low, up, source = carry
        t = STEPS - 1 - k
        factor = lines[MULT, t + 1]
        inverse = lines[IPIV, t]
        low = g_buf[t] * inverse + factor * low
        up = jnp.where(k == 0, coef[N, STEPS - 1] * inverse, factor * up)
        source = vp[t] * inverse + factor * source
        lines[LOWER, t] = low
        lines[UPPER, t] = up
        ve[t] = source
        return low, up, source

    lax.fori_loop(0, STEPS, respond, (zero,) * 3, unroll=4)
    unit = lax.broadcasted_iota(jnp.int32, (16, 128), 0)
    low_first, low_last = lines[LOWER, 0], lines[LOWER, STEPS - 1]
    up_first, up_last = lines[UPPER, 0], lines[UPPER, STEPS - 1]

    def spread(v, s):
        return jnp.broadcast_to(v[s : s + 1, :], (16, 128))

    source_first, source_last = ve[0], ve[STEPS - 1]
    alphas, betas, dens = [jnp.zeros((16, 128), F32)], [jnp.zeros((16, 128), F32)], []
    short = jnp.ones((16, 128), F32)
    for s in range(8):
        alpha, beta = alphas[-1], betas[-1]
        g_first = jnp.where(unit == s, 1.0, 0.0)
        g_last = jnp.where(unit == 8 + s, 1.0, 0.0)
        lf, ll, uf, ul = (spread(v, s) for v in (low_first, low_last, up_first, up_last))
        sf, sl = spread(source_first, s), spread(source_last, s)
        den = 1.0 / (sf + uf + short * lf)
        dens.append(den)
        alphas.append(g_last + ll * (alpha + beta * den * (g_first + lf * alpha)))
        betas.append(ul + ll * beta * den * uf)
        short = sl + ll * (short + beta * den * (sf + lf * short))
    above = jnp.zeros((16, 128), F32)
    for s in range(7, -1, -1):
        alpha, beta = alphas[s], betas[s]
        above_mat[:, s, :] = above
        lf, uf = spread(low_first, s), spread(up_first, s)
        g_first = jnp.where(unit == s, 1.0, 0.0)
        above = dens[s] * (g_first + lf * alpha + uf * above)
        below_mat[:, s, :] = alpha + beta * above
    finish_with = functools.partial(store_field, v_ref)
    for i in range(HALF):
        load = (lambda t: r0[t]) if i == 0 else (lambda t, i=i: w_ref[i - 1, t])
        value = (lambda t0, g: g) if i == 0 else (lambda t0, g: g * SCALE)
        line_solve(load, lines, below_mat, above_mat, y_buf, g_buf, finish_with(i, vp, ve, vw)(value))
        operate(v_ref, i, w_ref, coef, fold, vp, ve, vw)
    lefts = [at(v_ref, i) for i in range(HALF)]
    rights = [at(w_ref, j) for j in range(HALF)] + [at(r0)]
    gram_row(lefts, rights, gram_pairs(HALF), False, highs, lows, gram)


def second_body(sums, coef, lines, below_mat, above_mat, fold, r0, v1, w1, r_ref, y_out, v_ref, w_ref, gram, y_buf, g_buf, vp, ve, vw, highs, lows):
    y, ratio = small_solve(*sum_rows(sums[...]), HALF)
    y_out[...] = y
    bound = ratio * (2.0 / SCALE)
    step = 2.0 / bound
    weights = [jnp.broadcast_to(y[i : i + 1, :], (8, 128)) for i in range(HALF)]

    def renew(t, _):
        r = r0[t]
        for i in range(HALF):
            r = r - weights[i] * w1[i, t]
        r_ref[t] = r
        return 0

    lax.fori_loop(0, STEPS, renew, 0, unroll=4)
    finish_with = functools.partial(store_field, v_ref)
    for i in range(HALF):
        load = (lambda t: r_ref[t]) if i == 0 else (lambda t, i=i: w_ref[i - 1, t])
        if i == 0:
            value = lambda t0, g: g
        elif i == 1:
            value = lambda t0, g: v_ref[0, pl.ds(t0, 8)] - step * g
        else:
            value = lambda t0, g, i=i: 2.0 * (v_ref[i - 1, pl.ds(t0, 8)] - step * g) - v_ref[i - 2, pl.ds(t0, 8)]
        line_solve(load, lines, below_mat, above_mat, y_buf, g_buf, finish_with(i, vp, ve, vw)(value))
        operate(v_ref, i, w_ref, coef, fold, vp, ve, vw)
    lefts = [at(ref, i) for ref in (v1, v_ref) for i in range(HALF)]
    rights = [at(ref, j) for ref in (w1, w_ref) for j in range(HALF)] + [at(r_ref)]
    gram_row(lefts, rights, gram_pairs(TOTAL), True, highs, lows, gram)


def last_body(sums, y1, r_ref, v1, w1, v2, w2, out, x_rows, r_rows):
    y, _ = small_solve(*sum_rows(sums[...]), TOTAL)
    w_weights = [jnp.broadcast_to(y[i : i + 1, :], (8, 128)) for i in range(TOTAL)]
    v_weights = [w + (y1[i : i + 1, :] if i < HALF else 0.0) for i, w in enumerate(w_weights)]
    for t in range(STEPS):
        x = jnp.zeros((8, 128), F32)
        r = r_ref[t]
        for i in range(HALF):
            x = x + v_weights[i] * v1[i, t]
            r = r - w_weights[i] * w1[i, t]
        for i in range(HALF):
            x = x + v_weights[HALF + i] * v2[i, t]
            r = r - w_weights[HALF + i] * w2[i, t]
        x_rows[pl.ds(t, 8, stride=STEPS), :] = x
        r_rows[pl.ds(t, 8, stride=STEPS), :] = r
    for place, rows in enumerate((x_rows, r_rows)):
        for part in range(4):
            out[part, place] = rows[128 * part : 128 * part + 128, :].T[GHOST : GHOST + OWN, :]


def unpack_body(recv, x, r):
    for place, ref in enumerate((x, r)):
        ref[...] = jnp.concatenate([recv[part, place] for part in range(4)], axis=0).T


def shape(*dims):
    return jax.ShapeDtypeStruct(dims, F32)


def vmem(*dims):
    return pltpu.VMEM(dims, F32)


FIELD = (STEPS, 8, 128)
SCRATCH = [vmem(*FIELD), vmem(*FIELD), vmem(STEPS + 2, 8, 128), vmem(STEPS + 2, 8, 128), vmem(STEPS + 2, 8, 128), vmem(1024, 128), vmem(1024, 128)]


def all_sums(gram):
    return lax.all_to_all(gram, ("lat", *LON), split_axis=0, concat_axis=0, tiled=True)


def ring(block, step):
    return lax.ppermute(block, LON, [(d, (d + step) % 64) for d in range(64)])


def reflect(block, half):
    def branch(q):
        return lambda b: lax.ppermute(b, LON, [(d, (2 * q - d) % 64) for d in range(64)])

    return lax.switch(half, [branch(q) for q in range(32)], block)


def strips(block, odd):
    def even_branch(b):
        return ring(b[:, COLS - SIDE :], -1), b, ring(b[:, :SIDE], 1)

    def odd_branch(b):
        return b[:, COLS - SIDE :], ring(b, 1), ring(b[:, :SIDE], 2)

    return lax.cond(odd == 0, even_branch, odd_branch, block)


def shards(right_side, surface_term, east, north, neast, nwest, land_sea, fold_map):
    lat = lax.axis_index("lat").reshape(1)
    offset = (fold_map[0] + COLS * lax.axis_index(LON)) % NLON
    centre = ((offset - COLS // 2) % NLON) // COLS
    shift = (offset - COLS // 2) % COLS + COLS // 2
    smem = pl.BlockSpec(memory_space=pltpu.SMEM)
    whole = pl.BlockSpec(memory_space=pltpu.VMEM)
    packed, *chunks = pl.pallas_call(
        pack_body,
        in_specs=[smem] + [whole] * 7,
        out_shape=(shape(7, COLS, 128),) + (shape(7, OWN, 128),) * 4,
        name="pack",
    )(lat, right_side, surface_term, east, north, neast, nwest, land_sea)
    for step in range(1, 4):
        chunks[step] = lax.ppermute(chunks[step], "lat", [(i, (i + step) % 4) for i in range(4)])
    low, main, high = strips(reflect(packed, centre // 2), centre % 2)
    where = [64 * (k % 4) + k // 4 for k in range(256)]
    lefts = jnp.stack([c[:, OWN - GHOST :] for c in chunks])
    rights = jnp.stack([c[:, :GHOST] for c in chunks])
    lefts = lax.ppermute(lefts, ("lat", *LON), [(where[k], where[(k + 1) % 256]) for k in range(256)])
    rights = lax.ppermute(rights, ("lat", *LON), [(where[k], where[k - 1]) for k in range(256)])
    windows = pl.pallas_call(
        select_body,
        in_specs=[smem] + [whole] * 3,
        out_shape=shape(4, 7, WIDE, 128),
        name="select",
        compiler_params=params(),
    )(shift.reshape(1), low, main, high)
    facing = lax.all_to_all(windows, "lat", split_axis=0, concat_axis=0, tiled=True)
    coef, lines, below_mat, above_mat, fold, r0, v1, w1, gram = pl.pallas_call(
        first_body,
        out_shape=(
            shape(9, *FIELD),
            shape(4, STEPS + 8, 8, 128),
            shape(16, 8, 128),
            shape(16, 8, 128),
            shape(8, 128),
            shape(*FIELD),
            shape(HALF, *FIELD),
            shape(HALF, *FIELD),
            shape(512, 128),
        ),
        scratch_shapes=[vmem(7, 512, 128), vmem(7, STEPS + 2, 8, 128), *SCRATCH],
        in_specs=[smem] + [whole] * 7,
        name="phase_one",
        compiler_params=params(),
    )(lat, *chunks, lefts, rights, facing)
    sums = all_sums(gram)
    r4, y1, v2, w2, gram = pl.pallas_call(
        second_body,
        out_shape=(
            shape(*FIELD),
            shape(8, 128),
            shape(HALF, *FIELD),
            shape(HALF, *FIELD),
            shape(512, 128),
        ),
        scratch_shapes=SCRATCH,
        name="phase_two",
        compiler_params=params(),
    )(sums, coef, lines, below_mat, above_mat, fold, r0, v1, w1)
    sums = all_sums(gram)
    pieces = pl.pallas_call(
        last_body,
        out_shape=shape(4, 2, OWN, 128),
        scratch_shapes=[vmem(512, 128), vmem(512, 128)],
        name="combine",
        compiler_params=params(),
    )(sums, y1, r4, v1, w1, v2, w2)
    columns = lax.all_to_all(pieces, "lat", split_axis=0, concat_axis=0, tiled=True)
    return pl.pallas_call(unpack_body, out_shape=(shape(128, COLS), shape(128, COLS)), name="unpack")(columns)


def solution(mesh):
    finer = Mesh(mesh.devices.reshape(mesh.shape["lat"], 4, 8, 2), ("lat", *LON))
    field = P("lat", LON)
    return jax.shard_map(
        shards,
        mesh=finer,
        in_specs=(field,) * 7 + (P(LON),),
        out_specs=(field, field),
        check_vma=False,
    )
```

```python
import functools

import jax
import jax.numpy as jnp
from jax import lax
from jax.experimental import pallas as pl
from jax.experimental.pallas import tpu as pltpu
from jax.sharding import Mesh
from jax.sharding import PartitionSpec as P

LON = ("x", "z", "core")
NLON = 8192
COLS = 128
OWN = 32
GHOST = 8
WIDE = OWN + 2 * GHOST
PAD = COLS + 2 * GHOST
STEPS = 64
HALF = 4
TOTAL = 2 * HALF
SCALE = 1.0e-4
F32 = jnp.float32
HIGHEST = lax.Precision.HIGHEST
E, W, N, S, NE, SW, NW, SE, DIAG = range(9)
MULT, IPIV, LOWER, UPPER = range(4)


SIDE = 72


def params(mib=24):
    return pltpu.CompilerParams(vmem_limit_bytes=mib * 1024 * 1024)


def two_sum(a, b):
    s = a + b
    bb = s - a
    return s, (a - (s - bb)) + (b - bb)


def split(a):
    t = a * 4097.0
    hi = t - (t - a)
    return hi, a - hi


def two_prod(a, b):
    p = a * b
    ah, al = split(a)
    bh, bl = split(b)
    return p, ((ah * bh - p) + ah * bl + al * bh) + al * bl


def renorm(s, e):
    hi = s + e
    return hi, e - (hi - s)


def pair_sub(a, b):
    s, e = two_sum(a[0], -b[0])
    return renorm(s, e + (a[1] - b[1]))


def pair_mul(a, b):
    p, e = two_prod(a[0], b[0])
    return renorm(p, e + (a[0] * b[1] + a[1] * b[0]))


def pair_div(a, b):
    first = a[0] / b[0]
    zero = jnp.zeros_like(first)
    rest = pair_sub(a, pair_mul((first, zero), b))
    return renorm(first, rest[0] / b[0])


def sum_rows(values):
    s = values[0:8]
    e = jnp.zeros_like(s)
    for start in range(8, values.shape[0], 8):
        s, err = two_sum(s, values[start : start + 8])
        e = e + err
    for shift in (4, 2, 1):
        s_other = pltpu.roll(s, shift, 0)
        e_other = pltpu.roll(e, shift, 0)
        s, err = two_sum(s, s_other)
        e = e + e_other + err
    hi, lo = renorm(s, e)
    return hi[0:1], lo[0:1]


def small_solve(hi_row, lo_row, order):
    row = lax.broadcasted_iota(jnp.int32, (8, 128), 0)
    lane = lax.broadcasted_iota(jnp.int32, (8, 128), 1)

    def matrix(values):
        wide = jnp.broadcast_to(values, (8, 128))
        out = jnp.zeros((8, 128), F32)
        for i in range(order):
            turned = wide if i == 0 else pltpu.roll(wide, 128 - 16 * i, 1)
            out = jnp.where(row == i, turned, out)
        return jnp.where(lane < 16, out, 0.0)

    hi, lo = matrix(hi_row), matrix(lo_row)
    ratio = hi[3:4, 3:4] / hi[3:4, 2:3]
    start = jnp.sum(jnp.where(row == lane, hi, 0.0), axis=1, keepdims=True)
    live = jnp.ones((8, 128), F32)
    for k in range(order):
        col = tuple(jnp.broadcast_to(v[:, k : k + 1], (8, 128)) for v in (hi, lo))
        piv_row = tuple(jnp.broadcast_to(v[k : k + 1, :], (8, 128)) for v in (hi, lo))
        piv = tuple(jnp.broadcast_to(v[k : k + 1, k : k + 1], (8, 128)) for v in (hi, lo))
        good = piv[0] > 1e-11 * jnp.broadcast_to(start[k : k + 1, :], (8, 128))
        piv = (jnp.where(good, piv[0], 1.0), jnp.where(good, piv[1], 0.0))
        factor = pair_div(col, piv)
        new = pair_sub((hi, lo), pair_mul(factor, piv_row))
        change = good & (row != k)
        hi = jnp.where(change, new[0], hi)
        lo = jnp.where(change, new[1], lo)
        live = jnp.where((row == k) & ~good, 0.0, live)
    diag = jnp.sum(jnp.where(row == lane, hi, 0.0), axis=1, keepdims=True)
    diag = jnp.where((diag != 0.0) & (live[:, 0:1] > 0.0), diag, 1.0)
    y = jnp.broadcast_to(hi[:, 8:9] / diag, (8, 128)) * live
    y = jnp.where(row < order, y, 0.0)
    return y, jnp.broadcast_to(ratio, (8, 128))


def pack_body(place, rhs, surface, east, north, neast, nwest, land, out, *chunks):
    for k, ref in enumerate((rhs, surface, east, north, neast, nwest)):
        out[k] = ref[...].T
    out[6] = land[...].astype(F32).T
    for step, chunk in enumerate(chunks):
        start = pl.multiple_of(OWN * ((place[0] + step) & 3), OWN)
        chunk[...] = out[:, pl.ds(start, OWN), :]


def select_body(shift, low, main, high, out):
    i = lax.broadcasted_iota(jnp.int32, (PAD, COLS + 2 * SIDE), 0)
    u = lax.broadcasted_iota(jnp.int32, (PAD, COLS + 2 * SIDE), 1)
    reach = shift[0] + GHOST + SIDE
    plain = jnp.where(u == reach - i, 1.0, 0.0)
    moved = jnp.where(u == reach - 1 - i, 1.0, 0.0)
    for place, source in enumerate((0, 1, 2, 3, 5, 4, 6)):
        both = jnp.concatenate([low[source], main[source], high[source]], axis=0)
        facing = jnp.dot(moved if source == 2 else plain, both, precision=HIGHEST, preferred_element_type=F32)
        for part in range(4):
            out[part, place] = facing[OWN * part : OWN * part + WIDE, :]


def east_of(v):
    return pltpu.roll(v, 127, v.ndim - 1)


def west_of(v):
    return pltpu.roll(v, 1, v.ndim - 1)


def facing_of(v):
    return pltpu.roll(v, 64, v.ndim - 1)


def row_before(v):
    s = lax.broadcasted_iota(jnp.int32, (8, 128), 0)
    return jnp.where(s == 0, 0.0, pltpu.roll(v, 1, 0))


def row_after(v):
    s = lax.broadcasted_iota(jnp.int32, (8, 128), 0)
    return jnp.where(s == 7, 0.0, pltpu.roll(v, 7, 0))


def line_solve(load, lines, below_mat, above_mat, y_buf, g_buf, finish):
    zero = jnp.zeros((8, 128), F32)

    def forward(t, y):
        y = load(t) + lines[MULT, t] * y
        y_buf[t] = y
        return y

    lax.fori_loop(0, STEPS, forward, zero, unroll=8)

    def backward(k, x):
        t = STEPS - 1 - k
        x = y_buf[t] * lines[IPIV, t] + lines[MULT, t + 1] * x
        g_buf[t] = x
        return x

    lax.fori_loop(0, STEPS, backward, zero, unroll=8)
    first, last = g_buf[0], g_buf[STEPS - 1]
    below, above = zero, zero
    for k in range(8):
        for base, ends in ((0, first), (8, last)):
            end = jnp.broadcast_to(ends[k : k + 1, :], (8, 128))
            below = below + below_mat[base + k] * end
            above = above + above_mat[base + k] * end

    def combine(c, _):
        t0 = c * 8
        g = g_buf[pl.ds(t0, 8)] + lines[LOWER, pl.ds(t0, 8)] * below + lines[UPPER, pl.ds(t0, 8)] * above
        finish(t0, g)
        return 0

    lax.fori_loop(0, STEPS // 8, combine, 0, unroll=2)


def operate(v_ref, place, w_ref, coef, fold, vp, ve, vw):
    for t, v in ((0, row_before(v_ref[place, STEPS - 1])), (STEPS + 1, row_after(v_ref[place, 0]))):
        vp[t] = v
        ve[t] = east_of(v)
        vw[t] = west_of(v)

    def step(c, _):
        t = c * 4
        here, up, down = pl.ds(t + 1, 4), pl.ds(t + 2, 4), pl.ds(t, 4)
        at = pl.ds(t, 4)
        out = coef[DIAG, at] * vp[here]
        side = coef[E, at] * ve[here] + coef[W, at] * vw[here]
        north = coef[N, at] * vp[up] + coef[NE, at] * ve[up] + coef[NW, at] * vw[up]
        south = coef[S, at] * vp[down] + coef[SW, at] * vw[down] + coef[SE, at] * ve[down]
        w_ref[place, at] = out - (side + north + south)
        return 0

    lax.fori_loop(0, STEPS // 4, step, 0, unroll=2)
    w_ref[place, STEPS - 1] = w_ref[place, STEPS - 1] - fold[...] * facing_of(v_ref[place, STEPS - 1])


def store_field(v_ref, place, vp, ve, vw):
    def finish_with(value_of):
        def finish(t0, g):
            v = value_of(t0, g)
            v_ref[place, pl.ds(t0, 8)] = v
            vp[pl.ds(t0 + 1, 8)] = v
            ve[pl.ds(t0 + 1, 8)] = east_of(v)
            vw[pl.ds(t0 + 1, 8)] = west_of(v)

        return finish

    return finish_with


def gram_row(lefts, rights, pairs, exact, highs, lows, out):
    highs[...] = jnp.zeros(highs.shape, F32)
    lows[...] = jnp.zeros(lows.shape, F32)
    start = 0
    while start < len(pairs):
        end = start
        while end < len(pairs) and (pairs[end][0] == pairs[start][0] or end - start < 12) and end - start < 17:
            end += 1
        part = pairs[start:end]
        start = end

        def add(t, sums, part=part):
            left = {i: lefts[i](t) for i in sorted({i for i, _, _ in part})}
            right = {j: rights[j](t) for j in sorted({j for _, j, _ in part})}
            if not exact:
                return tuple((s + left[i] * right[j], e) for (s, e), (i, j, _) in zip(sums, part))
            left_halves = {i: split(v) for i, v in left.items()}
            right_halves = {j: split(v) for j, v in right.items()}
            out = []
            for (s, e), (i, j, _) in zip(sums, part):
                ah, al = left_halves[i]
                bh, bl = right_halves[j]
                s, err = two_sum(s, ah * bh)
                out.append((s, e + (err + (ah * bl + al * right[j]))))
            return tuple(out)

        zero = jnp.zeros((8, 128), F32)
        sums = lax.fori_loop(0, STEPS, add, tuple((zero, zero) for _ in part), unroll=1 if exact else 2)
        for (s, e), (_, _, lanes) in zip(sums, part):
            for lane in lanes:
                highs[pl.ds(lane, 8, stride=128), :] = s
                lows[pl.ds(lane, 8, stride=128), :] = e
    s, e = highs[0:128], lows[0:128]
    for k in range(1, 8):
        s, err = two_sum(s, highs[128 * k : 128 * k + 128])
        e = e + (err + lows[128 * k : 128 * k + 128])
    s, e = s.T, e.T
    hi, lo = sum_rows(jnp.concatenate([s[GHOST : GHOST + OWN], e[GHOST : GHOST + OWN]], axis=0))
    row = lax.broadcasted_iota(jnp.int32, (8, 128), 0)
    both = jnp.where((row & 1) == 0, jnp.broadcast_to(hi, (8, 128)), jnp.broadcast_to(lo, (8, 128)))
    out[...] = jnp.concatenate([both] * (out.shape[0] // 8), axis=0)


def gram_pairs(count):
    out = []
    for i in range(count):
        out += [(i, j, sorted({16 * i + j, 16 * j + i})) for j in range(i, count)]
        out.append((i, count, [16 * i + 8]))
    return out


def at(ref, *index):
    return lambda t: ref[(*index, t)]


def first_body(lat, c0, c1, c2, c3, lefts, rights, facing, coef, lines, below_mat, above_mat, fold, r0, v_ref, w_ref, gram, raw, grid, y_buf, g_buf, vp, ve, vw, highs, lows):
    s_id = lax.broadcasted_iota(jnp.int32, (8, 128), 0)
    zero = jnp.zeros((8, 128), F32)
    gap = jnp.zeros((64 - WIDE, 128), F32)
    for place in range(7):
        for step, chunk in enumerate((c0, c1, c2, c3)):
            source = (lat[0] - step) & 3
            left, right = lefts[(step - 1) % 4, place], rights[(step + 1) % 4, place]
            full = jnp.concatenate([left, chunk[place], right, gap, facing[source, place], gap], axis=0)
            raw[place, pl.ds(pl.multiple_of(128 * source, 128), 128), :] = full.T
        for t in range(STEPS):
            grid[place, t + 1] = raw[place, pl.ds(t, 8, stride=STEPS), :]
    top_north = grid[3, STEPS]
    top_ocean = grid[6, STEPS]
    last = s_id == 7
    fold_open = jnp.where(last, 0.5 * (top_north + facing_of(top_north)), 0.0)
    fold[...] = fold_open * top_ocean * facing_of(top_ocean)
    for place in (3, 4, 5):
        grid[place, STEPS] = jnp.where(last, 0.0, grid[place, STEPS])
    for place in (3, 4, 5, 6):
        grid[place, 0] = row_before(grid[place, STEPS])
        grid[place, STEPS + 1] = row_after(grid[place, 1])

    def weigh(t, _):
        o, o_up, o_down = grid[6, t + 1], grid[6, t + 2], grid[6, t]
        east = grid[2, t + 1]
        north, neast, nwest = grid[3, t + 1], grid[4, t + 1], grid[5, t + 1]
        south, s_neast, s_nwest = grid[3, t], grid[4, t], grid[5, t]
        open_sum = zero
        parts = (
            (E, east, east_of(o)),
            (W, west_of(east), west_of(o)),
            (N, north, o_up),
            (S, south, o_down),
            (NE, neast, east_of(o_up)),
            (SW, west_of(s_neast), west_of(o_down)),
            (NW, nwest, west_of(o_up)),
            (SE, east_of(s_nwest), east_of(o_down)),
        )
        for place, edge, other in parts:
            coef[place, t] = edge * o * other
            open_sum = open_sum + edge
        surface = grid[1, t + 1]
        coef[DIAG, t] = o * (surface + open_sum) + (1.0 - o)
        r0[t] = o * grid[0, t + 1]
        vw[t] = o * (surface + coef[N, t] + coef[S, t]) + (1.0 - o)
        return 0

    lax.fori_loop(0, STEPS, weigh, 0, unroll=2)
    surface = grid[1, STEPS]
    o = top_ocean
    coef[DIAG, STEPS - 1] = coef[DIAG, STEPS - 1] + o * fold_open

    def eliminate(t, carry):
        ratio, beyond = carry
        north = coef[N, t]
        pivot = vw[t] - coef[S, t] * ratio
        more, err = two_sum(pivot, -north)
        more = more + err
        y_buf[t] = more - ratio * beyond
        guess = north / pivot
        prod, err = two_prod(guess, pivot)
        return guess + ((north - prod) - err) / pivot, more

    ends = lax.fori_loop(0, STEPS, eliminate, (zero, zero), unroll=2)
    lax.fori_loop(0, STEPS, eliminate, tuple(row_before(v) for v in ends), unroll=2)

    def pivots(t, carry):
        before, beyond, response, source = carry
        rest = y_buf[t]
        mult = jnp.where(t == 0, zero, coef[S, t] * before)
        beyond = rest + jnp.where(t == 0, coef[S, 0], mult * beyond)
        inverse = 1.0 / (coef[N, t] + beyond)
        lines[MULT, t] = mult
        lines[IPIV, t] = inverse
        response = jnp.where(t == 0, coef[S, 0], mult * response)
        source = rest + mult * source
        g_buf[t] = response
        vp[t] = source
        return inverse, beyond, response, source

    lax.fori_loop(0, STEPS, pivots, (zero,) * 4, unroll=4)
    for t in range(STEPS, lines.shape[1]):
        lines[MULT, t] = zero

    def respond(k, carry):
        low, up, source = carry
        t = STEPS - 1 - k
        factor = lines[MULT, t + 1]
        inverse = lines[IPIV, t]
        low = g_buf[t] * inverse + factor * low
        up = jnp.where(k == 0, coef[N, STEPS - 1] * inverse, factor * up)
        source = vp[t] * inverse + factor * source
        lines[LOWER, t] = low
        lines[UPPER, t] = up
        ve[t] = source
        return low, up, source

    lax.fori_loop(0, STEPS, respond, (zero,) * 3, unroll=4)
    unit = lax.broadcasted_iota(jnp.int32, (16, 128), 0)
    low_first, low_last = lines[LOWER, 0], lines[LOWER, STEPS - 1]
    up_first, up_last = lines[UPPER, 0], lines[UPPER, STEPS - 1]

    def spread(v, s):
        return jnp.broadcast_to(v[s : s + 1, :], (16, 128))

    source_first, source_last = ve[0], ve[STEPS - 1]
    alphas, betas, dens = [jnp.zeros((16, 128), F32)], [jnp.zeros((16, 128), F32)], []
    short = jnp.ones((16, 128), F32)
    for s in range(8):
        alpha, beta = alphas[-1], betas[-1]
        g_first = jnp.where(unit == s, 1.0, 0.0)
        g_last = jnp.where(unit == 8 + s, 1.0, 0.0)
        lf, ll, uf, ul = (spread(v, s) for v in (low_first, low_last, up_first, up_last))
        sf, sl = spread(source_first, s), spread(source_last, s)
        den = 1.0 / (sf + uf + short * lf)
        dens.append(den)
        alphas.append(g_last + ll * (alpha + beta * den * (g_first + lf * alpha)))
        betas.append(ul + ll * beta * den * uf)
        short = sl + ll * (short + beta * den * (sf + lf * short))
    above = jnp.zeros((16, 128), F32)
    for s in range(7, -1, -1):
        alpha, beta = alphas[s], betas[s]
        above_mat[:, s, :] = above
        lf, uf = spread(low_first, s), spread(up_first, s)
        g_first = jnp.where(unit == s, 1.0, 0.0)
        above = dens[s] * (g_first + lf * alpha + uf * above)
        below_mat[:, s, :] = alpha + beta * above
    finish_with = functools.partial(store_field, v_ref)
    for i in range(HALF):
        load = (lambda t: r0[t]) if i == 0 else (lambda t, i=i: w_ref[i - 1, t])
        value = (lambda t0, g: g) if i == 0 else (lambda t0, g: g * SCALE)
        line_solve(load, lines, below_mat, above_mat, y_buf, g_buf, finish_with(i, vp, ve, vw)(value))
        operate(v_ref, i, w_ref, coef, fold, vp, ve, vw)
    lefts = [at(v_ref, i) for i in range(HALF)]
    rights = [at(w_ref, j) for j in range(HALF)] + [at(r0)]
    gram_row(lefts, rights, gram_pairs(HALF), False, highs, lows, gram)


def second_body(sums, coef, lines, below_mat, above_mat, fold, r0, v1, w1, r_ref, y_out, v_ref, w_ref, gram, y_buf, g_buf, vp, ve, vw, highs, lows):
    y, ratio = small_solve(*sum_rows(sums[...]), HALF)
    y_out[...] = y
    bound = ratio * (2.0 / SCALE)
    step = 2.0 / bound
    weights = [jnp.broadcast_to(y[i : i + 1, :], (8, 128)) for i in range(HALF)]

    def renew(t, _):
        r = r0[t]
        for i in range(HALF):
            r = r - weights[i] * w1[i, t]
        r_ref[t] = r
        return 0

    lax.fori_loop(0, STEPS, renew, 0, unroll=4)
    finish_with = functools.partial(store_field, v_ref)
    for i in range(HALF):
        load = (lambda t: r_ref[t]) if i == 0 else (lambda t, i=i: w_ref[i - 1, t])
        if i == 0:
            value = lambda t0, g: g
        elif i == 1:
            value = lambda t0, g: v_ref[0, pl.ds(t0, 8)] - step * g
        else:
            value = lambda t0, g, i=i: 2.0 * (v_ref[i - 1, pl.ds(t0, 8)] - step * g) - v_ref[i - 2, pl.ds(t0, 8)]
        line_solve(load, lines, below_mat, above_mat, y_buf, g_buf, finish_with(i, vp, ve, vw)(value))
        operate(v_ref, i, w_ref, coef, fold, vp, ve, vw)
    lefts = [at(ref, i) for ref in (v1, v_ref) for i in range(HALF)]
    rights = [at(ref, j) for ref in (w1, w_ref) for j in range(HALF)] + [at(r_ref)]
    gram_row(lefts, rights, gram_pairs(TOTAL), True, highs, lows, gram)


def last_body(sums, y1, r_ref, v1, w1, v2, w2, out, x_rows, r_rows):
    y, _ = small_solve(*sum_rows(sums[...]), TOTAL)
    w_weights = [jnp.broadcast_to(y[i : i + 1, :], (8, 128)) for i in range(TOTAL)]
    v_weights = [w + (y1[i : i + 1, :] if i < HALF else 0.0) for i, w in enumerate(w_weights)]
    for t in range(STEPS):
        x = jnp.zeros((8, 128), F32)
        r = r_ref[t]
        for i in range(HALF):
            x = x + v_weights[i] * v1[i, t]
            r = r - w_weights[i] * w1[i, t]
        for i in range(HALF):
            x = x + v_weights[HALF + i] * v2[i, t]
            r = r - w_weights[HALF + i] * w2[i, t]
        x_rows[pl.ds(t, 8, stride=STEPS), :] = x
        r_rows[pl.ds(t, 8, stride=STEPS), :] = r
    for place, rows in enumerate((x_rows, r_rows)):
        for part in range(4):
            out[part, place] = rows[128 * part : 128 * part + 128, :].T[GHOST : GHOST + OWN, :]


def unpack_body(recv, x, r):
    for place, ref in enumerate((x, r)):
        ref[...] = jnp.concatenate([recv[part, place] for part in range(4)], axis=0).T


def shape(*dims):
    return jax.ShapeDtypeStruct(dims, F32)


def vmem(*dims):
    return pltpu.VMEM(dims, F32)


FIELD = (STEPS, 8, 128)
SCRATCH = [vmem(*FIELD), vmem(*FIELD), vmem(STEPS + 2, 8, 128), vmem(STEPS + 2, 8, 128), vmem(STEPS + 2, 8, 128), vmem(1024, 128), vmem(1024, 128)]


def all_sums(gram):
    return lax.all_to_all(gram, ("lat", *LON), split_axis=0, concat_axis=0, tiled=True)


def ring(block, step):
    return lax.ppermute(block, LON, [(d, (d + step) % 64) for d in range(64)])


def reflect(block, quarter):
    def branch(q):
        return lambda b: lax.ppermute(b, LON, [(d, (4 * q - d) % 64) for d in range(64)])

    return lax.switch(quarter, [branch(q) for q in range(16)], block)


def strips(block, step):
    def branch(p):
        def moved(b, by):
            return ring(b, by) if by else b

        return lambda b: (moved(b[:, COLS - SIDE :], p - 1), moved(b, p), moved(b[:, :SIDE], p + 1))

    return lax.switch(step, [branch(p) for p in (-1, 0, 1, 2)], block)


def shards(right_side, surface_term, east, north, neast, nwest, land_sea, fold_map):
    lat = lax.axis_index("lat").reshape(1)
    offset = (fold_map[0] + COLS * lax.axis_index(LON)) % NLON
    centre = ((offset - COLS // 2) % NLON) // COLS
    shift = (offset - COLS // 2) % COLS + COLS // 2
    smem = pl.BlockSpec(memory_space=pltpu.SMEM)
    whole = pl.BlockSpec(memory_space=pltpu.VMEM)
    packed, *chunks = pl.pallas_call(
        pack_body,
        in_specs=[smem] + [whole] * 7,
        out_shape=(shape(7, COLS, 128),) + (shape(7, OWN, 128),) * 4,
        name="pack",
    )(lat, right_side, surface_term, east, north, neast, nwest, land_sea)
    for step in range(1, 4):
        chunks[step] = lax.ppermute(chunks[step], "lat", [(i, (i + step) % 4) for i in range(4)])
    ahead = (centre + 1) % 64
    low, main, high = strips(reflect(packed, ahead // 4), ahead % 4)
    where = [64 * (k % 4) + k // 4 for k in range(256)]
    lefts = jnp.stack([c[:, OWN - GHOST :] for c in chunks])
    rights = jnp.stack([c[:, :GHOST] for c in chunks])
    lefts = lax.ppermute(lefts, ("lat", *LON), [(where[k], where[(k + 1) % 256]) for k in range(256)])
    rights = lax.ppermute(rights, ("lat", *LON), [(where[k], where[k - 1]) for k in range(256)])
    windows = pl.pallas_call(
        select_body,
        in_specs=[smem] + [whole] * 3,
        out_shape=shape(4, 7, WIDE, 128),
        name="select",
        compiler_params=params(),
    )(shift.reshape(1), low, main, high)
    facing = lax.all_to_all(windows, "lat", split_axis=0, concat_axis=0, tiled=True)
    coef, lines, below_mat, above_mat, fold, r0, v1, w1, gram = pl.pallas_call(
        first_body,
        out_shape=(
            shape(9, *FIELD),
            shape(4, STEPS + 8, 8, 128),
            shape(16, 8, 128),
            shape(16, 8, 128),
            shape(8, 128),
            shape(*FIELD),
            shape(HALF, *FIELD),
            shape(HALF, *FIELD),
            shape(512, 128),
        ),
        scratch_shapes=[vmem(7, 512, 128), vmem(7, STEPS + 2, 8, 128), *SCRATCH],
        in_specs=[smem] + [whole] * 7,
        name="phase_one",
        compiler_params=params(),
    )(lat, *chunks, lefts, rights, facing)
    sums = all_sums(gram)
    r4, y1, v2, w2, gram = pl.pallas_call(
        second_body,
        out_shape=(
            shape(*FIELD),
            shape(8, 128),
            shape(HALF, *FIELD),
            shape(HALF, *FIELD),
            shape(512, 128),
        ),
        scratch_shapes=SCRATCH,
        name="phase_two",
        compiler_params=params(),
    )(sums, coef, lines, below_mat, above_mat, fold, r0, v1, w1)
    sums = all_sums(gram)
    pieces = pl.pallas_call(
        last_body,
        out_shape=shape(4, 2, OWN, 128),
        scratch_shapes=[vmem(512, 128), vmem(512, 128)],
        name="combine",
        compiler_params=params(),
    )(sums, y1, r4, v1, w1, v2, w2)
    columns = lax.all_to_all(pieces, "lat", split_axis=0, concat_axis=0, tiled=True)
    return pl.pallas_call(unpack_body, out_shape=(shape(128, COLS), shape(128, COLS)), name="unpack")(columns)


def solution(mesh):
    finer = Mesh(mesh.devices.reshape(mesh.shape["lat"], 4, 8, 2), ("lat", *LON))
    field = P("lat", LON)
    return jax.shard_map(
        shards,
        mesh=finer,
        in_specs=(field,) * 7 + (P(LON),),
        out_specs=(field, field),
        check_vma=False,
    )
```

```python
import functools

import jax
import jax.numpy as jnp
from jax import lax
from jax.experimental import pallas as pl
from jax.experimental.pallas import tpu as pltpu
from jax.sharding import Mesh
from jax.sharding import PartitionSpec as P


LON = ("x", "z", "core")
NLON = 8192
COLS = 128
OWN = 32
GHOST = 8
WIDE = OWN + 2 * GHOST
PAD = COLS + 2 * GHOST
STEPS = 64
HALF = 4
TOTAL = 2 * HALF
SCALE = 1.0e-4
F32 = jnp.float32
E, W, N, S, NE, SW, NW, SE, DIAG = range(9)
MULT, IPIV, LOWER, UPPER = range(4)


SIDE = 72


def params(mib=24):
    return pltpu.CompilerParams(vmem_limit_bytes=mib * 1024 * 1024)


def two_sum(a, b):
    s = a + b
    bb = s - a
    return s, (a - (s - bb)) + (b - bb)


def split(a):
    t = a * 4097.0
    hi = t - (t - a)
    return hi, a - hi


def two_prod(a, b):
    p = a * b
    ah, al = split(a)
    bh, bl = split(b)
    return p, ((ah * bh - p) + ah * bl + al * bh) + al * bl


def renorm(s, e):
    hi = s + e
    return hi, e - (hi - s)


def pair_sub(a, b):
    s, e = two_sum(a[0], -b[0])
    return renorm(s, e + (a[1] - b[1]))


def pair_mul(a, b):
    p, e = two_prod(a[0], b[0])
    return renorm(p, e + (a[0] * b[1] + a[1] * b[0]))


def pair_div(a, b):
    first = a[0] / b[0]
    zero = jnp.zeros_like(first)
    rest = pair_sub(a, pair_mul((first, zero), b))
    return renorm(first, rest[0] / b[0])


def sum_rows(values):
    s = values[0:8]
    e = jnp.zeros_like(s)
    for start in range(8, values.shape[0], 8):
        s, err = two_sum(s, values[start : start + 8])
        e = e + err
    for shift in (4, 2, 1):
        s_other = pltpu.roll(s, shift, 0)
        e_other = pltpu.roll(e, shift, 0)
        s, err = two_sum(s, s_other)
        e = e + e_other + err
    hi, lo = renorm(s, e)
    return hi[0:1], lo[0:1]


def small_solve(hi_row, lo_row, order):
    row = lax.broadcasted_iota(jnp.int32, (8, 128), 0)
    lane = lax.broadcasted_iota(jnp.int32, (8, 128), 1)

    def matrix(values):
        wide = jnp.broadcast_to(values, (8, 128))
        out = jnp.zeros((8, 128), F32)
        for i in range(order):
            turned = wide if i == 0 else pltpu.roll(wide, 128 - 16 * i, 1)
            out = jnp.where(row == i, turned, out)
        return jnp.where(lane < 16, out, 0.0)

    hi, lo = matrix(hi_row), matrix(lo_row)
    ratio = hi[3:4, 3:4] / hi[3:4, 2:3]
    start = jnp.sum(jnp.where(row == lane, hi, 0.0), axis=1, keepdims=True)
    live = jnp.ones((8, 128), F32)
    for k in range(order):
        col = tuple(jnp.broadcast_to(v[:, k : k + 1], (8, 128)) for v in (hi, lo))
        piv_row = tuple(jnp.broadcast_to(v[k : k + 1, :], (8, 128)) for v in (hi, lo))
        piv = tuple(jnp.broadcast_to(v[k : k + 1, k : k + 1], (8, 128)) for v in (hi, lo))
        good = piv[0] > 1e-11 * jnp.broadcast_to(start[k : k + 1, :], (8, 128))
        piv = (jnp.where(good, piv[0], 1.0), jnp.where(good, piv[1], 0.0))
        factor = pair_div(col, piv)
        new = pair_sub((hi, lo), pair_mul(factor, piv_row))
        change = good & (row != k)
        hi = jnp.where(change, new[0], hi)
        lo = jnp.where(change, new[1], lo)
        live = jnp.where((row == k) & ~good, 0.0, live)
    diag = jnp.sum(jnp.where(row == lane, hi, 0.0), axis=1, keepdims=True)
    diag = jnp.where((diag != 0.0) & (live[:, 0:1] > 0.0), diag, 1.0)
    y = jnp.broadcast_to(hi[:, 8:9] / diag, (8, 128)) * live
    y = jnp.where(row < order, y, 0.0)
    return y, jnp.broadcast_to(ratio, (8, 128))


def pack_body(rhs, surface, east, north, neast, nwest, land, out):
    for k, ref in enumerate((rhs, surface, east, north, neast, nwest)):
        out[k] = ref[...].T
    out[6] = land[...].astype(F32).T


def window_body(before, packed, after, out):
    for place in range(7):
        wide = jnp.concatenate([before[place], packed[place], after[place]], axis=0)
        for part in range(4):
            out[part, place] = wide[OWN * part : OWN * part + WIDE, :]


def select_body(shift, low, main, high, out):
    i = lax.broadcasted_iota(jnp.int32, (PAD, COLS + 2 * SIDE), 0)
    u = lax.broadcasted_iota(jnp.int32, (PAD, COLS + 2 * SIDE), 1)
    reach = shift[0] + GHOST + SIDE
    plain = jnp.where(u == reach - i, 1.0, 0.0).astype(jnp.bfloat16)
    moved = jnp.where(u == reach - 1 - i, 1.0, 0.0).astype(jnp.bfloat16)

    def pick(choice, values):
        return jnp.dot(choice, values, preferred_element_type=F32)

    for place, source in enumerate((0, 1, 2, 3, 5, 4, 6)):
        both = jnp.concatenate([low[source], main[source], high[source]], axis=0)
        top = both.astype(jnp.bfloat16)
        rest = both - top.astype(F32)
        middle = rest.astype(jnp.bfloat16)
        bottom = (rest - middle.astype(F32)).astype(jnp.bfloat16)
        choice = moved if source == 2 else plain
        facing = (pick(choice, top) + pick(choice, middle)) + pick(choice, bottom)
        for part in range(4):
            out[part, place] = facing[OWN * part : OWN * part + WIDE, :]


def east_of(v):
    return pltpu.roll(v, 127, v.ndim - 1)


def west_of(v):
    return pltpu.roll(v, 1, v.ndim - 1)


def facing_of(v):
    return pltpu.roll(v, 64, v.ndim - 1)


def row_before(v):
    s = lax.broadcasted_iota(jnp.int32, (8, 128), 0)
    return jnp.where(s == 0, 0.0, pltpu.roll(v, 1, 0))


def row_after(v):
    s = lax.broadcasted_iota(jnp.int32, (8, 128), 0)
    return jnp.where(s == 7, 0.0, pltpu.roll(v, 7, 0))


def line_solve(load, lines, below_mat, above_mat, y_buf, g_buf, finish):
    zero = jnp.zeros((8, 128), F32)

    def forward(t, y):
        y = load(t) + lines[MULT, t] * y
        y_buf[t] = y
        return y

    lax.fori_loop(0, STEPS, forward, zero, unroll=8)

    def backward(k, x):
        t = STEPS - 1 - k
        x = y_buf[t] * lines[IPIV, t] + lines[MULT, t + 1] * x
        g_buf[t] = x
        return x

    lax.fori_loop(0, STEPS, backward, zero, unroll=8)
    first, last = g_buf[0], g_buf[STEPS - 1]
    below, above = zero, zero
    for k in range(8):
        for base, ends in ((0, first), (8, last)):
            end = jnp.broadcast_to(ends[k : k + 1, :], (8, 128))
            below = below + below_mat[base + k] * end
            above = above + above_mat[base + k] * end

    def combine(c, _):
        t0 = c * 8
        g = g_buf[pl.ds(t0, 8)] + lines[LOWER, pl.ds(t0, 8)] * below + lines[UPPER, pl.ds(t0, 8)] * above
        finish(t0, g)
        return 0

    lax.fori_loop(0, STEPS // 8, combine, 0, unroll=2)


def operate(v_ref, place, w_ref, coef, fold, vp, ve, vw):
    for t, v in ((0, row_before(v_ref[place, STEPS - 1])), (STEPS + 1, row_after(v_ref[place, 0]))):
        vp[t] = v
        ve[t] = east_of(v)
        vw[t] = west_of(v)

    def step(c, _):
        t = c * 4
        here, up, down = pl.ds(t + 1, 4), pl.ds(t + 2, 4), pl.ds(t, 4)
        at = pl.ds(t, 4)
        out = coef[DIAG, at] * vp[here]
        side = coef[E, at] * ve[here] + coef[W, at] * vw[here]
        north = coef[N, at] * vp[up] + coef[NE, at] * ve[up] + coef[NW, at] * vw[up]
        south = coef[S, at] * vp[down] + coef[SW, at] * vw[down] + coef[SE, at] * ve[down]
        w_ref[place, at] = out - (side + north + south)
        return 0

    lax.fori_loop(0, STEPS // 4, step, 0, unroll=2)
    w_ref[place, STEPS - 1] = w_ref[place, STEPS - 1] - fold[...] * facing_of(v_ref[place, STEPS - 1])


def store_field(v_ref, place, vp, ve, vw):
    def finish_with(value_of):
        def finish(t0, g):
            v = value_of(t0, g)
            v_ref[place, pl.ds(t0, 8)] = v
            vp[pl.ds(t0 + 1, 8)] = v
            ve[pl.ds(t0 + 1, 8)] = east_of(v)
            vw[pl.ds(t0 + 1, 8)] = west_of(v)

        return finish

    return finish_with


def gram_row(lefts, rights, pairs, exact, highs, lows, out):
    highs[...] = jnp.zeros(highs.shape, F32)
    lows[...] = jnp.zeros(lows.shape, F32)
    start = 0
    while start < len(pairs):
        end = start
        while end < len(pairs) and (pairs[end][0] == pairs[start][0] or end - start < 12) and end - start < 17:
            end += 1
        part = pairs[start:end]
        start = end

        def add(t, sums, part=part):
            left = {i: lefts[i](t) for i in sorted({i for i, _, _ in part})}
            right = {j: rights[j](t) for j in sorted({j for _, j, _ in part})}
            if not exact:
                return tuple((s + left[i] * right[j], e) for (s, e), (i, j, _) in zip(sums, part))
            left_halves = {i: split(v) for i, v in left.items()}
            right_halves = {j: split(v) for j, v in right.items()}
            out = []
            for (s, e), (i, j, _) in zip(sums, part):
                ah, al = left_halves[i]
                bh, bl = right_halves[j]
                s, err = two_sum(s, ah * bh)
                out.append((s, e + (err + (ah * bl + al * right[j]))))
            return tuple(out)

        zero = jnp.zeros((8, 128), F32)
        sums = lax.fori_loop(0, STEPS, add, tuple((zero, zero) for _ in part), unroll=1 if exact else 2)
        for (s, e), (_, _, lanes) in zip(sums, part):
            for lane in lanes:
                highs[pl.ds(lane, 8, stride=128), :] = s
                lows[pl.ds(lane, 8, stride=128), :] = e
    s, e = highs[0:128], lows[0:128]
    for k in range(1, 8):
        s, err = two_sum(s, highs[128 * k : 128 * k + 128])
        e = e + (err + lows[128 * k : 128 * k + 128])
    s, e = s.T, e.T
    hi, lo = sum_rows(jnp.concatenate([s[GHOST : GHOST + OWN], e[GHOST : GHOST + OWN]], axis=0))
    row = lax.broadcasted_iota(jnp.int32, (8, 128), 0)
    both = jnp.where((row & 1) == 0, jnp.broadcast_to(hi, (8, 128)), jnp.broadcast_to(lo, (8, 128)))
    out[...] = jnp.concatenate([both] * (out.shape[0] // 8), axis=0)


def gram_pairs(count):
    out = []
    for i in range(count):
        out += [(i, j, sorted({16 * i + j, 16 * j + i})) for j in range(i, count)]
        out.append((i, count, [16 * i + 8]))
    return out


def at(ref, *index):
    return lambda t: ref[(*index, t)]


def first_body(own, facing, coef, lines, below_mat, above_mat, fold, r0, v_ref, w_ref, gram, raw, grid, y_buf, g_buf, vp, ve, vw, highs, lows):
    s_id = lax.broadcasted_iota(jnp.int32, (8, 128), 0)
    zero = jnp.zeros((8, 128), F32)
    gap = jnp.zeros((64 - WIDE, 128), F32)
    for place in range(7):
        for source in range(4):
            full = jnp.concatenate([own[source, place], gap, facing[source, place], gap], axis=0)
            raw[place, 128 * source : 128 * source + 128, :] = full.T
        for t in range(STEPS):
            grid[place, t + 1] = raw[place, pl.ds(t, 8, stride=STEPS), :]
    top_north = grid[3, STEPS]
    top_ocean = grid[6, STEPS]
    last = s_id == 7
    fold_open = jnp.where(last, 0.5 * (top_north + facing_of(top_north)), 0.0)
    fold[...] = fold_open * top_ocean * facing_of(top_ocean)
    for place in (3, 4, 5):
        grid[place, STEPS] = jnp.where(last, 0.0, grid[place, STEPS])
    for place in (3, 4, 5, 6):
        grid[place, 0] = row_before(grid[place, STEPS])
        grid[place, STEPS + 1] = row_after(grid[place, 1])

    def weigh(t, _):
        o, o_up, o_down = grid[6, t + 1], grid[6, t + 2], grid[6, t]
        east = grid[2, t + 1]
        north, neast, nwest = grid[3, t + 1], grid[4, t + 1], grid[5, t + 1]
        south, s_neast, s_nwest = grid[3, t], grid[4, t], grid[5, t]
        open_sum = zero
        parts = (
            (E, east, east_of(o)),
            (W, west_of(east), west_of(o)),
            (N, north, o_up),
            (S, south, o_down),
            (NE, neast, east_of(o_up)),
            (SW, west_of(s_neast), west_of(o_down)),
            (NW, nwest, west_of(o_up)),
            (SE, east_of(s_nwest), east_of(o_down)),
        )
        for place, edge, other in parts:
            coef[place, t] = edge * o * other
            open_sum = open_sum + edge
        surface = grid[1, t + 1]
        coef[DIAG, t] = o * (surface + open_sum) + (1.0 - o)
        r0[t] = o * grid[0, t + 1]
        vw[t] = o * (surface + coef[N, t] + coef[S, t]) + (1.0 - o)
        return 0

    lax.fori_loop(0, STEPS, weigh, 0, unroll=2)
    o = top_ocean
    coef[DIAG, STEPS - 1] = coef[DIAG, STEPS - 1] + o * fold_open

    def eliminate(t, carry):
        ratio, beyond = carry
        north = coef[N, t]
        pivot = vw[t] - coef[S, t] * ratio
        more, err = two_sum(pivot, -north)
        more = more + err
        y_buf[t] = more - ratio * beyond
        guess = north / pivot
        prod, err = two_prod(guess, pivot)
        return guess + ((north - prod) - err) / pivot, more

    ends = lax.fori_loop(0, STEPS, eliminate, (zero, zero), unroll=2)
    lax.fori_loop(0, STEPS, eliminate, tuple(row_before(v) for v in ends), unroll=2)

    def pivots(t, carry):
        before, beyond, response, source = carry
        rest = y_buf[t]
        mult = jnp.where(t == 0, zero, coef[S, t] * before)
        beyond = rest + jnp.where(t == 0, coef[S, 0], mult * beyond)
        inverse = 1.0 / (coef[N, t] + beyond)
        lines[MULT, t] = mult
        lines[IPIV, t] = inverse
        response = jnp.where(t == 0, coef[S, 0], mult * response)
        source = rest + mult * source
        g_buf[t] = response
        vp[t] = source
        return inverse, beyond, response, source

    lax.fori_loop(0, STEPS, pivots, (zero,) * 4, unroll=4)
    for t in range(STEPS, lines.shape[1]):
        lines[MULT, t] = zero

    def respond(k, carry):
        low, up, source = carry
        t = STEPS - 1 - k
        factor = lines[MULT, t + 1]
        inverse = lines[IPIV, t]
        low = g_buf[t] * inverse + factor * low
        up = jnp.where(k == 0, coef[N, STEPS - 1] * inverse, factor * up)
        source = vp[t] * inverse + factor * source
        lines[LOWER, t] = low
        lines[UPPER, t] = up
        ve[t] = source
        return low, up, source

    lax.fori_loop(0, STEPS, respond, (zero,) * 3, unroll=4)
    unit = lax.broadcasted_iota(jnp.int32, (16, 128), 0)
    low_first, low_last = lines[LOWER, 0], lines[LOWER, STEPS - 1]
    up_first, up_last = lines[UPPER, 0], lines[UPPER, STEPS - 1]

    def spread(v, s):
        return jnp.broadcast_to(v[s : s + 1, :], (16, 128))

    source_first, source_last = ve[0], ve[STEPS - 1]
    alphas, betas, dens = [jnp.zeros((16, 128), F32)], [jnp.zeros((16, 128), F32)], []
    short = jnp.ones((16, 128), F32)
    for s in range(8):
        alpha, beta = alphas[-1], betas[-1]
        g_first = jnp.where(unit == s, 1.0, 0.0)
        g_last = jnp.where(unit == 8 + s, 1.0, 0.0)
        lf, ll, uf, ul = (spread(v, s) for v in (low_first, low_last, up_first, up_last))
        sf, sl = spread(source_first, s), spread(source_last, s)
        den = 1.0 / (sf + uf + short * lf)
        dens.append(den)
        alphas.append(g_last + ll * (alpha + beta * den * (g_first + lf * alpha)))
        betas.append(ul + ll * beta * den * uf)
        short = sl + ll * (short + beta * den * (sf + lf * short))
    above = jnp.zeros((16, 128), F32)
    for s in range(7, -1, -1):
        alpha, beta = alphas[s], betas[s]
        above_mat[:, s, :] = above
        lf, uf = spread(low_first, s), spread(up_first, s)
        g_first = jnp.where(unit == s, 1.0, 0.0)
        above = dens[s] * (g_first + lf * alpha + uf * above)
        below_mat[:, s, :] = alpha + beta * above
    finish_with = functools.partial(store_field, v_ref)
    for i in range(HALF):
        load = (lambda t: r0[t]) if i == 0 else (lambda t, i=i: w_ref[i - 1, t])
        value = (lambda t0, g: g) if i == 0 else (lambda t0, g: g * SCALE)
        line_solve(load, lines, below_mat, above_mat, y_buf, g_buf, finish_with(i, vp, ve, vw)(value))
        operate(v_ref, i, w_ref, coef, fold, vp, ve, vw)
    lefts = [at(v_ref, i) for i in range(HALF)]
    rights = [at(w_ref, j) for j in range(HALF)] + [at(r0)]
    gram_row(lefts, rights, gram_pairs(HALF), False, highs, lows, gram)


def second_body(sums, coef, lines, below_mat, above_mat, fold, r0, v1, w1, r_ref, y_out, v_ref, w_ref, gram, y_buf, g_buf, vp, ve, vw, highs, lows):
    y, ratio = small_solve(*sum_rows(sums[...]), HALF)
    y_out[...] = y
    bound = ratio * (2.0 / SCALE)
    step = 2.0 / bound
    weights = [jnp.broadcast_to(y[i : i + 1, :], (8, 128)) for i in range(HALF)]

    def renew(t, _):
        r = r0[t]
        for i in range(HALF):
            r = r - weights[i] * w1[i, t]
        r_ref[t] = r
        return 0

    lax.fori_loop(0, STEPS, renew, 0, unroll=4)
    finish_with = functools.partial(store_field, v_ref)
    for i in range(HALF):
        load = (lambda t: r_ref[t]) if i == 0 else (lambda t, i=i: w_ref[i - 1, t])
        if i == 0:
            value = lambda t0, g: g
        elif i == 1:
            value = lambda t0, g: v_ref[0, pl.ds(t0, 8)] - step * g
        else:
            value = lambda t0, g, i=i: 2.0 * (v_ref[i - 1, pl.ds(t0, 8)] - step * g) - v_ref[i - 2, pl.ds(t0, 8)]
        line_solve(load, lines, below_mat, above_mat, y_buf, g_buf, finish_with(i, vp, ve, vw)(value))
        operate(v_ref, i, w_ref, coef, fold, vp, ve, vw)
    lefts = [at(ref, i) for ref in (v1, v_ref) for i in range(HALF)]
    rights = [at(ref, j) for ref in (w1, w_ref) for j in range(HALF)] + [at(r_ref)]
    gram_row(lefts, rights, gram_pairs(TOTAL), True, highs, lows, gram)


def last_body(sums, y1, r_ref, v1, w1, v2, w2, out, x_rows, r_rows):
    y, _ = small_solve(*sum_rows(sums[...]), TOTAL)
    w_weights = [jnp.broadcast_to(y[i : i + 1, :], (8, 128)) for i in range(TOTAL)]
    v_weights = [w + (y1[i : i + 1, :] if i < HALF else 0.0) for i, w in enumerate(w_weights)]
    for t in range(STEPS):
        x = jnp.zeros((8, 128), F32)
        r = r_ref[t]
        for i in range(HALF):
            x = x + v_weights[i] * v1[i, t]
            r = r - w_weights[i] * w1[i, t]
        for i in range(HALF):
            x = x + v_weights[HALF + i] * v2[i, t]
            r = r - w_weights[HALF + i] * w2[i, t]
        x_rows[pl.ds(t, 8, stride=STEPS), :] = x
        r_rows[pl.ds(t, 8, stride=STEPS), :] = r
    for place, rows in enumerate((x_rows, r_rows)):
        for part in range(4):
            out[part, place] = rows[128 * part : 128 * part + 128, :].T[GHOST : GHOST + OWN, :]


def unpack_body(recv, x, r):
    for place, ref in enumerate((x, r)):
        ref[...] = jnp.concatenate([recv[part, place] for part in range(4)], axis=0).T


def shape(*dims):
    return jax.ShapeDtypeStruct(dims, F32)


def vmem(*dims):
    return pltpu.VMEM(dims, F32)


FIELD = (STEPS, 8, 128)
SCRATCH = [vmem(*FIELD), vmem(*FIELD), vmem(STEPS + 2, 8, 128), vmem(STEPS + 2, 8, 128), vmem(STEPS + 2, 8, 128), vmem(1024, 128), vmem(1024, 128)]


def all_sums(gram):
    return lax.all_to_all(gram, ("lat", *LON), split_axis=0, concat_axis=0, tiled=True)


def ring(block, step):
    return lax.ppermute(block, LON, [(d, (d + step) % 64) for d in range(64)])


def reflect(block, half):
    def branch(q):
        return lambda b: lax.ppermute(b, LON, [(d, (2 * q - d) % 64) for d in range(64)])

    return lax.switch(half, [branch(q) for q in range(32)], block)


def strips(block, odd):
    def even_branch(b):
        return ring(b[:, COLS - SIDE :], -1), b, ring(b[:, :SIDE], 1)

    def odd_branch(b):
        return b[:, COLS - SIDE :], ring(b, 1), ring(b[:, :SIDE], 2)

    return lax.cond(odd == 0, even_branch, odd_branch, block)


def swap_lat(pieces):
    return lax.all_to_all(pieces, "lat", split_axis=0, concat_axis=0, tiled=True)


def shards(right_side, surface_term, east, north, neast, nwest, land_sea, fold_map):
    offset = (fold_map[0] + COLS * lax.axis_index(LON)) % NLON
    centre = ((offset - COLS // 2) % NLON) // COLS
    shift = (offset - COLS // 2) % COLS + COLS // 2
    smem = pl.BlockSpec(memory_space=pltpu.SMEM)
    whole = pl.BlockSpec(memory_space=pltpu.VMEM)
    packed = pl.pallas_call(pack_body, out_shape=shape(7, COLS, 128), name="pack")(
        right_side, surface_term, east, north, neast, nwest, land_sea
    )
    before = ring(packed[:, COLS - GHOST :], 1)
    after = ring(packed[:, :GHOST], -1)
    block = reflect(packed, centre // 2)
    own = pl.pallas_call(window_body, out_shape=shape(4, 7, WIDE, 128), name="window", compiler_params=params())(
        before, packed, after
    )
    own = swap_lat(own)
    low, main, high = strips(block, centre % 2)
    windows = pl.pallas_call(
        select_body,
        in_specs=[smem] + [whole] * 3,
        out_shape=shape(4, 7, WIDE, 128),
        name="select",
        compiler_params=params(),
    )(shift.reshape(1), low, main, high)
    facing = swap_lat(windows)
    coef, lines, below_mat, above_mat, fold, r0, v1, w1, gram = pl.pallas_call(
        first_body,
        out_shape=(
            shape(9, *FIELD),
            shape(4, STEPS + 8, 8, 128),
            shape(16, 8, 128),
            shape(16, 8, 128),
            shape(8, 128),
            shape(*FIELD),
            shape(HALF, *FIELD),
            shape(HALF, *FIELD),
            shape(512, 128),
        ),
        scratch_shapes=[vmem(7, 512, 128), vmem(7, STEPS + 2, 8, 128), *SCRATCH],
        name="phase_one",
        compiler_params=params(),
    )(own, facing)
    sums = all_sums(gram)
    r4, y1, v2, w2, gram = pl.pallas_call(
        second_body,
        out_shape=(
            shape(*FIELD),
            shape(8, 128),
            shape(HALF, *FIELD),
            shape(HALF, *FIELD),
            shape(512, 128),
        ),
        scratch_shapes=SCRATCH,
        name="phase_two",
        compiler_params=params(),
    )(sums, coef, lines, below_mat, above_mat, fold, r0, v1, w1)
    sums = all_sums(gram)
    pieces = pl.pallas_call(
        last_body,
        out_shape=shape(4, 2, OWN, 128),
        scratch_shapes=[vmem(512, 128), vmem(512, 128)],
        name="combine",
        compiler_params=params(),
    )(sums, y1, r4, v1, w1, v2, w2)
    columns = swap_lat(pieces)
    return pl.pallas_call(unpack_body, out_shape=(shape(128, COLS), shape(128, COLS)), name="unpack")(columns)


def solution(mesh):
    finer = Mesh(mesh.devices.reshape(mesh.shape["lat"], 4, 8, 2), ("lat", *LON))
    field = P("lat", LON)
    return jax.shard_map(
        shards,
        mesh=finer,
        in_specs=(field,) * 7 + (P(LON),),
        out_specs=(field, field),
        check_vma=False,
    )
```

```python
import functools

import jax
import jax.numpy as jnp
from jax import lax
from jax.experimental import pallas as pl
from jax.experimental.pallas import tpu as pltpu
from jax.sharding import Mesh
from jax.sharding import PartitionSpec as P


LON = ("x", "z", "core")
NLON = 8192
COLS = 128
OWN = 32
GHOST = 8
WIDE = OWN + 2 * GHOST
PAD = COLS + 2 * GHOST
STEPS = 64
HALF = 4
TOTAL = 2 * HALF
SCALE = 1.0e-4
F32 = jnp.float32
E, W, N, S, NE, SW, NW, SE, DIAG = range(9)
MULT, IPIV, LOWER, UPPER, RISE, FALL = range(6)
SPAN = 8


SIDE = 72


def params(mib=24):
    return pltpu.CompilerParams(vmem_limit_bytes=mib * 1024 * 1024)


def two_sum(a, b):
    s = a + b
    bb = s - a
    return s, (a - (s - bb)) + (b - bb)


def split(a):
    t = a * 4097.0
    hi = t - (t - a)
    return hi, a - hi


def two_prod(a, b):
    p = a * b
    ah, al = split(a)
    bh, bl = split(b)
    return p, ((ah * bh - p) + ah * bl + al * bh) + al * bl


def renorm(s, e):
    hi = s + e
    return hi, e - (hi - s)


def pair_sub(a, b):
    s, e = two_sum(a[0], -b[0])
    return renorm(s, e + (a[1] - b[1]))


def pair_mul(a, b):
    p, e = two_prod(a[0], b[0])
    return renorm(p, e + (a[0] * b[1] + a[1] * b[0]))


def pair_div(a, b):
    first = a[0] / b[0]
    zero = jnp.zeros_like(first)
    rest = pair_sub(a, pair_mul((first, zero), b))
    return renorm(first, rest[0] / b[0])


def sum_rows(values):
    s = values[0:8]
    e = jnp.zeros_like(s)
    for start in range(8, values.shape[0], 8):
        s, err = two_sum(s, values[start : start + 8])
        e = e + err
    for shift in (4, 2, 1):
        s_other = pltpu.roll(s, shift, 0)
        e_other = pltpu.roll(e, shift, 0)
        s, err = two_sum(s, s_other)
        e = e + e_other + err
    hi, lo = renorm(s, e)
    return hi[0:1], lo[0:1]


def small_solve(hi_row, lo_row, order):
    row = lax.broadcasted_iota(jnp.int32, (8, 128), 0)
    lane = lax.broadcasted_iota(jnp.int32, (8, 128), 1)

    def matrix(values):
        wide = jnp.broadcast_to(values, (8, 128))
        out = jnp.zeros((8, 128), F32)
        for i in range(order):
            turned = wide if i == 0 else pltpu.roll(wide, 128 - 16 * i, 1)
            out = jnp.where(row == i, turned, out)
        return jnp.where(lane < 16, out, 0.0)

    hi, lo = matrix(hi_row), matrix(lo_row)
    ratio = hi[3:4, 3:4] / hi[3:4, 2:3]
    start = jnp.sum(jnp.where(row == lane, hi, 0.0), axis=1, keepdims=True)
    live = jnp.ones((8, 128), F32)
    for k in range(order):
        col = tuple(jnp.broadcast_to(v[:, k : k + 1], (8, 128)) for v in (hi, lo))
        piv_row = tuple(jnp.broadcast_to(v[k : k + 1, :], (8, 128)) for v in (hi, lo))
        piv = tuple(jnp.broadcast_to(v[k : k + 1, k : k + 1], (8, 128)) for v in (hi, lo))
        good = piv[0] > 1e-11 * jnp.broadcast_to(start[k : k + 1, :], (8, 128))
        piv = (jnp.where(good, piv[0], 1.0), jnp.where(good, piv[1], 0.0))
        factor = pair_div(col, piv)
        new = pair_sub((hi, lo), pair_mul(factor, piv_row))
        change = good & (row != k)
        hi = jnp.where(change, new[0], hi)
        lo = jnp.where(change, new[1], lo)
        live = jnp.where((row == k) & ~good, 0.0, live)
    diag = jnp.sum(jnp.where(row == lane, hi, 0.0), axis=1, keepdims=True)
    diag = jnp.where((diag != 0.0) & (live[:, 0:1] > 0.0), diag, 1.0)
    y = jnp.broadcast_to(hi[:, 8:9] / diag, (8, 128)) * live
    y = jnp.where(row < order, y, 0.0)
    return y, jnp.broadcast_to(ratio, (8, 128))


def pack_body(rhs, surface, east, north, neast, nwest, land, out):
    for k, ref in enumerate((rhs, surface, east, north, neast, nwest)):
        out[k] = ref[...].T
    out[6] = land[...].astype(F32).T


def window_body(before, packed, after, out):
    for place in range(7):
        wide = jnp.concatenate([before[place], packed[place], after[place]], axis=0)
        for part in range(4):
            out[part, place] = wide[OWN * part : OWN * part + WIDE, :]


def select_body(shift, low, main, high, out):
    i = lax.broadcasted_iota(jnp.int32, (PAD, COLS + 2 * SIDE), 0)
    u = lax.broadcasted_iota(jnp.int32, (PAD, COLS + 2 * SIDE), 1)
    reach = shift[0] + GHOST + SIDE
    plain = jnp.where(u == reach - i, 1.0, 0.0).astype(jnp.bfloat16)
    moved = jnp.where(u == reach - 1 - i, 1.0, 0.0).astype(jnp.bfloat16)

    def pick(choice, values):
        return jnp.dot(choice, values, preferred_element_type=F32)

    for place, source in enumerate((0, 1, 2, 3, 5, 4, 6)):
        both = jnp.concatenate([low[source], main[source], high[source]], axis=0)
        top = both.astype(jnp.bfloat16)
        rest = both - top.astype(F32)
        middle = rest.astype(jnp.bfloat16)
        bottom = (rest - middle.astype(F32)).astype(jnp.bfloat16)
        choice = moved if source == 2 else plain
        facing = (pick(choice, top) + pick(choice, middle)) + pick(choice, bottom)
        for part in range(4):
            out[part, place] = facing[OWN * part : OWN * part + WIDE, :]


def east_of(v):
    return pltpu.roll(v, 127, v.ndim - 1)


def west_of(v):
    return pltpu.roll(v, 1, v.ndim - 1)


def facing_of(v):
    return pltpu.roll(v, 64, v.ndim - 1)


def row_before(v):
    s = lax.broadcasted_iota(jnp.int32, (8, 128), 0)
    return jnp.where(s == 0, 0.0, pltpu.roll(v, 1, 0))


def row_after(v):
    s = lax.broadcasted_iota(jnp.int32, (8, 128), 0)
    return jnp.where(s == 7, 0.0, pltpu.roll(v, 7, 0))


def line_solve(load, lines, below_mat, above_mat, y_buf, g_buf, finish):
    zero = jnp.zeros((8, 128), F32)

    carried = zero
    for start in range(0, STEPS, SPAN):
        local = zero
        before = carried
        for t in range(start, start + SPAN):
            local = load(t) + lines[MULT, t] * local if t > start else load(t)
            y = local + lines[RISE, t] * before
            y_buf[t] = y
        carried = y
    carried = zero
    for start in range(STEPS - 1, -1, -SPAN):
        local = zero
        after = carried
        for t in range(start, start - SPAN, -1):
            scaled = y_buf[t] * lines[IPIV, t]
            local = scaled + lines[MULT, t + 1] * local if t < start else scaled
            x = local + lines[FALL, t] * after
            g_buf[t] = x
        carried = x
    first, last = g_buf[0], g_buf[STEPS - 1]
    below, above = zero, zero
    for k in range(8):
        for base, ends in ((0, first), (8, last)):
            end = jnp.broadcast_to(ends[k : k + 1, :], (8, 128))
            below = below + below_mat[base + k] * end
            above = above + above_mat[base + k] * end

    def combine(c, _):
        t0 = c * 8
        g = g_buf[pl.ds(t0, 8)] + lines[LOWER, pl.ds(t0, 8)] * below + lines[UPPER, pl.ds(t0, 8)] * above
        finish(t0, g)
        return 0

    lax.fori_loop(0, STEPS // 8, combine, 0, unroll=2)


def operate(v_ref, place, w_ref, coef, fold, vp, ve, vw):
    for t, v in ((0, row_before(v_ref[place, STEPS - 1])), (STEPS + 1, row_after(v_ref[place, 0]))):
        vp[t] = v
        ve[t] = east_of(v)
        vw[t] = west_of(v)

    def step(c, _):
        t = c * 4
        here, up, down = pl.ds(t + 1, 4), pl.ds(t + 2, 4), pl.ds(t, 4)
        at = pl.ds(t, 4)
        out = coef[DIAG, at] * vp[here]
        side = coef[E, at] * ve[here] + coef[W, at] * vw[here]
        north = coef[N, at] * vp[up] + coef[NE, at] * ve[up] + coef[NW, at] * vw[up]
        south = coef[S, at] * vp[down] + coef[SW, at] * vw[down] + coef[SE, at] * ve[down]
        w_ref[place, at] = out - (side + north + south)
        return 0

    lax.fori_loop(0, STEPS // 4, step, 0, unroll=2)
    w_ref[place, STEPS - 1] = w_ref[place, STEPS - 1] - fold[...] * facing_of(v_ref[place, STEPS - 1])


def store_field(v_ref, place, vp, ve, vw):
    def finish_with(value_of):
        def finish(t0, g):
            v = value_of(t0, g)
            v_ref[place, pl.ds(t0, 8)] = v
            vp[pl.ds(t0 + 1, 8)] = v
            ve[pl.ds(t0 + 1, 8)] = east_of(v)
            vw[pl.ds(t0 + 1, 8)] = west_of(v)

        return finish

    return finish_with


def gram_row(lefts, rights, pairs, exact, highs, lows, out):
    highs[...] = jnp.zeros(highs.shape, F32)
    lows[...] = jnp.zeros(lows.shape, F32)
    start = 0
    while start < len(pairs):
        end = start
        while end < len(pairs) and (pairs[end][0] == pairs[start][0] or end - start < 12) and end - start < 17:
            end += 1
        part = pairs[start:end]
        start = end

        def add(t, sums, part=part):
            left = {i: lefts[i](t) for i in sorted({i for i, _, _ in part})}
            right = {j: rights[j](t) for j in sorted({j for _, j, _ in part})}
            if not exact:
                return tuple((s + left[i] * right[j], e) for (s, e), (i, j, _) in zip(sums, part))
            left_halves = {i: split(v) for i, v in left.items()}
            right_halves = {j: split(v) for j, v in right.items()}
            out = []
            for (s, e), (i, j, _) in zip(sums, part):
                ah, al = left_halves[i]
                bh, bl = right_halves[j]
                s, err = two_sum(s, ah * bh)
                out.append((s, e + (err + (ah * bl + al * right[j]))))
            return tuple(out)

        zero = jnp.zeros((8, 128), F32)
        sums = lax.fori_loop(0, STEPS, add, tuple((zero, zero) for _ in part), unroll=1 if exact else 2)
        for (s, e), (_, _, lanes) in zip(sums, part):
            for lane in lanes:
                highs[pl.ds(lane, 8, stride=128), :] = s
                lows[pl.ds(lane, 8, stride=128), :] = e
    s, e = highs[0:128], lows[0:128]
    for k in range(1, 8):
        s, err = two_sum(s, highs[128 * k : 128 * k + 128])
        e = e + (err + lows[128 * k : 128 * k + 128])
    s, e = s.T, e.T
    hi, lo = sum_rows(jnp.concatenate([s[GHOST : GHOST + OWN], e[GHOST : GHOST + OWN]], axis=0))
    row = lax.broadcasted_iota(jnp.int32, (8, 128), 0)
    both = jnp.where((row & 1) == 0, jnp.broadcast_to(hi, (8, 128)), jnp.broadcast_to(lo, (8, 128)))
    out[...] = jnp.concatenate([both] * (out.shape[0] // 8), axis=0)


def gram_pairs(count):
    out = []
    for i in range(count):
        out += [(i, j, sorted({16 * i + j, 16 * j + i})) for j in range(i, count)]
        out.append((i, count, [16 * i + 8]))
    return out


def at(ref, *index):
    return lambda t: ref[(*index, t)]


def first_body(own, facing, coef, lines, below_mat, above_mat, fold, r0, v_ref, w_ref, gram, raw, grid, y_buf, g_buf, vp, ve, vw, highs, lows):
    s_id = lax.broadcasted_iota(jnp.int32, (8, 128), 0)
    zero = jnp.zeros((8, 128), F32)
    gap = jnp.zeros((64 - WIDE, 128), F32)
    for place in range(7):
        for source in range(4):
            full = jnp.concatenate([own[source, place], gap, facing[source, place], gap], axis=0)
            raw[place, 128 * source : 128 * source + 128, :] = full.T
        for t in range(STEPS):
            grid[place, t + 1] = raw[place, pl.ds(t, 8, stride=STEPS), :]
    top_north = grid[3, STEPS]
    top_ocean = grid[6, STEPS]
    last = s_id == 7
    fold_open = jnp.where(last, 0.5 * (top_north + facing_of(top_north)), 0.0)
    fold[...] = fold_open * top_ocean * facing_of(top_ocean)
    for place in (3, 4, 5):
        grid[place, STEPS] = jnp.where(last, 0.0, grid[place, STEPS])
    for place in (3, 4, 5, 6):
        grid[place, 0] = row_before(grid[place, STEPS])
        grid[place, STEPS + 1] = row_after(grid[place, 1])

    def weigh(t, _):
        o, o_up, o_down = grid[6, t + 1], grid[6, t + 2], grid[6, t]
        east = grid[2, t + 1]
        north, neast, nwest = grid[3, t + 1], grid[4, t + 1], grid[5, t + 1]
        south, s_neast, s_nwest = grid[3, t], grid[4, t], grid[5, t]
        open_sum = zero
        parts = (
            (E, east, east_of(o)),
            (W, west_of(east), west_of(o)),
            (N, north, o_up),
            (S, south, o_down),
            (NE, neast, east_of(o_up)),
            (SW, west_of(s_neast), west_of(o_down)),
            (NW, nwest, west_of(o_up)),
            (SE, east_of(s_nwest), east_of(o_down)),
        )
        for place, edge, other in parts:
            coef[place, t] = edge * o * other
            open_sum = open_sum + edge
        surface = grid[1, t + 1]
        coef[DIAG, t] = o * (surface + open_sum) + (1.0 - o)
        r0[t] = o * grid[0, t + 1]
        vw[t] = o * (surface + coef[N, t] + coef[S, t]) + (1.0 - o)
        return 0

    lax.fori_loop(0, STEPS, weigh, 0, unroll=2)
    o = top_ocean
    coef[DIAG, STEPS - 1] = coef[DIAG, STEPS - 1] + o * fold_open

    def eliminate(t, carry):
        ratio, beyond = carry
        north = coef[N, t]
        pivot = vw[t] - coef[S, t] * ratio
        more, err = two_sum(pivot, -north)
        more = more + err
        y_buf[t] = more - ratio * beyond
        guess = north / pivot
        prod, err = two_prod(guess, pivot)
        return guess + ((north - prod) - err) / pivot, more

    ends = lax.fori_loop(0, STEPS, eliminate, (zero, zero), unroll=2)
    lax.fori_loop(0, STEPS, eliminate, tuple(row_before(v) for v in ends), unroll=2)

    def pivots(t, carry):
        before, beyond, response, source = carry
        rest = y_buf[t]
        mult = jnp.where(t == 0, zero, coef[S, t] * before)
        beyond = rest + jnp.where(t == 0, coef[S, 0], mult * beyond)
        inverse = 1.0 / (coef[N, t] + beyond)
        lines[MULT, t] = mult
        lines[IPIV, t] = inverse
        response = jnp.where(t == 0, coef[S, 0], mult * response)
        source = rest + mult * source
        g_buf[t] = response
        vp[t] = source
        return inverse, beyond, response, source

    lax.fori_loop(0, STEPS, pivots, (zero,) * 4, unroll=4)
    for t in range(STEPS, lines.shape[1]):
        lines[MULT, t] = zero
    for start in range(0, STEPS, SPAN):
        rise = lines[MULT, start]
        fall = lines[MULT, start + SPAN]
        for k in range(SPAN):
            lines[RISE, start + k] = rise
            lines[FALL, start + SPAN - 1 - k] = fall
            rise = rise * lines[MULT, start + k + 1]
            fall = fall * lines[MULT, start + SPAN - 1 - k]

    def respond(k, carry):
        low, up, source = carry
        t = STEPS - 1 - k
        factor = lines[MULT, t + 1]
        inverse = lines[IPIV, t]
        low = g_buf[t] * inverse + factor * low
        up = jnp.where(k == 0, coef[N, STEPS - 1] * inverse, factor * up)
        source = vp[t] * inverse + factor * source
        lines[LOWER, t] = low
        lines[UPPER, t] = up
        ve[t] = source
        return low, up, source

    lax.fori_loop(0, STEPS, respond, (zero,) * 3, unroll=4)
    unit = lax.broadcasted_iota(jnp.int32, (16, 128), 0)
    low_first, low_last = lines[LOWER, 0], lines[LOWER, STEPS - 1]
    up_first, up_last = lines[UPPER, 0], lines[UPPER, STEPS - 1]

    def spread(v, s):
        return jnp.broadcast_to(v[s : s + 1, :], (16, 128))

    source_first, source_last = ve[0], ve[STEPS - 1]
    alphas, betas, dens = [jnp.zeros((16, 128), F32)], [jnp.zeros((16, 128), F32)], []
    short = jnp.ones((16, 128), F32)
    for s in range(8):
        alpha, beta = alphas[-1], betas[-1]
        g_first = jnp.where(unit == s, 1.0, 0.0)
        g_last = jnp.where(unit == 8 + s, 1.0, 0.0)
        lf, ll, uf, ul = (spread(v, s) for v in (low_first, low_last, up_first, up_last))
        sf, sl = spread(source_first, s), spread(source_last, s)
        den = 1.0 / (sf + uf + short * lf)
        dens.append(den)
        alphas.append(g_last + ll * (alpha + beta * den * (g_first + lf * alpha)))
        betas.append(ul + ll * beta * den * uf)
        short = sl + ll * (short + beta * den * (sf + lf * short))
    above = jnp.zeros((16, 128), F32)
    for s in range(7, -1, -1):
        alpha, beta = alphas[s], betas[s]
        above_mat[:, s, :] = above
        lf, uf = spread(low_first, s), spread(up_first, s)
        g_first = jnp.where(unit == s, 1.0, 0.0)
        above = dens[s] * (g_first + lf * alpha + uf * above)
        below_mat[:, s, :] = alpha + beta * above
    finish_with = functools.partial(store_field, v_ref)
    for i in range(HALF):
        load = (lambda t: r0[t]) if i == 0 else (lambda t, i=i: w_ref[i - 1, t])
        value = (lambda t0, g: g) if i == 0 else (lambda t0, g: g * SCALE)
        line_solve(load, lines, below_mat, above_mat, y_buf, g_buf, finish_with(i, vp, ve, vw)(value))
        operate(v_ref, i, w_ref, coef, fold, vp, ve, vw)
    lefts = [at(v_ref, i) for i in range(HALF)]
    rights = [at(w_ref, j) for j in range(HALF)] + [at(r0)]
    gram_row(lefts, rights, gram_pairs(HALF), False, highs, lows, gram)


def second_body(sums, coef, lines, below_mat, above_mat, fold, r0, v1, w1, r_ref, y_out, v_ref, w_ref, gram, y_buf, g_buf, vp, ve, vw, highs, lows):
    y, ratio = small_solve(*sum_rows(sums[...]), HALF)
    y_out[...] = y
    bound = ratio * (2.0 / SCALE)
    step = 2.0 / bound
    weights = [jnp.broadcast_to(y[i : i + 1, :], (8, 128)) for i in range(HALF)]

    def renew(t, _):
        r = r0[t]
        for i in range(HALF):
            r = r - weights[i] * w1[i, t]
        r_ref[t] = r
        return 0

    lax.fori_loop(0, STEPS, renew, 0, unroll=4)
    finish_with = functools.partial(store_field, v_ref)
    for i in range(HALF):
        load = (lambda t: r_ref[t]) if i == 0 else (lambda t, i=i: w_ref[i - 1, t])
        if i == 0:
            value = lambda t0, g: g
        elif i == 1:
            value = lambda t0, g: v_ref[0, pl.ds(t0, 8)] - step * g
        else:
            value = lambda t0, g, i=i: 2.0 * (v_ref[i - 1, pl.ds(t0, 8)] - step * g) - v_ref[i - 2, pl.ds(t0, 8)]
        line_solve(load, lines, below_mat, above_mat, y_buf, g_buf, finish_with(i, vp, ve, vw)(value))
        operate(v_ref, i, w_ref, coef, fold, vp, ve, vw)
    lefts = [at(ref, i) for ref in (v1, v_ref) for i in range(HALF)]
    rights = [at(ref, j) for ref in (w1, w_ref) for j in range(HALF)] + [at(r_ref)]
    gram_row(lefts, rights, gram_pairs(TOTAL), True, highs, lows, gram)


def last_body(sums, y1, r_ref, v1, w1, v2, w2, out, x_rows, r_rows):
    y, _ = small_solve(*sum_rows(sums[...]), TOTAL)
    w_weights = [jnp.broadcast_to(y[i : i + 1, :], (8, 128)) for i in range(TOTAL)]
    v_weights = [w + (y1[i : i + 1, :] if i < HALF else 0.0) for i, w in enumerate(w_weights)]
    for t in range(STEPS):
        x = jnp.zeros((8, 128), F32)
        r = r_ref[t]
        for i in range(HALF):
            x = x + v_weights[i] * v1[i, t]
            r = r - w_weights[i] * w1[i, t]
        for i in range(HALF):
            x = x + v_weights[HALF + i] * v2[i, t]
            r = r - w_weights[HALF + i] * w2[i, t]
        x_rows[pl.ds(t, 8, stride=STEPS), :] = x
        r_rows[pl.ds(t, 8, stride=STEPS), :] = r
    for place, rows in enumerate((x_rows, r_rows)):
        for part in range(4):
            out[part, place] = rows[128 * part : 128 * part + 128, :].T[GHOST : GHOST + OWN, :]


def unpack_body(recv, x, r):
    for place, ref in enumerate((x, r)):
        ref[...] = jnp.concatenate([recv[part, place] for part in range(4)], axis=0).T


def shape(*dims):
    return jax.ShapeDtypeStruct(dims, F32)


def vmem(*dims):
    return pltpu.VMEM(dims, F32)


FIELD = (STEPS, 8, 128)
SCRATCH = [vmem(*FIELD), vmem(*FIELD), vmem(STEPS + 2, 8, 128), vmem(STEPS + 2, 8, 128), vmem(STEPS + 2, 8, 128), vmem(1024, 128), vmem(1024, 128)]


def all_sums(gram):
    return lax.all_to_all(gram, ("lat", *LON), split_axis=0, concat_axis=0, tiled=True)


def ring(block, step):
    return lax.ppermute(block, LON, [(d, (d + step) % 64) for d in range(64)])


def reflect(block, half):
    def branch(q):
        return lambda b: lax.ppermute(b, LON, [(d, (2 * q - d) % 64) for d in range(64)])

    return lax.switch(half, [branch(q) for q in range(32)], block)


def strips(block, odd):
    def even_branch(b):
        return ring(b[:, COLS - SIDE :], -1), b, ring(b[:, :SIDE], 1)

    def odd_branch(b):
        return b[:, COLS - SIDE :], ring(b, 1), ring(b[:, :SIDE], 2)

    return lax.cond(odd == 0, even_branch, odd_branch, block)


def swap_lat(pieces):
    return lax.all_to_all(pieces, "lat", split_axis=0, concat_axis=0, tiled=True)


def shards(right_side, surface_term, east, north, neast, nwest, land_sea, fold_map):
    offset = (fold_map[0] + COLS * lax.axis_index(LON)) % NLON
    centre = ((offset - COLS // 2) % NLON) // COLS
    shift = (offset - COLS // 2) % COLS + COLS // 2
    smem = pl.BlockSpec(memory_space=pltpu.SMEM)
    whole = pl.BlockSpec(memory_space=pltpu.VMEM)
    packed = pl.pallas_call(pack_body, out_shape=shape(7, COLS, 128), name="pack")(
        right_side, surface_term, east, north, neast, nwest, land_sea
    )
    before = ring(packed[:, COLS - GHOST :], 1)
    after = ring(packed[:, :GHOST], -1)
    block = reflect(packed, centre // 2)
    own = pl.pallas_call(window_body, out_shape=shape(4, 7, WIDE, 128), name="window", compiler_params=params())(
        before, packed, after
    )
    own = swap_lat(own)
    low, main, high = strips(block, centre % 2)
    windows = pl.pallas_call(
        select_body,
        in_specs=[smem] + [whole] * 3,
        out_shape=shape(4, 7, WIDE, 128),
        name="select",
        compiler_params=params(),
    )(shift.reshape(1), low, main, high)
    facing = swap_lat(windows)
    coef, lines, below_mat, above_mat, fold, r0, v1, w1, gram = pl.pallas_call(
        first_body,
        out_shape=(
            shape(9, *FIELD),
            shape(6, STEPS + 8, 8, 128),
            shape(16, 8, 128),
            shape(16, 8, 128),
            shape(8, 128),
            shape(*FIELD),
            shape(HALF, *FIELD),
            shape(HALF, *FIELD),
            shape(512, 128),
        ),
        scratch_shapes=[vmem(7, 512, 128), vmem(7, STEPS + 2, 8, 128), *SCRATCH],
        name="phase_one",
        compiler_params=params(),
    )(own, facing)
    sums = all_sums(gram)
    r4, y1, v2, w2, gram = pl.pallas_call(
        second_body,
        out_shape=(
            shape(*FIELD),
            shape(8, 128),
            shape(HALF, *FIELD),
            shape(HALF, *FIELD),
            shape(512, 128),
        ),
        scratch_shapes=SCRATCH,
        name="phase_two",
        compiler_params=params(),
    )(sums, coef, lines, below_mat, above_mat, fold, r0, v1, w1)
    sums = all_sums(gram)
    pieces = pl.pallas_call(
        last_body,
        out_shape=shape(4, 2, OWN, 128),
        scratch_shapes=[vmem(512, 128), vmem(512, 128)],
        name="combine",
        compiler_params=params(),
    )(sums, y1, r4, v1, w1, v2, w2)
    columns = swap_lat(pieces)
    return pl.pallas_call(unpack_body, out_shape=(shape(128, COLS), shape(128, COLS)), name="unpack")(columns)


def solution(mesh):
    finer = Mesh(mesh.devices.reshape(mesh.shape["lat"], 4, 8, 2), ("lat", *LON))
    field = P("lat", LON)
    return jax.shard_map(
        shards,
        mesh=finer,
        in_specs=(field,) * 7 + (P(LON),),
        out_specs=(field, field),
        check_vma=False,
    )
```

```python
import functools

import jax
import jax.numpy as jnp
from jax import lax
from jax.experimental import pallas as pl
from jax.experimental.pallas import tpu as pltpu
from jax.sharding import Mesh
from jax.sharding import PartitionSpec as P


LON = ("x", "z", "core")
NLON = 8192
COLS = 128
OWN = 32
GHOST = 8
WIDE = OWN + 2 * GHOST
PAD = COLS + 2 * GHOST
STEPS = 64
HALF = 4
TOTAL = 2 * HALF
SCALE = 1.0e-4
F32 = jnp.float32
E, W, N, S, NE, SW, NW, SE, DIAG = range(9)
MULT, IPIV, LOWER, UPPER, RISE, FALL = range(6)
SPAN = 8


SIDE = 72


def params(mib=24):
    return pltpu.CompilerParams(vmem_limit_bytes=mib * 1024 * 1024)


def two_sum(a, b):
    s = a + b
    bb = s - a
    return s, (a - (s - bb)) + (b - bb)


def split(a):
    t = a * 4097.0
    hi = t - (t - a)
    return hi, a - hi


def two_prod(a, b):
    p = a * b
    ah, al = split(a)
    bh, bl = split(b)
    return p, ((ah * bh - p) + ah * bl + al * bh) + al * bl


def renorm(s, e):
    hi = s + e
    return hi, e - (hi - s)


def pair_sub(a, b):
    s, e = two_sum(a[0], -b[0])
    return renorm(s, e + (a[1] - b[1]))


def pair_mul(a, b):
    p, e = two_prod(a[0], b[0])
    return renorm(p, e + (a[0] * b[1] + a[1] * b[0]))


def pair_div(a, b):
    first = a[0] / b[0]
    zero = jnp.zeros_like(first)
    rest = pair_sub(a, pair_mul((first, zero), b))
    return renorm(first, rest[0] / b[0])


def sum_rows(values):
    s = values[0:8]
    e = jnp.zeros_like(s)
    for start in range(8, values.shape[0], 8):
        s, err = two_sum(s, values[start : start + 8])
        e = e + err
    for shift in (4, 2, 1):
        s_other = pltpu.roll(s, shift, 0)
        e_other = pltpu.roll(e, shift, 0)
        s, err = two_sum(s, s_other)
        e = e + e_other + err
    hi, lo = renorm(s, e)
    return hi[0:1], lo[0:1]


def small_solve(hi_row, lo_row, order):
    row = lax.broadcasted_iota(jnp.int32, (8, 128), 0)
    lane = lax.broadcasted_iota(jnp.int32, (8, 128), 1)

    def matrix(values):
        wide = jnp.broadcast_to(values, (8, 128))
        out = jnp.zeros((8, 128), F32)
        for i in range(order):
            turned = wide if i == 0 else pltpu.roll(wide, 128 - 16 * i, 1)
            out = jnp.where(row == i, turned, out)
        return jnp.where(lane < 16, out, 0.0)

    hi, lo = matrix(hi_row), matrix(lo_row)
    ratio = hi[3:4, 3:4] / hi[3:4, 2:3]
    start = jnp.sum(jnp.where(row == lane, hi, 0.0), axis=1, keepdims=True)
    live = jnp.ones((8, 128), F32)
    for k in range(order):
        col = tuple(jnp.broadcast_to(v[:, k : k + 1], (8, 128)) for v in (hi, lo))
        piv_row = tuple(jnp.broadcast_to(v[k : k + 1, :], (8, 128)) for v in (hi, lo))
        piv = tuple(jnp.broadcast_to(v[k : k + 1, k : k + 1], (8, 128)) for v in (hi, lo))
        good = piv[0] > 1e-11 * jnp.broadcast_to(start[k : k + 1, :], (8, 128))
        piv = (jnp.where(good, piv[0], 1.0), jnp.where(good, piv[1], 0.0))
        factor = pair_div(col, piv)
        new = pair_sub((hi, lo), pair_mul(factor, piv_row))
        change = good & (row != k)
        hi = jnp.where(change, new[0], hi)
        lo = jnp.where(change, new[1], lo)
        live = jnp.where((row == k) & ~good, 0.0, live)
    diag = jnp.sum(jnp.where(row == lane, hi, 0.0), axis=1, keepdims=True)
    diag = jnp.where((diag != 0.0) & (live[:, 0:1] > 0.0), diag, 1.0)
    y = jnp.broadcast_to(hi[:, 8:9] / diag, (8, 128)) * live
    y = jnp.where(row < order, y, 0.0)
    return y, jnp.broadcast_to(ratio, (8, 128))


def pack_body(rhs, surface, east, north, neast, nwest, land, out):
    for k, ref in enumerate((rhs, surface, east, north, neast, nwest)):
        out[k] = ref[...].T
    out[6] = land[...].astype(F32).T


def window_body(before, packed, after, out):
    for place in range(7):
        wide = jnp.concatenate([before[place], packed[place], after[place]], axis=0)
        for part in range(4):
            out[part, place] = wide[OWN * part : OWN * part + WIDE, :]


def select_body(shift, low, main, high, out):
    i = lax.broadcasted_iota(jnp.int32, (PAD, COLS + 2 * SIDE), 0)
    u = lax.broadcasted_iota(jnp.int32, (PAD, COLS + 2 * SIDE), 1)
    reach = shift[0] + GHOST + SIDE
    plain = jnp.where(u == reach - i, 1.0, 0.0).astype(jnp.bfloat16)
    moved = jnp.where(u == reach - 1 - i, 1.0, 0.0).astype(jnp.bfloat16)

    def pick(choice, values):
        return jnp.dot(choice, values, preferred_element_type=F32)

    for place, source in enumerate((0, 1, 2, 3, 5, 4, 6)):
        both = jnp.concatenate([low[source], main[source], high[source]], axis=0)
        top = both.astype(jnp.bfloat16)
        rest = both - top.astype(F32)
        middle = rest.astype(jnp.bfloat16)
        bottom = (rest - middle.astype(F32)).astype(jnp.bfloat16)
        choice = moved if source == 2 else plain
        facing = (pick(choice, top) + pick(choice, middle)) + pick(choice, bottom)
        for part in range(4):
            out[part, place] = facing[OWN * part : OWN * part + WIDE, :]


def east_of(v):
    return pltpu.roll(v, 127, v.ndim - 1)


def west_of(v):
    return pltpu.roll(v, 1, v.ndim - 1)


def facing_of(v):
    return pltpu.roll(v, 64, v.ndim - 1)


def row_before(v):
    s = lax.broadcasted_iota(jnp.int32, (8, 128), 0)
    return jnp.where(s == 0, 0.0, pltpu.roll(v, 1, 0))


def row_after(v):
    s = lax.broadcasted_iota(jnp.int32, (8, 128), 0)
    return jnp.where(s == 7, 0.0, pltpu.roll(v, 7, 0))


def line_solve(load, lines, below_mat, above_mat, y_buf, g_buf, finish):
    zero = jnp.zeros((8, 128), F32)

    carried = zero
    for start in range(0, STEPS, SPAN):
        local = zero
        before = carried
        for t in range(start, start + SPAN):
            local = load(t) + lines[MULT, t] * local if t > start else load(t)
            y = local + lines[RISE, t] * before
            y_buf[t] = y
        carried = y
    carried = zero
    for start in range(STEPS - 1, -1, -SPAN):
        local = zero
        after = carried
        for t in range(start, start - SPAN, -1):
            scaled = y_buf[t] * lines[IPIV, t]
            local = scaled + lines[MULT, t + 1] * local if t < start else scaled
            x = local + lines[FALL, t] * after
            g_buf[t] = x
        carried = x
    first, last = g_buf[0], g_buf[STEPS - 1]
    below, above = zero, zero
    for k in range(8):
        for base, ends in ((0, first), (8, last)):
            end = jnp.broadcast_to(ends[k : k + 1, :], (8, 128))
            below = below + below_mat[base + k] * end
            above = above + above_mat[base + k] * end

    def combine(c, _):
        t0 = c * 8
        g = g_buf[pl.ds(t0, 8)] + lines[LOWER, pl.ds(t0, 8)] * below + lines[UPPER, pl.ds(t0, 8)] * above
        finish(t0, g)
        return 0

    lax.fori_loop(0, STEPS // 8, combine, 0, unroll=2)


def operate(v_ref, place, w_ref, coef, fold, vp, ve, vw):
    for t, v in ((0, row_before(v_ref[place, STEPS - 1])), (STEPS + 1, row_after(v_ref[place, 0]))):
        vp[t] = v
        ve[t] = east_of(v)
        vw[t] = west_of(v)

    def step(c, _):
        t = c * 4
        here, up, down = pl.ds(t + 1, 4), pl.ds(t + 2, 4), pl.ds(t, 4)
        at = pl.ds(t, 4)
        out = coef[DIAG, at] * vp[here]
        side = coef[E, at] * ve[here] + coef[W, at] * vw[here]
        north = coef[N, at] * vp[up] + coef[NE, at] * ve[up] + coef[NW, at] * vw[up]
        south = coef[S, at] * vp[down] + coef[SW, at] * vw[down] + coef[SE, at] * ve[down]
        w_ref[place, at] = out - (side + north + south)
        return 0

    lax.fori_loop(0, STEPS // 4, step, 0, unroll=2)
    w_ref[place, STEPS - 1] = w_ref[place, STEPS - 1] - fold[...] * facing_of(v_ref[place, STEPS - 1])


def store_field(v_ref, place, vp, ve, vw):
    def finish_with(value_of):
        def finish(t0, g):
            v = value_of(t0, g)
            v_ref[place, pl.ds(t0, 8)] = v
            vp[pl.ds(t0 + 1, 8)] = v
            ve[pl.ds(t0 + 1, 8)] = east_of(v)
            vw[pl.ds(t0 + 1, 8)] = west_of(v)

        return finish

    return finish_with


def pack_own(sources, packed):
    lane = lax.broadcasted_iota(jnp.int32, (8, 128), 1)

    def step(c, _):
        for k, source in enumerate(sources):
            out = pltpu.roll(source(4 * c), 128 - GHOST, 1)
            for part in range(1, 4):
                moved = pltpu.roll(source(4 * c + part), OWN * part - GHOST, 1)
                out = jnp.where(lane >= OWN * part, moved, out)
            packed[k, c] = out
        return 0

    lax.fori_loop(0, STEPS // 4, step, 0)


def gram_row(lefts, rights, pairs, exact, columns, highs, lows, out):
    highs[...] = jnp.zeros(highs.shape, F32)
    lows[...] = jnp.zeros(lows.shape, F32)
    start = 0
    while start < len(pairs):
        end = start
        while end < len(pairs) and (pairs[end][0] == pairs[start][0] or end - start < 12) and end - start < 17:
            end += 1
        part = pairs[start:end]
        start = end

        def add(t, sums, part=part):
            left = {i: lefts[i](t) for i in sorted({i for i, _, _ in part})}
            right = {j: rights[j](t) for j in sorted({j for _, j, _ in part})}
            if not exact:
                return tuple((s + left[i] * right[j], e) for (s, e), (i, j, _) in zip(sums, part))
            left_halves = {i: split(v) for i, v in left.items()}
            right_halves = {j: split(v) for j, v in right.items()}
            out = []
            for (s, e), (i, j, _) in zip(sums, part):
                ah, al = left_halves[i]
                bh, bl = right_halves[j]
                s, err = two_sum(s, ah * bh)
                out.append((s, e + (err + (ah * bl + al * right[j]))))
            return tuple(out)

        zero = jnp.zeros((8, 128), F32)
        sums = lax.fori_loop(0, STEPS // 4 if exact else STEPS, add, tuple((zero, zero) for _ in part), unroll=1 if exact else 2)
        for (s, e), (_, _, lanes) in zip(sums, part):
            for lane in lanes:
                highs[pl.ds(lane, 8, stride=128), :] = s
                lows[pl.ds(lane, 8, stride=128), :] = e
    s, e = highs[0:128], lows[0:128]
    for k in range(1, 8):
        s, err = two_sum(s, highs[128 * k : 128 * k + 128])
        e = e + (err + lows[128 * k : 128 * k + 128])
    s, e = s.T, e.T
    hi, lo = sum_rows(jnp.concatenate([s[columns], e[columns]], axis=0))
    row = lax.broadcasted_iota(jnp.int32, (8, 128), 0)
    both = jnp.where((row & 1) == 0, jnp.broadcast_to(hi, (8, 128)), jnp.broadcast_to(lo, (8, 128)))
    out[...] = jnp.concatenate([both] * (out.shape[0] // 8), axis=0)


def gram_pairs(count):
    out = []
    for i in range(count):
        out += [(i, j, sorted({16 * i + j, 16 * j + i})) for j in range(i, count)]
        out.append((i, count, [16 * i + 8]))
    return out


def at(ref, *index):
    return lambda t: ref[(*index, t)]


def first_body(own, facing, coef, lines, below_mat, above_mat, fold, r0, v_ref, w_ref, gram, raw, grid, y_buf, g_buf, vp, ve, vw, highs, lows):
    s_id = lax.broadcasted_iota(jnp.int32, (8, 128), 0)
    zero = jnp.zeros((8, 128), F32)
    gap = jnp.zeros((64 - WIDE, 128), F32)
    for place in range(7):
        for source in range(4):
            full = jnp.concatenate([own[source, place], gap, facing[source, place], gap], axis=0)
            raw[place, 128 * source : 128 * source + 128, :] = full.T
        for t in range(STEPS):
            grid[place, t + 1] = raw[place, pl.ds(t, 8, stride=STEPS), :]
    top_north = grid[3, STEPS]
    top_ocean = grid[6, STEPS]
    last = s_id == 7
    fold_open = jnp.where(last, 0.5 * (top_north + facing_of(top_north)), 0.0)
    fold[...] = fold_open * top_ocean * facing_of(top_ocean)
    for place in (3, 4, 5):
        grid[place, STEPS] = jnp.where(last, 0.0, grid[place, STEPS])
    for place in (3, 4, 5, 6):
        grid[place, 0] = row_before(grid[place, STEPS])
        grid[place, STEPS + 1] = row_after(grid[place, 1])

    def weigh(t, _):
        o, o_up, o_down = grid[6, t + 1], grid[6, t + 2], grid[6, t]
        east = grid[2, t + 1]
        north, neast, nwest = grid[3, t + 1], grid[4, t + 1], grid[5, t + 1]
        south, s_neast, s_nwest = grid[3, t], grid[4, t], grid[5, t]
        open_sum = zero
        parts = (
            (E, east, east_of(o)),
            (W, west_of(east), west_of(o)),
            (N, north, o_up),
            (S, south, o_down),
            (NE, neast, east_of(o_up)),
            (SW, west_of(s_neast), west_of(o_down)),
            (NW, nwest, west_of(o_up)),
            (SE, east_of(s_nwest), east_of(o_down)),
        )
        for place, edge, other in parts:
            coef[place, t] = edge * o * other
            open_sum = open_sum + edge
        surface = grid[1, t + 1]
        coef[DIAG, t] = o * (surface + open_sum) + (1.0 - o)
        r0[t] = o * grid[0, t + 1]
        vw[t] = o * (surface + coef[N, t] + coef[S, t]) + (1.0 - o)
        return 0

    lax.fori_loop(0, STEPS, weigh, 0, unroll=2)
    o = top_ocean
    coef[DIAG, STEPS - 1] = coef[DIAG, STEPS - 1] + o * fold_open

    def eliminate(t, carry):
        ratio, beyond = carry
        north = coef[N, t]
        pivot = vw[t] - coef[S, t] * ratio
        more, err = two_sum(pivot, -north)
        more = more + err
        y_buf[t] = more - ratio * beyond
        guess = north / pivot
        prod, err = two_prod(guess, pivot)
        return guess + ((north - prod) - err) / pivot, more

    ends = lax.fori_loop(0, STEPS, eliminate, (zero, zero), unroll=2)
    lax.fori_loop(0, STEPS, eliminate, tuple(row_before(v) for v in ends), unroll=2)

    def pivots(t, carry):
        before, beyond, response, source = carry
        rest = y_buf[t]
        mult = jnp.where(t == 0, zero, coef[S, t] * before)
        beyond = rest + jnp.where(t == 0, coef[S, 0], mult * beyond)
        inverse = 1.0 / (coef[N, t] + beyond)
        lines[MULT, t] = mult
        lines[IPIV, t] = inverse
        response = jnp.where(t == 0, coef[S, 0], mult * response)
        source = rest + mult * source
        g_buf[t] = response
        vp[t] = source
        return inverse, beyond, response, source

    lax.fori_loop(0, STEPS, pivots, (zero,) * 4, unroll=4)
    for t in range(STEPS, lines.shape[1]):
        lines[MULT, t] = zero
    for start in range(0, STEPS, SPAN):
        rise = lines[MULT, start]
        fall = lines[MULT, start + SPAN]
        for k in range(SPAN):
            lines[RISE, start + k] = rise
            lines[FALL, start + SPAN - 1 - k] = fall
            rise = rise * lines[MULT, start + k + 1]
            fall = fall * lines[MULT, start + SPAN - 1 - k]

    def respond(k, carry):
        low, up, source = carry
        t = STEPS - 1 - k
        factor = lines[MULT, t + 1]
        inverse = lines[IPIV, t]
        low = g_buf[t] * inverse + factor * low
        up = jnp.where(k == 0, coef[N, STEPS - 1] * inverse, factor * up)
        source = vp[t] * inverse + factor * source
        lines[LOWER, t] = low
        lines[UPPER, t] = up
        ve[t] = source
        return low, up, source

    lax.fori_loop(0, STEPS, respond, (zero,) * 3, unroll=4)
    unit = lax.broadcasted_iota(jnp.int32, (16, 128), 0)
    low_first, low_last = lines[LOWER, 0], lines[LOWER, STEPS - 1]
    up_first, up_last = lines[UPPER, 0], lines[UPPER, STEPS - 1]

    def spread(v, s):
        return jnp.broadcast_to(v[s : s + 1, :], (16, 128))

    source_first, source_last = ve[0], ve[STEPS - 1]
    alphas, betas, dens = [jnp.zeros((16, 128), F32)], [jnp.zeros((16, 128), F32)], []
    short = jnp.ones((16, 128), F32)
    for s in range(8):
        alpha, beta = alphas[-1], betas[-1]
        g_first = jnp.where(unit == s, 1.0, 0.0)
        g_last = jnp.where(unit == 8 + s, 1.0, 0.0)
        lf, ll, uf, ul = (spread(v, s) for v in (low_first, low_last, up_first, up_last))
        sf, sl = spread(source_first, s), spread(source_last, s)
        den = 1.0 / (sf + uf + short * lf)
        dens.append(den)
        alphas.append(g_last + ll * (alpha + beta * den * (g_first + lf * alpha)))
        betas.append(ul + ll * beta * den * uf)
        short = sl + ll * (short + beta * den * (sf + lf * short))
    above = jnp.zeros((16, 128), F32)
    for s in range(7, -1, -1):
        alpha, beta = alphas[s], betas[s]
        above_mat[:, s, :] = above
        lf, uf = spread(low_first, s), spread(up_first, s)
        g_first = jnp.where(unit == s, 1.0, 0.0)
        above = dens[s] * (g_first + lf * alpha + uf * above)
        below_mat[:, s, :] = alpha + beta * above
    finish_with = functools.partial(store_field, v_ref)
    for i in range(HALF):
        load = (lambda t: r0[t]) if i == 0 else (lambda t, i=i: w_ref[i - 1, t])
        value = (lambda t0, g: g) if i == 0 else (lambda t0, g: g * SCALE)
        line_solve(load, lines, below_mat, above_mat, y_buf, g_buf, finish_with(i, vp, ve, vw)(value))
        operate(v_ref, i, w_ref, coef, fold, vp, ve, vw)
    lefts = [at(v_ref, i) for i in range(HALF)]
    rights = [at(w_ref, j) for j in range(HALF)] + [at(r0)]
    gram_row(lefts, rights, gram_pairs(HALF), False, slice(GHOST, GHOST + OWN), highs, lows, gram)


def second_body(sums, coef, lines, below_mat, above_mat, fold, r0, v1, w1, r_ref, y_out, v_ref, w_ref, gram, packed, y_buf, g_buf, vp, ve, vw, highs, lows):
    y, ratio = small_solve(*sum_rows(sums[...]), HALF)
    y_out[...] = y
    bound = ratio * (2.0 / SCALE)
    step = 2.0 / bound
    weights = [jnp.broadcast_to(y[i : i + 1, :], (8, 128)) for i in range(HALF)]

    def renew(t, _):
        r = r0[t]
        for i in range(HALF):
            r = r - weights[i] * w1[i, t]
        r_ref[t] = r
        return 0

    lax.fori_loop(0, STEPS, renew, 0, unroll=4)
    finish_with = functools.partial(store_field, v_ref)
    for i in range(HALF):
        load = (lambda t: r_ref[t]) if i == 0 else (lambda t, i=i: w_ref[i - 1, t])
        if i == 0:
            value = lambda t0, g: g
        elif i == 1:
            value = lambda t0, g: v_ref[0, pl.ds(t0, 8)] - step * g
        else:
            value = lambda t0, g, i=i: 2.0 * (v_ref[i - 1, pl.ds(t0, 8)] - step * g) - v_ref[i - 2, pl.ds(t0, 8)]
        line_solve(load, lines, below_mat, above_mat, y_buf, g_buf, finish_with(i, vp, ve, vw)(value))
        operate(v_ref, i, w_ref, coef, fold, vp, ve, vw)
    vectors = [at(ref, i) for ref in (v1, v_ref, w1, w_ref) for i in range(HALF)] + [at(r_ref)]
    pack_own(vectors, packed)
    lefts = [at(packed, i) for i in range(TOTAL)]
    rights = [at(packed, TOTAL + j) for j in range(TOTAL + 1)]
    gram_row(lefts, rights, gram_pairs(TOTAL), True, slice(0, 128), highs, lows, gram)


def last_body(sums, y1, r_ref, v1, w1, v2, w2, out, x_rows, r_rows):
    y, _ = small_solve(*sum_rows(sums[...]), TOTAL)
    w_weights = [jnp.broadcast_to(y[i : i + 1, :], (8, 128)) for i in range(TOTAL)]
    v_weights = [w + (y1[i : i + 1, :] if i < HALF else 0.0) for i, w in enumerate(w_weights)]
    for t in range(STEPS):
        x = jnp.zeros((8, 128), F32)
        r = r_ref[t]
        for i in range(HALF):
            x = x + v_weights[i] * v1[i, t]
            r = r - w_weights[i] * w1[i, t]
        for i in range(HALF):
            x = x + v_weights[HALF + i] * v2[i, t]
            r = r - w_weights[HALF + i] * w2[i, t]
        x_rows[pl.ds(t, 8, stride=STEPS), :] = x
        r_rows[pl.ds(t, 8, stride=STEPS), :] = r
    for place, rows in enumerate((x_rows, r_rows)):
        for part in range(4):
            out[part, place] = rows[128 * part : 128 * part + 128, :].T[GHOST : GHOST + OWN, :]


def unpack_body(recv, x, r):
    for place, ref in enumerate((x, r)):
        ref[...] = jnp.concatenate([recv[part, place] for part in range(4)], axis=0).T


def shape(*dims):
    return jax.ShapeDtypeStruct(dims, F32)


def vmem(*dims):
    return pltpu.VMEM(dims, F32)


FIELD = (STEPS, 8, 128)
SCRATCH = [vmem(*FIELD), vmem(*FIELD), vmem(STEPS + 2, 8, 128), vmem(STEPS + 2, 8, 128), vmem(STEPS + 2, 8, 128), vmem(1024, 128), vmem(1024, 128)]


def all_sums(gram):
    return lax.all_to_all(gram, ("lat", *LON), split_axis=0, concat_axis=0, tiled=True)


def ring(block, step):
    return lax.ppermute(block, LON, [(d, (d + step) % 64) for d in range(64)])


def reflect(block, half):
    def branch(q):
        return lambda b: lax.ppermute(b, LON, [(d, (2 * q - d) % 64) for d in range(64)])

    return lax.switch(half, [branch(q) for q in range(32)], block)


def strips(block, odd):
    def even_branch(b):
        return ring(b[:, COLS - SIDE :], -1), b, ring(b[:, :SIDE], 1)

    def odd_branch(b):
        return b[:, COLS - SIDE :], ring(b, 1), ring(b[:, :SIDE], 2)

    return lax.cond(odd == 0, even_branch, odd_branch, block)


def swap_lat(pieces):
    return lax.all_to_all(pieces, "lat", split_axis=0, concat_axis=0, tiled=True)


def shards(right_side, surface_term, east, north, neast, nwest, land_sea, fold_map):
    offset = (fold_map[0] + COLS * lax.axis_index(LON)) % NLON
    centre = ((offset - COLS // 2) % NLON) // COLS
    shift = (offset - COLS // 2) % COLS + COLS // 2
    smem = pl.BlockSpec(memory_space=pltpu.SMEM)
    whole = pl.BlockSpec(memory_space=pltpu.VMEM)
    packed = pl.pallas_call(pack_body, out_shape=shape(7, COLS, 128), name="pack")(
        right_side, surface_term, east, north, neast, nwest, land_sea
    )
    before = ring(packed[:, COLS - GHOST :], 1)
    after = ring(packed[:, :GHOST], -1)
    block = reflect(packed, centre // 2)
    own = pl.pallas_call(window_body, out_shape=shape(4, 7, WIDE, 128), name="window", compiler_params=params())(
        before, packed, after
    )
    own = swap_lat(own)
    low, main, high = strips(block, centre % 2)
    windows = pl.pallas_call(
        select_body,
        in_specs=[smem] + [whole] * 3,
        out_shape=shape(4, 7, WIDE, 128),
        name="select",
        compiler_params=params(),
    )(shift.reshape(1), low, main, high)
    facing = swap_lat(windows)
    coef, lines, below_mat, above_mat, fold, r0, v1, w1, gram = pl.pallas_call(
        first_body,
        out_shape=(
            shape(9, *FIELD),
            shape(6, STEPS + 8, 8, 128),
            shape(16, 8, 128),
            shape(16, 8, 128),
            shape(8, 128),
            shape(*FIELD),
            shape(HALF, *FIELD),
            shape(HALF, *FIELD),
            shape(512, 128),
        ),
        scratch_shapes=[vmem(7, 512, 128), vmem(7, STEPS + 2, 8, 128), *SCRATCH],
        name="phase_one",
        compiler_params=params(),
    )(own, facing)
    sums = all_sums(gram)
    r4, y1, v2, w2, gram = pl.pallas_call(
        second_body,
        out_shape=(
            shape(*FIELD),
            shape(8, 128),
            shape(HALF, *FIELD),
            shape(HALF, *FIELD),
            shape(512, 128),
        ),
        scratch_shapes=[vmem(2 * TOTAL + 1, STEPS // 4, 8, 128), *SCRATCH],
        name="phase_two",
        compiler_params=params(),
    )(sums, coef, lines, below_mat, above_mat, fold, r0, v1, w1)
    sums = all_sums(gram)
    pieces = pl.pallas_call(
        last_body,
        out_shape=shape(4, 2, OWN, 128),
        scratch_shapes=[vmem(512, 128), vmem(512, 128)],
        name="combine",
        compiler_params=params(),
    )(sums, y1, r4, v1, w1, v2, w2)
    columns = swap_lat(pieces)
    return pl.pallas_call(unpack_body, out_shape=(shape(128, COLS), shape(128, COLS)), name="unpack")(columns)


def solution(mesh):
    finer = Mesh(mesh.devices.reshape(mesh.shape["lat"], 4, 8, 2), ("lat", *LON))
    field = P("lat", LON)
    return jax.shard_map(
        shards,
        mesh=finer,
        in_specs=(field,) * 7 + (P(LON),),
        out_specs=(field, field),
        check_vma=False,
    )
```

```python
import functools

import jax
import jax.numpy as jnp
from jax import lax
from jax.experimental import pallas as pl
from jax.experimental.pallas import tpu as pltpu
from jax.sharding import Mesh
from jax.sharding import PartitionSpec as P


LON = ("x", "z", "core")
NLON = 8192
COLS = 128
OWN = 32
GHOST = 8
WIDE = OWN + 2 * GHOST
PAD = COLS + 2 * GHOST
STEPS = 64
HALF = 4
TOTAL = 2 * HALF
SCALE = 1.0e-4
F32 = jnp.float32
E, W, N, S, NE, SW, NW, SE, DIAG = range(9)
MULT, IPIV, LOWER, UPPER, RISE, FALL = range(6)
SPAN = 8


SIDE = 72


def params(mib=24):
    return pltpu.CompilerParams(vmem_limit_bytes=mib * 1024 * 1024)


def two_sum(a, b):
    s = a + b
    bb = s - a
    return s, (a - (s - bb)) + (b - bb)


def split(a):
    t = a * 4097.0
    hi = t - (t - a)
    return hi, a - hi


def two_prod(a, b):
    p = a * b
    ah, al = split(a)
    bh, bl = split(b)
    return p, ((ah * bh - p) + ah * bl + al * bh) + al * bl


def renorm(s, e):
    hi = s + e
    return hi, e - (hi - s)


def pair_sub(a, b):
    s, e = two_sum(a[0], -b[0])
    return renorm(s, e + (a[1] - b[1]))


def pair_mul(a, b):
    p, e = two_prod(a[0], b[0])
    return renorm(p, e + (a[0] * b[1] + a[1] * b[0]))


def pair_div(a, b):
    first = a[0] / b[0]
    zero = jnp.zeros_like(first)
    rest = pair_sub(a, pair_mul((first, zero), b))
    return renorm(first, rest[0] / b[0])


def sum_rows(values):
    s = values[0:8]
    e = jnp.zeros_like(s)
    for start in range(8, values.shape[0], 8):
        s, err = two_sum(s, values[start : start + 8])
        e = e + err
    for shift in (4, 2, 1):
        s_other = pltpu.roll(s, shift, 0)
        e_other = pltpu.roll(e, shift, 0)
        s, err = two_sum(s, s_other)
        e = e + e_other + err
    hi, lo = renorm(s, e)
    return hi[0:1], lo[0:1]


def small_solve(hi_row, lo_row, order):
    row = lax.broadcasted_iota(jnp.int32, (8, 128), 0)
    lane = lax.broadcasted_iota(jnp.int32, (8, 128), 1)

    def matrix(values):
        wide = jnp.broadcast_to(values, (8, 128))
        out = jnp.zeros((8, 128), F32)
        for i in range(order):
            turned = wide if i == 0 else pltpu.roll(wide, 128 - 16 * i, 1)
            out = jnp.where(row == i, turned, out)
        return jnp.where(lane < 16, out, 0.0)

    hi, lo = matrix(hi_row), matrix(lo_row)
    ratio = hi[3:4, 3:4] / hi[3:4, 2:3]
    start = jnp.sum(jnp.where(row == lane, hi, 0.0), axis=1, keepdims=True)
    live = jnp.ones((8, 128), F32)
    for k in range(order):
        col = tuple(jnp.broadcast_to(v[:, k : k + 1], (8, 128)) for v in (hi, lo))
        piv_row = tuple(jnp.broadcast_to(v[k : k + 1, :], (8, 128)) for v in (hi, lo))
        piv = tuple(jnp.broadcast_to(v[k : k + 1, k : k + 1], (8, 128)) for v in (hi, lo))
        good = piv[0] > 1e-11 * jnp.broadcast_to(start[k : k + 1, :], (8, 128))
        piv = (jnp.where(good, piv[0], 1.0), jnp.where(good, piv[1], 0.0))
        factor = pair_div(col, piv)
        new = pair_sub((hi, lo), pair_mul(factor, piv_row))
        change = good & (row != k)
        hi = jnp.where(change, new[0], hi)
        lo = jnp.where(change, new[1], lo)
        live = jnp.where((row == k) & ~good, 0.0, live)
    diag = jnp.sum(jnp.where(row == lane, hi, 0.0), axis=1, keepdims=True)
    diag = jnp.where((diag != 0.0) & (live[:, 0:1] > 0.0), diag, 1.0)
    y = jnp.broadcast_to(hi[:, 8:9] / diag, (8, 128)) * live
    y = jnp.where(row < order, y, 0.0)
    return y, jnp.broadcast_to(ratio, (8, 128))


def pack_body(rhs, surface, east, north, neast, nwest, land, out):
    for k, ref in enumerate((rhs, surface, east, north, neast, nwest)):
        out[k] = ref[...].T
    out[6] = land[...].astype(F32).T


def window_body(before, packed, after, out):
    for place in range(7):
        wide = jnp.concatenate([before[place], packed[place], after[place]], axis=0)
        for part in range(4):
            out[part, place] = wide[OWN * part : OWN * part + WIDE, :]


def select_body(shift, low, main, high, out):
    i = lax.broadcasted_iota(jnp.int32, (PAD, COLS + 2 * SIDE), 0)
    u = lax.broadcasted_iota(jnp.int32, (PAD, COLS + 2 * SIDE), 1)
    reach = shift[0] + GHOST + SIDE
    plain = jnp.where(u == reach - i, 1.0, 0.0).astype(jnp.bfloat16)
    moved = jnp.where(u == reach - 1 - i, 1.0, 0.0).astype(jnp.bfloat16)

    def pick(choice, values):
        return jnp.dot(choice, values, preferred_element_type=F32)

    for place, source in enumerate((0, 1, 2, 3, 5, 4, 6)):
        both = jnp.concatenate([low[source], main[source], high[source]], axis=0)
        top = both.astype(jnp.bfloat16)
        rest = both - top.astype(F32)
        middle = rest.astype(jnp.bfloat16)
        bottom = (rest - middle.astype(F32)).astype(jnp.bfloat16)
        choice = moved if source == 2 else plain
        facing = (pick(choice, top) + pick(choice, middle)) + pick(choice, bottom)
        for part in range(4):
            out[part, place] = facing[OWN * part : OWN * part + WIDE, :]


def east_of(v):
    return pltpu.roll(v, 127, v.ndim - 1)


def west_of(v):
    return pltpu.roll(v, 1, v.ndim - 1)


def facing_of(v):
    return pltpu.roll(v, 64, v.ndim - 1)


def row_before(v):
    s = lax.broadcasted_iota(jnp.int32, (8, 128), 0)
    return jnp.where(s == 0, 0.0, pltpu.roll(v, 1, 0))


def row_after(v):
    s = lax.broadcasted_iota(jnp.int32, (8, 128), 0)
    return jnp.where(s == 7, 0.0, pltpu.roll(v, 7, 0))


def line_solve(load, lines, below_mat, above_mat, y_buf, g_buf, finish):
    zero = jnp.zeros((8, 128), F32)

    carried = zero
    for start in range(0, STEPS, SPAN):
        local = zero
        before = carried
        for t in range(start, start + SPAN):
            local = load(t) + lines[MULT, t] * local if t > start else load(t)
            y = local + lines[RISE, t] * before
            y_buf[t] = y
        carried = y
    carried = zero
    for start in range(STEPS - 1, -1, -SPAN):
        local = zero
        after = carried
        for t in range(start, start - SPAN, -1):
            scaled = y_buf[t] * lines[IPIV, t]
            local = scaled + lines[MULT, t + 1] * local if t < start else scaled
            x = local + lines[FALL, t] * after
            g_buf[t] = x
        carried = x
    first, last = g_buf[0], g_buf[STEPS - 1]
    below, above = zero, zero
    for k in range(8):
        for base, ends in ((0, first), (8, last)):
            end = jnp.broadcast_to(ends[k : k + 1, :], (8, 128))
            below = below + below_mat[base + k] * end
            above = above + above_mat[base + k] * end

    def combine(c, _):
        t0 = c * 8
        g = g_buf[pl.ds(t0, 8)] + lines[LOWER, pl.ds(t0, 8)] * below + lines[UPPER, pl.ds(t0, 8)] * above
        finish(t0, g)
        return 0

    lax.fori_loop(0, STEPS // 8, combine, 0, unroll=2)


def operate(v_ref, place, w_ref, coef, fold, vp, ve, vw):
    for t, v in ((0, row_before(v_ref[place, STEPS - 1])), (STEPS + 1, row_after(v_ref[place, 0]))):
        vp[t] = v
        ve[t] = east_of(v)
        vw[t] = west_of(v)

    def step(c, _):
        t = c * 4
        here, up, down = pl.ds(t + 1, 4), pl.ds(t + 2, 4), pl.ds(t, 4)
        at = pl.ds(t, 4)
        out = coef[DIAG, at] * vp[here]
        side = coef[E, at] * ve[here] + coef[W, at] * vw[here]
        north = coef[N, at] * vp[up] + coef[NE, at] * ve[up] + coef[NW, at] * vw[up]
        south = coef[S, at] * vp[down] + coef[SW, at] * vw[down] + coef[SE, at] * ve[down]
        w_ref[place, at] = out - (side + north + south)
        return 0

    lax.fori_loop(0, STEPS // 4, step, 0, unroll=2)
    w_ref[place, STEPS - 1] = w_ref[place, STEPS - 1] - fold[...] * facing_of(v_ref[place, STEPS - 1])


def store_field(v_ref, place, vp, ve, vw):
    def finish_with(value_of):
        def finish(t0, g):
            v = value_of(t0, g)
            v_ref[place, pl.ds(t0, 8)] = v
            vp[pl.ds(t0 + 1, 8)] = v
            ve[pl.ds(t0 + 1, 8)] = east_of(v)
            vw[pl.ds(t0 + 1, 8)] = west_of(v)

        return finish

    return finish_with


def pack_own(sources, packed):
    lane = lax.broadcasted_iota(jnp.int32, (8, 128), 1)

    def step(c, _):
        for k, source in enumerate(sources):
            out = pltpu.roll(source(4 * c), 128 - GHOST, 1)
            for part in range(1, 4):
                moved = pltpu.roll(source(4 * c + part), OWN * part - GHOST, 1)
                out = jnp.where(lane >= OWN * part, moved, out)
            packed[k, c] = out
        return 0

    lax.fori_loop(0, STEPS // 4, step, 0)


def gram_row(lefts, rights, pairs, exact, columns, highs, lows, out):
    highs[...] = jnp.zeros(highs.shape, F32)
    lows[...] = jnp.zeros(lows.shape, F32)
    start = 0
    while start < len(pairs):
        end = start
        while end < len(pairs) and (pairs[end][0] == pairs[start][0] or end - start < 12) and end - start < 17:
            end += 1
        part = pairs[start:end]
        start = end

        def add(t, sums, part=part):
            left = {i: lefts[i](t) for i in sorted({i for i, _, _ in part})}
            right = {j: rights[j](t) for j in sorted({j for _, j, _ in part})}
            if not exact:
                return tuple((s + left[i] * right[j], e) for (s, e), (i, j, _) in zip(sums, part))
            left_halves = {i: split(v) for i, v in left.items()}
            right_halves = {j: split(v) for j, v in right.items()}
            out = []
            for (s, e), (i, j, _) in zip(sums, part):
                ah, al = left_halves[i]
                bh, bl = right_halves[j]
                s, err = two_sum(s, ah * bh)
                out.append((s, e + (err + (ah * bl + al * right[j]))))
            return tuple(out)

        zero = jnp.zeros((8, 128), F32)
        sums = lax.fori_loop(0, STEPS // 4 if exact else STEPS, add, tuple((zero, zero) for _ in part), unroll=1 if exact else 2)
        for (s, e), (_, _, lanes) in zip(sums, part):
            for lane in lanes:
                highs[pl.ds(lane, 8, stride=128), :] = s
                lows[pl.ds(lane, 8, stride=128), :] = e
    s, e = highs[0:128], lows[0:128]
    for k in range(1, 8):
        s, err = two_sum(s, highs[128 * k : 128 * k + 128])
        e = e + (err + lows[128 * k : 128 * k + 128])
    s, e = s.T, e.T
    hi, lo = sum_rows(jnp.concatenate([s[columns], e[columns]], axis=0))
    row = lax.broadcasted_iota(jnp.int32, (8, 128), 0)
    both = jnp.broadcast_to(hi, (8, 128))
    if exact:
        both = jnp.where((row & 1) == 0, both, jnp.broadcast_to(lo, (8, 128)))
    out[...] = jnp.concatenate([both] * (out.shape[0] // 8), axis=0)


def gram_pairs(count):
    out = []
    for i in range(count):
        out += [(i, j, sorted({16 * i + j, 16 * j + i})) for j in range(i, count)]
        out.append((i, count, [16 * i + 8]))
    return out


def at(ref, *index):
    return lambda t: ref[(*index, t)]


def first_body(own, facing, coef, lines, below_mat, above_mat, fold, r0, v_ref, w_ref, gram, raw, grid, y_buf, g_buf, vp, ve, vw, highs, lows):
    s_id = lax.broadcasted_iota(jnp.int32, (8, 128), 0)
    zero = jnp.zeros((8, 128), F32)
    gap = jnp.zeros((64 - WIDE, 128), F32)
    for place in range(7):
        for source in range(4):
            full = jnp.concatenate([own[source, place], gap, facing[source, place], gap], axis=0)
            raw[place, 128 * source : 128 * source + 128, :] = full.T
        for t in range(STEPS):
            grid[place, t + 1] = raw[place, pl.ds(t, 8, stride=STEPS), :]
    top_north = grid[3, STEPS]
    top_ocean = grid[6, STEPS]
    last = s_id == 7
    fold_open = jnp.where(last, 0.5 * (top_north + facing_of(top_north)), 0.0)
    fold[...] = fold_open * top_ocean * facing_of(top_ocean)
    for place in (3, 4, 5):
        grid[place, STEPS] = jnp.where(last, 0.0, grid[place, STEPS])
    for place in (3, 4, 5, 6):
        grid[place, 0] = row_before(grid[place, STEPS])
        grid[place, STEPS + 1] = row_after(grid[place, 1])

    def weigh(t, _):
        o, o_up, o_down = grid[6, t + 1], grid[6, t + 2], grid[6, t]
        east = grid[2, t + 1]
        north, neast, nwest = grid[3, t + 1], grid[4, t + 1], grid[5, t + 1]
        south, s_neast, s_nwest = grid[3, t], grid[4, t], grid[5, t]
        open_sum = zero
        parts = (
            (E, east, east_of(o)),
            (W, west_of(east), west_of(o)),
            (N, north, o_up),
            (S, south, o_down),
            (NE, neast, east_of(o_up)),
            (SW, west_of(s_neast), west_of(o_down)),
            (NW, nwest, west_of(o_up)),
            (SE, east_of(s_nwest), east_of(o_down)),
        )
        for place, edge, other in parts:
            coef[place, t] = edge * o * other
            open_sum = open_sum + edge
        surface = grid[1, t + 1]
        coef[DIAG, t] = o * (surface + open_sum) + (1.0 - o)
        r0[t] = o * grid[0, t + 1]
        vw[t] = o * (surface + coef[N, t] + coef[S, t]) + (1.0 - o)
        return 0

    lax.fori_loop(0, STEPS, weigh, 0, unroll=2)
    o = top_ocean
    coef[DIAG, STEPS - 1] = coef[DIAG, STEPS - 1] + o * fold_open

    def eliminate(t, carry):
        ratio, beyond = carry
        north = coef[N, t]
        pivot = vw[t] - coef[S, t] * ratio
        more, err = two_sum(pivot, -north)
        more = more + err
        y_buf[t] = more - ratio * beyond
        inverse = 1.0 / pivot
        guess = north * inverse
        prod, err = two_prod(guess, pivot)
        return guess + ((north - prod) - err) * inverse, more

    ends = lax.fori_loop(0, STEPS, eliminate, (zero, zero), unroll=2)
    lax.fori_loop(0, STEPS, eliminate, tuple(row_before(v) for v in ends), unroll=2)

    def pivots(t, carry):
        before, beyond, response, source = carry
        rest = y_buf[t]
        mult = jnp.where(t == 0, zero, coef[S, t] * before)
        beyond = rest + jnp.where(t == 0, coef[S, 0], mult * beyond)
        inverse = 1.0 / (coef[N, t] + beyond)
        lines[MULT, t] = mult
        lines[IPIV, t] = inverse
        response = jnp.where(t == 0, coef[S, 0], mult * response)
        source = rest + mult * source
        g_buf[t] = response
        vp[t] = source
        return inverse, beyond, response, source

    lax.fori_loop(0, STEPS, pivots, (zero,) * 4, unroll=4)
    for t in range(STEPS, lines.shape[1]):
        lines[MULT, t] = zero
    for start in range(0, STEPS, SPAN):
        rise = lines[MULT, start]
        fall = lines[MULT, start + SPAN]
        for k in range(SPAN):
            lines[RISE, start + k] = rise
            lines[FALL, start + SPAN - 1 - k] = fall
            rise = rise * lines[MULT, start + k + 1]
            fall = fall * lines[MULT, start + SPAN - 1 - k]

    def respond(k, carry):
        low, up, source = carry
        t = STEPS - 1 - k
        factor = lines[MULT, t + 1]
        inverse = lines[IPIV, t]
        low = g_buf[t] * inverse + factor * low
        up = jnp.where(k == 0, coef[N, STEPS - 1] * inverse, factor * up)
        source = vp[t] * inverse + factor * source
        lines[LOWER, t] = low
        lines[UPPER, t] = up
        ve[t] = source
        return low, up, source

    lax.fori_loop(0, STEPS, respond, (zero,) * 3, unroll=4)
    unit = lax.broadcasted_iota(jnp.int32, (16, 128), 0)
    low_first, low_last = lines[LOWER, 0], lines[LOWER, STEPS - 1]
    up_first, up_last = lines[UPPER, 0], lines[UPPER, STEPS - 1]

    def spread(v, s):
        return jnp.broadcast_to(v[s : s + 1, :], (16, 128))

    source_first, source_last = ve[0], ve[STEPS - 1]
    alphas, betas, dens = [jnp.zeros((16, 128), F32)], [jnp.zeros((16, 128), F32)], []
    short = jnp.ones((16, 128), F32)
    for s in range(8):
        alpha, beta = alphas[-1], betas[-1]
        g_first = jnp.where(unit == s, 1.0, 0.0)
        g_last = jnp.where(unit == 8 + s, 1.0, 0.0)
        lf, ll, uf, ul = (spread(v, s) for v in (low_first, low_last, up_first, up_last))
        sf, sl = spread(source_first, s), spread(source_last, s)
        den = 1.0 / (sf + uf + short * lf)
        dens.append(den)
        alphas.append(g_last + ll * (alpha + beta * den * (g_first + lf * alpha)))
        betas.append(ul + ll * beta * den * uf)
        short = sl + ll * (short + beta * den * (sf + lf * short))
    above = jnp.zeros((16, 128), F32)
    for s in range(7, -1, -1):
        alpha, beta = alphas[s], betas[s]
        above_mat[:, s, :] = above
        lf, uf = spread(low_first, s), spread(up_first, s)
        g_first = jnp.where(unit == s, 1.0, 0.0)
        above = dens[s] * (g_first + lf * alpha + uf * above)
        below_mat[:, s, :] = alpha + beta * above
    finish_with = functools.partial(store_field, v_ref)
    for i in range(HALF):
        load = (lambda t: r0[t]) if i == 0 else (lambda t, i=i: w_ref[i - 1, t])
        value = (lambda t0, g: g) if i == 0 else (lambda t0, g: g * SCALE)
        line_solve(load, lines, below_mat, above_mat, y_buf, g_buf, finish_with(i, vp, ve, vw)(value))
        operate(v_ref, i, w_ref, coef, fold, vp, ve, vw)
    lefts = [at(v_ref, i) for i in range(HALF)]
    rights = [at(w_ref, j) for j in range(HALF)] + [at(r0)]
    gram_row(lefts, rights, gram_pairs(HALF), False, slice(GHOST, GHOST + OWN), highs, lows, gram)


def second_body(sums, coef, lines, below_mat, above_mat, fold, r0, v1, w1, r_ref, y_out, v_ref, w_ref, gram, packed, y_buf, g_buf, vp, ve, vw, highs, lows):
    y, ratio = small_solve(*sum_rows(sums[...]), HALF)
    y_out[...] = y
    bound = ratio * (2.0 / SCALE)
    step = 2.0 / bound
    weights = [jnp.broadcast_to(y[i : i + 1, :], (8, 128)) for i in range(HALF)]

    def renew(t, _):
        r = r0[t]
        for i in range(HALF):
            r = r - weights[i] * w1[i, t]
        r_ref[t] = r
        return 0

    lax.fori_loop(0, STEPS, renew, 0, unroll=4)
    finish_with = functools.partial(store_field, v_ref)
    for i in range(HALF):
        load = (lambda t: r_ref[t]) if i == 0 else (lambda t, i=i: w_ref[i - 1, t])
        if i == 0:
            value = lambda t0, g: g
        elif i == 1:
            value = lambda t0, g: v_ref[0, pl.ds(t0, 8)] - step * g
        else:
            value = lambda t0, g, i=i: 2.0 * (v_ref[i - 1, pl.ds(t0, 8)] - step * g) - v_ref[i - 2, pl.ds(t0, 8)]
        line_solve(load, lines, below_mat, above_mat, y_buf, g_buf, finish_with(i, vp, ve, vw)(value))
        operate(v_ref, i, w_ref, coef, fold, vp, ve, vw)
    vectors = [at(ref, i) for ref in (v1, v_ref, w1, w_ref) for i in range(HALF)] + [at(r_ref)]
    pack_own(vectors, packed)
    lefts = [at(packed, i) for i in range(TOTAL)]
    rights = [at(packed, TOTAL + j) for j in range(TOTAL + 1)]
    gram_row(lefts, rights, gram_pairs(TOTAL), True, slice(0, 128), highs, lows, gram)


def last_body(sums, y1, r_ref, v1, w1, v2, w2, out, x_rows, r_rows):
    y, _ = small_solve(*sum_rows(sums[...]), TOTAL)
    w_weights = [jnp.broadcast_to(y[i : i + 1, :], (8, 128)) for i in range(TOTAL)]
    v_weights = [w + (y1[i : i + 1, :] if i < HALF else 0.0) for i, w in enumerate(w_weights)]
    for t in range(STEPS):
        x = jnp.zeros((8, 128), F32)
        r = r_ref[t]
        for i in range(HALF):
            x = x + v_weights[i] * v1[i, t]
            r = r - w_weights[i] * w1[i, t]
        for i in range(HALF):
            x = x + v_weights[HALF + i] * v2[i, t]
            r = r - w_weights[HALF + i] * w2[i, t]
        x_rows[pl.ds(t, 8, stride=STEPS), :] = x
        r_rows[pl.ds(t, 8, stride=STEPS), :] = r
    for place, rows in enumerate((x_rows, r_rows)):
        for part in range(4):
            out[part, place] = rows[128 * part : 128 * part + 128, :].T[GHOST : GHOST + OWN, :]


def unpack_body(recv, x, r):
    for place, ref in enumerate((x, r)):
        ref[...] = jnp.concatenate([recv[part, place] for part in range(4)], axis=0).T


def shape(*dims):
    return jax.ShapeDtypeStruct(dims, F32)


def vmem(*dims):
    return pltpu.VMEM(dims, F32)


FIELD = (STEPS, 8, 128)
SCRATCH = [vmem(*FIELD), vmem(*FIELD), vmem(STEPS + 2, 8, 128), vmem(STEPS + 2, 8, 128), vmem(STEPS + 2, 8, 128), vmem(1024, 128), vmem(1024, 128)]


def all_sums(gram):
    return lax.all_to_all(gram, ("lat", *LON), split_axis=0, concat_axis=0, tiled=True)


def ring(block, step):
    return lax.ppermute(block, LON, [(d, (d + step) % 64) for d in range(64)])


def reflect(block, half):
    def branch(q):
        return lambda b: lax.ppermute(b, LON, [(d, (2 * q - d) % 64) for d in range(64)])

    return lax.switch(half, [branch(q) for q in range(32)], block)


def strips(block, odd):
    def even_branch(b):
        return ring(b[:, COLS - SIDE :], -1), b, ring(b[:, :SIDE], 1)

    def odd_branch(b):
        return b[:, COLS - SIDE :], ring(b, 1), ring(b[:, :SIDE], 2)

    return lax.cond(odd == 0, even_branch, odd_branch, block)


def swap_lat(pieces):
    return lax.all_to_all(pieces, "lat", split_axis=0, concat_axis=0, tiled=True)


def shards(right_side, surface_term, east, north, neast, nwest, land_sea, fold_map):
    offset = (fold_map[0] + COLS * lax.axis_index(LON)) % NLON
    centre = ((offset - COLS // 2) % NLON) // COLS
    shift = (offset - COLS // 2) % COLS + COLS // 2
    smem = pl.BlockSpec(memory_space=pltpu.SMEM)
    whole = pl.BlockSpec(memory_space=pltpu.VMEM)
    packed = pl.pallas_call(pack_body, out_shape=shape(7, COLS, 128), name="pack")(
        right_side, surface_term, east, north, neast, nwest, land_sea
    )
    before = ring(packed[:, COLS - GHOST :], 1)
    after = ring(packed[:, :GHOST], -1)
    block = reflect(packed, centre // 2)
    own = pl.pallas_call(window_body, out_shape=shape(4, 7, WIDE, 128), name="window", compiler_params=params())(
        before, packed, after
    )
    own = swap_lat(own)
    low, main, high = strips(block, centre % 2)
    windows = pl.pallas_call(
        select_body,
        in_specs=[smem] + [whole] * 3,
        out_shape=shape(4, 7, WIDE, 128),
        name="select",
        compiler_params=params(),
    )(shift.reshape(1), low, main, high)
    facing = swap_lat(windows)
    coef, lines, below_mat, above_mat, fold, r0, v1, w1, gram = pl.pallas_call(
        first_body,
        out_shape=(
            shape(9, *FIELD),
            shape(6, STEPS + 8, 8, 128),
            shape(16, 8, 128),
            shape(16, 8, 128),
            shape(8, 128),
            shape(*FIELD),
            shape(HALF, *FIELD),
            shape(HALF, *FIELD),
            shape(256, 128),
        ),
        scratch_shapes=[vmem(7, 512, 128), vmem(7, STEPS + 2, 8, 128), *SCRATCH],
        name="phase_one",
        compiler_params=params(),
    )(own, facing)
    sums = all_sums(gram)
    r4, y1, v2, w2, gram = pl.pallas_call(
        second_body,
        out_shape=(
            shape(*FIELD),
            shape(8, 128),
            shape(HALF, *FIELD),
            shape(HALF, *FIELD),
            shape(512, 128),
        ),
        scratch_shapes=[vmem(2 * TOTAL + 1, STEPS // 4, 8, 128), *SCRATCH],
        name="phase_two",
        compiler_params=params(),
    )(sums, coef, lines, below_mat, above_mat, fold, r0, v1, w1)
    sums = all_sums(gram)
    pieces = pl.pallas_call(
        last_body,
        out_shape=shape(4, 2, OWN, 128),
        scratch_shapes=[vmem(512, 128), vmem(512, 128)],
        name="combine",
        compiler_params=params(),
    )(sums, y1, r4, v1, w1, v2, w2)
    columns = swap_lat(pieces)
    return pl.pallas_call(unpack_body, out_shape=(shape(128, COLS), shape(128, COLS)), name="unpack")(columns)


def solution(mesh):
    finer = Mesh(mesh.devices.reshape(mesh.shape["lat"], 4, 8, 2), ("lat", *LON))
    field = P("lat", LON)
    return jax.shard_map(
        shards,
        mesh=finer,
        in_specs=(field,) * 7 + (P(LON),),
        out_specs=(field, field),
        check_vma=False,
    )
```

```python
import functools

import jax
import jax.numpy as jnp
from jax import lax
from jax.experimental import pallas as pl
from jax.experimental.pallas import tpu as pltpu
from jax.sharding import Mesh
from jax.sharding import PartitionSpec as P


LON = ("x", "z", "core")
NLON = 8192
COLS = 128
OWN = 32
GHOST = 8
WIDE = OWN + 2 * GHOST
PAD = COLS + 2 * GHOST
STEPS = 64
LINE = STEPS + 8
SLAB = 128 + 8
HALF = 4
TOTAL = 2 * HALF
SCALE = 1.0e-4
F32 = jnp.float32
E, W, N, S, NE, SW, NW, SE, DIAG = range(9)
MULT, IPIV, LOWER, UPPER, RISE, FALL = range(6)
SPAN = 8


SIDE = 72


def params(mib=24):
    return pltpu.CompilerParams(vmem_limit_bytes=mib * 1024 * 1024)


def two_sum(a, b):
    s = a + b
    bb = s - a
    return s, (a - (s - bb)) + (b - bb)


def split(a):
    t = a * 4097.0
    hi = t - (t - a)
    return hi, a - hi


def two_prod(a, b):
    p = a * b
    ah, al = split(a)
    bh, bl = split(b)
    return p, ((ah * bh - p) + ah * bl + al * bh) + al * bl


def renorm(s, e):
    hi = s + e
    return hi, e - (hi - s)


def pair_sub(a, b):
    s, e = two_sum(a[0], -b[0])
    return renorm(s, e + (a[1] - b[1]))


def pair_mul(a, b):
    p, e = two_prod(a[0], b[0])
    return renorm(p, e + (a[0] * b[1] + a[1] * b[0]))


def pair_div(a, b):
    first = a[0] / b[0]
    zero = jnp.zeros_like(first)
    rest = pair_sub(a, pair_mul((first, zero), b))
    return renorm(first, rest[0] / b[0])


def sum_rows(values):
    s = values[0:8]
    e = jnp.zeros_like(s)
    for start in range(8, values.shape[0], 8):
        s, err = two_sum(s, values[start : start + 8])
        e = e + err
    for shift in (4, 2, 1):
        s_other = pltpu.roll(s, shift, 0)
        e_other = pltpu.roll(e, shift, 0)
        s, err = two_sum(s, s_other)
        e = e + e_other + err
    hi, lo = renorm(s, e)
    return hi[0:1], lo[0:1]


def small_solve(hi_row, lo_row, order):
    row = lax.broadcasted_iota(jnp.int32, (8, 128), 0)
    lane = lax.broadcasted_iota(jnp.int32, (8, 128), 1)

    def matrix(values):
        wide = jnp.broadcast_to(values, (8, 128))
        out = jnp.zeros((8, 128), F32)
        for i in range(order):
            turned = wide if i == 0 else pltpu.roll(wide, 128 - 16 * i, 1)
            out = jnp.where(row == i, turned, out)
        return jnp.where(lane < 16, out, 0.0)

    hi, lo = matrix(hi_row), matrix(lo_row)
    ratio = hi[3:4, 3:4] / hi[3:4, 2:3]
    start = jnp.sum(jnp.where(row == lane, hi, 0.0), axis=1, keepdims=True)
    live = jnp.ones((8, 128), F32)
    for k in range(order):
        col = tuple(jnp.broadcast_to(v[:, k : k + 1], (8, 128)) for v in (hi, lo))
        piv_row = tuple(jnp.broadcast_to(v[k : k + 1, :], (8, 128)) for v in (hi, lo))
        piv = tuple(jnp.broadcast_to(v[k : k + 1, k : k + 1], (8, 128)) for v in (hi, lo))
        good = piv[0] > 1e-11 * jnp.broadcast_to(start[k : k + 1, :], (8, 128))
        piv = (jnp.where(good, piv[0], 1.0), jnp.where(good, piv[1], 0.0))
        factor = pair_div(col, piv)
        new = pair_sub((hi, lo), pair_mul(factor, piv_row))
        change = good & (row != k)
        hi = jnp.where(change, new[0], hi)
        lo = jnp.where(change, new[1], lo)
        live = jnp.where((row == k) & ~good, 0.0, live)
    diag = jnp.sum(jnp.where(row == lane, hi, 0.0), axis=1, keepdims=True)
    diag = jnp.where((diag != 0.0) & (live[:, 0:1] > 0.0), diag, 1.0)
    y = jnp.broadcast_to(hi[:, 8:9] / diag, (8, 128)) * live
    y = jnp.where(row < order, y, 0.0)
    return y, jnp.broadcast_to(ratio, (8, 128))


def pack_body(rhs, surface, east, north, neast, nwest, land, out):
    for k, ref in enumerate((rhs, surface, east, north, neast, nwest)):
        out[k] = ref[...].T
    out[6] = land[...].astype(F32).T


def window_body(before, packed, after, out):
    for place in range(7):
        wide = jnp.concatenate([before[place], packed[place], after[place]], axis=0)
        for part in range(4):
            out[part, place] = wide[OWN * part : OWN * part + WIDE, :]


def select_body(shift, low, main, high, out):
    i = lax.broadcasted_iota(jnp.int32, (PAD, COLS + 2 * SIDE), 0)
    u = lax.broadcasted_iota(jnp.int32, (PAD, COLS + 2 * SIDE), 1)
    reach = shift[0] + GHOST + SIDE
    plain = jnp.where(u == reach - i, 1.0, 0.0).astype(jnp.bfloat16)
    moved = jnp.where(u == reach - 1 - i, 1.0, 0.0).astype(jnp.bfloat16)

    def pick(choice, values):
        return jnp.dot(choice, values, preferred_element_type=F32)

    for place, source in enumerate((0, 1, 2, 3, 5, 4, 6)):
        both = jnp.concatenate([low[source], main[source], high[source]], axis=0)
        top = both.astype(jnp.bfloat16)
        rest = both - top.astype(F32)
        middle = rest.astype(jnp.bfloat16)
        bottom = (rest - middle.astype(F32)).astype(jnp.bfloat16)
        choice = moved if source == 2 else plain
        facing = (pick(choice, top) + pick(choice, middle)) + pick(choice, bottom)
        for part in range(4):
            out[part, place] = facing[OWN * part : OWN * part + WIDE, :]


def east_of(v):
    return pltpu.roll(v, 127, v.ndim - 1)


def west_of(v):
    return pltpu.roll(v, 1, v.ndim - 1)


def facing_of(v):
    return pltpu.roll(v, 64, v.ndim - 1)


def row_before(v):
    s = lax.broadcasted_iota(jnp.int32, (8, 128), 0)
    return jnp.where(s == 0, 0.0, pltpu.roll(v, 1, 0))


def row_after(v):
    s = lax.broadcasted_iota(jnp.int32, (8, 128), 0)
    return jnp.where(s == 7, 0.0, pltpu.roll(v, 7, 0))


def line_solve(load, lines, below_mat, above_mat, y_buf, g_buf, finish):
    zero = jnp.zeros((8, 128), F32)

    carried = zero
    for start in range(0, STEPS, SPAN):
        local = zero
        before = carried
        for t in range(start, start + SPAN):
            local = load(t) + lines[MULT, t] * local if t > start else load(t)
            y = local + lines[RISE, t] * before
            y_buf[t] = y
        carried = y
    carried = zero
    for start in range(STEPS - 1, -1, -SPAN):
        local = zero
        after = carried
        for t in range(start, start - SPAN, -1):
            scaled = y_buf[t] * lines[IPIV, t]
            local = scaled + lines[MULT, t + 1] * local if t < start else scaled
            x = local + lines[FALL, t] * after
            g_buf[t] = x
        carried = x
    first, last = g_buf[0], g_buf[STEPS - 1]
    below, above = zero, zero
    for k in range(8):
        for base, ends in ((0, first), (8, last)):
            end = jnp.broadcast_to(ends[k : k + 1, :], (8, 128))
            below = below + below_mat[base + k] * end
            above = above + above_mat[base + k] * end

    def combine(c, _):
        t0 = c * 8
        g = g_buf[pl.ds(t0, 8)] + lines[LOWER, pl.ds(t0, 8)] * below + lines[UPPER, pl.ds(t0, 8)] * above
        finish(t0, g)
        return 0

    lax.fori_loop(0, STEPS // 8, combine, 0, unroll=2)


def operate(v_ref, place, w_ref, coef, fold, vp, ve, vw):
    for t, v in ((0, row_before(v_ref[place, STEPS - 1])), (STEPS + 1, row_after(v_ref[place, 0]))):
        vp[t] = v
        ve[t] = east_of(v)
        vw[t] = west_of(v)

    def step(c, _):
        t = c * 4
        here, up, down = pl.ds(t + 1, 4), pl.ds(t + 2, 4), pl.ds(t, 4)
        at = pl.ds(t, 4)
        out = coef[DIAG, at] * vp[here]
        side = coef[E, at] * ve[here] + coef[W, at] * vw[here]
        north = coef[N, at] * vp[up] + coef[NE, at] * ve[up] + coef[NW, at] * vw[up]
        south = coef[S, at] * vp[down] + coef[SW, at] * vw[down] + coef[SE, at] * ve[down]
        w_ref[place, at] = out - (side + north + south)
        return 0

    lax.fori_loop(0, STEPS // 4, step, 0, unroll=2)
    w_ref[place, STEPS - 1] = w_ref[place, STEPS - 1] - fold[...] * facing_of(v_ref[place, STEPS - 1])


def store_field(v_ref, place, vp, ve, vw):
    def finish_with(value_of):
        def finish(t0, g):
            v = value_of(t0, g)
            v_ref[place, pl.ds(t0, 8)] = v
            vp[pl.ds(t0 + 1, 8)] = v
            ve[pl.ds(t0 + 1, 8)] = east_of(v)
            vw[pl.ds(t0 + 1, 8)] = west_of(v)

        return finish

    return finish_with


def pack_own(sources, packed):
    lane = lax.broadcasted_iota(jnp.int32, (8, 128), 1)

    def step(c, _):
        for k, source in enumerate(sources):
            out = pltpu.roll(source(4 * c), 128 - GHOST, 1)
            for part in range(1, 4):
                moved = pltpu.roll(source(4 * c + part), OWN * part - GHOST, 1)
                out = jnp.where(lane >= OWN * part, moved, out)
            packed[k, c] = out
        return 0

    lax.fori_loop(0, STEPS // 4, step, 0)


def gram_row(lefts, rights, pairs, exact, columns, highs, lows, out):
    highs[...] = jnp.zeros(highs.shape, F32)
    lows[...] = jnp.zeros(lows.shape, F32)
    start = 0
    while start < len(pairs):
        end = start
        while end < len(pairs) and (pairs[end][0] == pairs[start][0] or end - start < 12) and end - start < 17:
            end += 1
        part = pairs[start:end]
        start = end

        def add(t, sums, part=part):
            left = {i: lefts[i](t) for i in sorted({i for i, _, _ in part})}
            right = {j: rights[j](t) for j in sorted({j for _, j, _ in part})}
            if not exact:
                return tuple((s + left[i] * right[j], e) for (s, e), (i, j, _) in zip(sums, part))
            left_halves = {i: split(v) for i, v in left.items()}
            right_halves = {j: split(v) for j, v in right.items()}
            out = []
            for (s, e), (i, j, _) in zip(sums, part):
                ah, al = left_halves[i]
                bh, bl = right_halves[j]
                s, err = two_sum(s, ah * bh)
                out.append((s, e + (err + (ah * bl + al * right[j]))))
            return tuple(out)

        zero = jnp.zeros((8, 128), F32)
        sums = lax.fori_loop(0, STEPS // 4 if exact else STEPS, add, tuple((zero, zero) for _ in part), unroll=1 if exact else 2)
        for (s, e), (_, _, lanes) in zip(sums, part):
            for lane in lanes:
                highs[pl.ds(lane, 8, stride=SLAB), :] = s
                lows[pl.ds(lane, 8, stride=SLAB), :] = e
    s, e = highs[0:128], lows[0:128]
    for k in range(1, 8):
        s, err = two_sum(s, highs[SLAB * k : SLAB * k + 128])
        e = e + (err + lows[SLAB * k : SLAB * k + 128])
    s, e = s.T, e.T
    hi, lo = sum_rows(jnp.concatenate([s[columns], e[columns]], axis=0))
    row = lax.broadcasted_iota(jnp.int32, (8, 128), 0)
    both = jnp.broadcast_to(hi, (8, 128))
    if exact:
        both = jnp.where((row & 1) == 0, both, jnp.broadcast_to(lo, (8, 128)))
    out[...] = jnp.concatenate([both] * (out.shape[0] // 8), axis=0)


def gram_pairs(count):
    out = []
    for i in range(count):
        out += [(i, j, sorted({16 * i + j, 16 * j + i})) for j in range(i, count)]
        out.append((i, count, [16 * i + 8]))
    return out


def at(ref, *index):
    return lambda t: ref[(*index, t)]


def first_body(own, facing, coef, lines, below_mat, above_mat, fold, r0, v_ref, w_ref, gram, raw, grid, y_buf, g_buf, vp, ve, vw, highs, lows):
    s_id = lax.broadcasted_iota(jnp.int32, (8, 128), 0)
    zero = jnp.zeros((8, 128), F32)
    gap = jnp.zeros((64 - WIDE, 128), F32)
    for place in range(7):
        for source in range(4):
            full = jnp.concatenate([own[source, place], gap, facing[source, place], gap], axis=0)
            full = full.T
            for part in range(2):
                row = LINE * (2 * source + part)
                raw[place, row : row + STEPS, :] = full[STEPS * part : STEPS * part + STEPS]
        for t in range(STEPS):
            grid[place, t + 1] = raw[place, pl.ds(t, 8, stride=LINE), :]
    top_north = grid[3, STEPS]
    top_ocean = grid[6, STEPS]
    last = s_id == 7
    fold_open = jnp.where(last, 0.5 * (top_north + facing_of(top_north)), 0.0)
    fold[...] = fold_open * top_ocean * facing_of(top_ocean)
    for place in (3, 4, 5):
        grid[place, STEPS] = jnp.where(last, 0.0, grid[place, STEPS])
    for place in (3, 4, 5, 6):
        grid[place, 0] = row_before(grid[place, STEPS])
        grid[place, STEPS + 1] = row_after(grid[place, 1])

    def weigh(t, _):
        o, o_up, o_down = grid[6, t + 1], grid[6, t + 2], grid[6, t]
        east = grid[2, t + 1]
        north, neast, nwest = grid[3, t + 1], grid[4, t + 1], grid[5, t + 1]
        south, s_neast, s_nwest = grid[3, t], grid[4, t], grid[5, t]
        open_sum = zero
        parts = (
            (E, east, east_of(o)),
            (W, west_of(east), west_of(o)),
            (N, north, o_up),
            (S, south, o_down),
            (NE, neast, east_of(o_up)),
            (SW, west_of(s_neast), west_of(o_down)),
            (NW, nwest, west_of(o_up)),
            (SE, east_of(s_nwest), east_of(o_down)),
        )
        for place, edge, other in parts:
            coef[place, t] = edge * o * other
            open_sum = open_sum + edge
        surface = grid[1, t + 1]
        coef[DIAG, t] = o * (surface + open_sum) + (1.0 - o)
        r0[t] = o * grid[0, t + 1]
        vw[t] = o * (surface + coef[N, t] + coef[S, t]) + (1.0 - o)
        return 0

    lax.fori_loop(0, STEPS, weigh, 0, unroll=2)
    o = top_ocean
    coef[DIAG, STEPS - 1] = coef[DIAG, STEPS - 1] + o * fold_open

    def eliminate(t, carry):
        ratio, beyond = carry
        north = coef[N, t]
        pivot = vw[t] - jnp.maximum(coef[S, t] * ratio, 0.0)
        more, err = two_sum(pivot, -north)
        more = more + err
        y_buf[t] = more - ratio * beyond
        inverse = 1.0 / pivot
        guess = north * inverse
        prod, err = two_prod(guess, pivot)
        return guess + ((north - prod) - err) * inverse, more

    ends = lax.fori_loop(0, STEPS, eliminate, (zero, zero), unroll=2)
    lax.fori_loop(0, STEPS, eliminate, tuple(row_before(v) for v in ends), unroll=2)

    def pivots(t, carry):
        before, beyond, response, source = carry
        rest = y_buf[t]
        mult = jnp.where(t == 0, zero, coef[S, t] * before)
        beyond = rest + jnp.where(t == 0, coef[S, 0], mult * beyond)
        inverse = 1.0 / (coef[N, t] + beyond)
        lines[MULT, t] = mult
        lines[IPIV, t] = inverse
        response = jnp.where(t == 0, coef[S, 0], mult * response)
        source = rest + mult * source
        g_buf[t] = response
        vp[t] = source
        return inverse, beyond, response, source

    lax.fori_loop(0, STEPS, pivots, (zero,) * 4, unroll=4)
    for t in range(STEPS, lines.shape[1]):
        lines[MULT, t] = zero
    for start in range(0, STEPS, SPAN):
        rise = lines[MULT, start]
        fall = lines[MULT, start + SPAN]
        for k in range(SPAN):
            lines[RISE, start + k] = rise
            lines[FALL, start + SPAN - 1 - k] = fall
            rise = rise * lines[MULT, start + k + 1]
            fall = fall * lines[MULT, start + SPAN - 1 - k]

    def respond(k, carry):
        low, up, source = carry
        t = STEPS - 1 - k
        factor = lines[MULT, t + 1]
        inverse = lines[IPIV, t]
        low = g_buf[t] * inverse + factor * low
        up = jnp.where(k == 0, coef[N, STEPS - 1] * inverse, factor * up)
        source = vp[t] * inverse + factor * source
        lines[LOWER, t] = low
        lines[UPPER, t] = up
        ve[t] = source
        return low, up, source

    lax.fori_loop(0, STEPS, respond, (zero,) * 3, unroll=4)
    unit = lax.broadcasted_iota(jnp.int32, (16, 128), 0)
    low_first, low_last = lines[LOWER, 0], lines[LOWER, STEPS - 1]
    up_first, up_last = lines[UPPER, 0], lines[UPPER, STEPS - 1]

    def spread(v, s):
        return jnp.broadcast_to(v[s : s + 1, :], (16, 128))

    source_first, source_last = ve[0], ve[STEPS - 1]
    alphas, betas, dens = [jnp.zeros((16, 128), F32)], [jnp.zeros((16, 128), F32)], []
    short = jnp.ones((16, 128), F32)
    for s in range(8):
        alpha, beta = alphas[-1], betas[-1]
        g_first = jnp.where(unit == s, 1.0, 0.0)
        g_last = jnp.where(unit == 8 + s, 1.0, 0.0)
        lf, ll, uf, ul = (spread(v, s) for v in (low_first, low_last, up_first, up_last))
        sf, sl = spread(source_first, s), spread(source_last, s)
        den = 1.0 / (sf + uf + short * lf)
        dens.append(den)
        alphas.append(g_last + ll * (alpha + beta * den * (g_first + lf * alpha)))
        betas.append(ul + ll * beta * den * uf)
        short = sl + ll * (short + beta * den * (sf + lf * short))
    above = jnp.zeros((16, 128), F32)
    for s in range(7, -1, -1):
        alpha, beta = alphas[s], betas[s]
        above_mat[:, s, :] = above
        lf, uf = spread(low_first, s), spread(up_first, s)
        g_first = jnp.where(unit == s, 1.0, 0.0)
        above = dens[s] * (g_first + lf * alpha + uf * above)
        below_mat[:, s, :] = alpha + beta * above
    finish_with = functools.partial(store_field, v_ref)
    for i in range(HALF):
        load = (lambda t: r0[t]) if i == 0 else (lambda t, i=i: w_ref[i - 1, t])
        value = (lambda t0, g: g) if i == 0 else (lambda t0, g: g * SCALE)
        line_solve(load, lines, below_mat, above_mat, y_buf, g_buf, finish_with(i, vp, ve, vw)(value))
        operate(v_ref, i, w_ref, coef, fold, vp, ve, vw)
    lefts = [at(v_ref, i) for i in range(HALF)]
    rights = [at(w_ref, j) for j in range(HALF)] + [at(r0)]
    gram_row(lefts, rights, gram_pairs(HALF), False, slice(GHOST, GHOST + OWN), highs, lows, gram)


def second_body(sums, coef, lines, below_mat, above_mat, fold, r0, v1, w1, r_ref, y_out, v_ref, w_ref, gram, packed, y_buf, g_buf, vp, ve, vw, highs, lows):
    y, ratio = small_solve(*sum_rows(sums[...]), HALF)
    y_out[...] = y
    bound = ratio * (2.0 / SCALE)
    step = 2.0 / bound
    weights = [jnp.broadcast_to(y[i : i + 1, :], (8, 128)) for i in range(HALF)]

    def renew(t, _):
        r = r0[t]
        for i in range(HALF):
            r = r - weights[i] * w1[i, t]
        r_ref[t] = r
        return 0

    lax.fori_loop(0, STEPS, renew, 0, unroll=4)
    finish_with = functools.partial(store_field, v_ref)
    for i in range(HALF):
        load = (lambda t: r_ref[t]) if i == 0 else (lambda t, i=i: w_ref[i - 1, t])
        if i == 0:
            value = lambda t0, g: g
        elif i == 1:
            value = lambda t0, g: v_ref[0, pl.ds(t0, 8)] - step * g
        else:
            value = lambda t0, g, i=i: 2.0 * (v_ref[i - 1, pl.ds(t0, 8)] - step * g) - v_ref[i - 2, pl.ds(t0, 8)]
        line_solve(load, lines, below_mat, above_mat, y_buf, g_buf, finish_with(i, vp, ve, vw)(value))
        operate(v_ref, i, w_ref, coef, fold, vp, ve, vw)
    vectors = [at(ref, i) for ref in (v1, v_ref, w1, w_ref) for i in range(HALF)] + [at(r_ref)]
    pack_own(vectors, packed)
    lefts = [at(packed, i) for i in range(TOTAL)]
    rights = [at(packed, TOTAL + j) for j in range(TOTAL + 1)]
    gram_row(lefts, rights, gram_pairs(TOTAL), True, slice(0, 128), highs, lows, gram)


def last_body(sums, y1, r_ref, v1, w1, v2, w2, out, x_rows, r_rows):
    y, _ = small_solve(*sum_rows(sums[...]), TOTAL)
    w_weights = [jnp.broadcast_to(y[i : i + 1, :], (8, 128)) for i in range(TOTAL)]
    v_weights = [w + (y1[i : i + 1, :] if i < HALF else 0.0) for i, w in enumerate(w_weights)]
    for t in range(STEPS):
        x = jnp.zeros((8, 128), F32)
        r = r_ref[t]
        for i in range(HALF):
            x = x + v_weights[i] * v1[i, t]
            r = r - w_weights[i] * w1[i, t]
        for i in range(HALF):
            x = x + v_weights[HALF + i] * v2[i, t]
            r = r - w_weights[HALF + i] * w2[i, t]
        x_rows[pl.ds(t, 8, stride=LINE), :] = x
        r_rows[pl.ds(t, 8, stride=LINE), :] = r
    for place, rows in enumerate((x_rows, r_rows)):
        for part in range(4):
            low, high = (rows[LINE * k : LINE * k + STEPS, :] for k in (2 * part, 2 * part + 1))
            out[part, place] = jnp.concatenate([low, high], axis=0).T[GHOST : GHOST + OWN, :]


def unpack_body(recv, x, r):
    for place, ref in enumerate((x, r)):
        ref[...] = jnp.concatenate([recv[part, place] for part in range(4)], axis=0).T


def shape(*dims):
    return jax.ShapeDtypeStruct(dims, F32)


def vmem(*dims):
    return pltpu.VMEM(dims, F32)


FIELD = (STEPS, 8, 128)
SCRATCH = [vmem(*FIELD), vmem(*FIELD), vmem(STEPS + 2, 8, 128), vmem(STEPS + 2, 8, 128), vmem(STEPS + 2, 8, 128), vmem(8 * SLAB, 128), vmem(8 * SLAB, 128)]


def all_sums(gram):
    return lax.all_to_all(gram, ("lat", *LON), split_axis=0, concat_axis=0, tiled=True)


def ring(block, step):
    return lax.ppermute(block, LON, [(d, (d + step) % 64) for d in range(64)])


def reflect(block, half):
    def branch(q):
        return lambda b: lax.ppermute(b, LON, [(d, (2 * q - d) % 64) for d in range(64)])

    return lax.switch(half, [branch(q) for q in range(32)], block)


def strips(block, odd):
    def even_branch(b):
        return ring(b[:, COLS - SIDE :], -1), b, ring(b[:, :SIDE], 1)

    def odd_branch(b):
        return b[:, COLS - SIDE :], ring(b, 1), ring(b[:, :SIDE], 2)

    return lax.cond(odd == 0, even_branch, odd_branch, block)


def swap_lat(pieces):
    return lax.all_to_all(pieces, "lat", split_axis=0, concat_axis=0, tiled=True)


def shards(right_side, surface_term, east, north, neast, nwest, land_sea, fold_map):
    offset = (fold_map[0] + COLS * lax.axis_index(LON)) % NLON
    centre = ((offset - COLS // 2) % NLON) // COLS
    shift = (offset - COLS // 2) % COLS + COLS // 2
    smem = pl.BlockSpec(memory_space=pltpu.SMEM)
    whole = pl.BlockSpec(memory_space=pltpu.VMEM)
    packed = pl.pallas_call(pack_body, out_shape=shape(7, COLS, 128), name="pack")(
        right_side, surface_term, east, north, neast, nwest, land_sea
    )
    before = ring(packed[:, COLS - GHOST :], 1)
    after = ring(packed[:, :GHOST], -1)
    block = reflect(packed, centre // 2)
    own = pl.pallas_call(window_body, out_shape=shape(4, 7, WIDE, 128), name="window", compiler_params=params())(
        before, packed, after
    )
    own = swap_lat(own)
    low, main, high = strips(block, centre % 2)
    windows = pl.pallas_call(
        select_body,
        in_specs=[smem] + [whole] * 3,
        out_shape=shape(4, 7, WIDE, 128),
        name="select",
        compiler_params=params(),
    )(shift.reshape(1), low, main, high)
    facing = swap_lat(windows)
    coef, lines, below_mat, above_mat, fold, r0, v1, w1, gram = pl.pallas_call(
        first_body,
        out_shape=(
            shape(9, *FIELD),
            shape(6, STEPS + 8, 8, 128),
            shape(16, 8, 128),
            shape(16, 8, 128),
            shape(8, 128),
            shape(*FIELD),
            shape(HALF, *FIELD),
            shape(HALF, *FIELD),
            shape(256, 128),
        ),
        scratch_shapes=[vmem(7, 8 * LINE, 128), vmem(7, STEPS + 2, 8, 128), *SCRATCH],
        name="phase_one",
        compiler_params=params(),
    )(own, facing)
    sums = all_sums(gram)
    r4, y1, v2, w2, gram = pl.pallas_call(
        second_body,
        out_shape=(
            shape(*FIELD),
            shape(8, 128),
            shape(HALF, *FIELD),
            shape(HALF, *FIELD),
            shape(512, 128),
        ),
        scratch_shapes=[vmem(2 * TOTAL + 1, STEPS // 4, 8, 128), *SCRATCH],
        name="phase_two",
        compiler_params=params(),
    )(sums, coef, lines, below_mat, above_mat, fold, r0, v1, w1)
    sums = all_sums(gram)
    pieces = pl.pallas_call(
        last_body,
        out_shape=shape(4, 2, OWN, 128),
        scratch_shapes=[vmem(8 * LINE, 128), vmem(8 * LINE, 128)],
        name="combine",
        compiler_params=params(),
    )(sums, y1, r4, v1, w1, v2, w2)
    columns = swap_lat(pieces)
    return pl.pallas_call(unpack_body, out_shape=(shape(128, COLS), shape(128, COLS)), name="unpack")(columns)


def solution(mesh):
    finer = Mesh(mesh.devices.reshape(mesh.shape["lat"], 4, 8, 2), ("lat", *LON))
    field = P("lat", LON)
    return jax.shard_map(
        shards,
        mesh=finer,
        in_specs=(field,) * 7 + (P(LON),),
        out_specs=(field, field),
        check_vma=False,
    )
```

```python
import functools

import jax
import jax.numpy as jnp
from jax import lax
from jax.experimental import pallas as pl
from jax.experimental.pallas import tpu as pltpu
from jax.sharding import Mesh
from jax.sharding import PartitionSpec as P


LON = ("x", "z", "core")
NLON = 8192
COLS = 128
OWN = 32
GHOST = 8
WIDE = OWN + 2 * GHOST
PAD = COLS + 2 * GHOST
STEPS = 64
LINE = STEPS + 8
SLAB = 128 + 8
HALF = 4
TOTAL = 2 * HALF
SCALE = 1.0e-4
F32 = jnp.float32
E, W, N, S, NE, SW, NW, SE, DIAG = range(9)
MULT, IPIV, LOWER, UPPER, RISE, FALL = range(6)
SPAN = 8


SIDE = 72


def params(mib=24):
    return pltpu.CompilerParams(vmem_limit_bytes=mib * 1024 * 1024)


def two_sum(a, b):
    s = a + b
    bb = s - a
    return s, (a - (s - bb)) + (b - bb)


def split(a):
    t = a * 4097.0
    hi = t - (t - a)
    return hi, a - hi


def two_prod(a, b):
    p = a * b
    ah, al = split(a)
    bh, bl = split(b)
    return p, ((ah * bh - p) + ah * bl + al * bh) + al * bl


def renorm(s, e):
    hi = s + e
    return hi, e - (hi - s)


def pair_sub(a, b):
    s, e = two_sum(a[0], -b[0])
    return renorm(s, e + (a[1] - b[1]))


def pair_mul(a, b):
    p, e = two_prod(a[0], b[0])
    return renorm(p, e + (a[0] * b[1] + a[1] * b[0]))


def pair_div(a, b):
    first = a[0] / b[0]
    zero = jnp.zeros_like(first)
    rest = pair_sub(a, pair_mul((first, zero), b))
    return renorm(first, rest[0] / b[0])


def sum_rows(values):
    s = values[0:8]
    e = jnp.zeros_like(s)
    for start in range(8, values.shape[0], 8):
        s, err = two_sum(s, values[start : start + 8])
        e = e + err
    for shift in (4, 2, 1):
        s_other = pltpu.roll(s, shift, 0)
        e_other = pltpu.roll(e, shift, 0)
        s, err = two_sum(s, s_other)
        e = e + e_other + err
    hi, lo = renorm(s, e)
    return hi[0:1], lo[0:1]


def small_solve(hi_row, lo_row, order):
    row = lax.broadcasted_iota(jnp.int32, (8, 128), 0)
    lane = lax.broadcasted_iota(jnp.int32, (8, 128), 1)

    def matrix(values):
        wide = jnp.broadcast_to(values, (8, 128))
        out = jnp.zeros((8, 128), F32)
        for i in range(order):
            turned = wide if i == 0 else pltpu.roll(wide, 128 - 16 * i, 1)
            out = jnp.where(row == i, turned, out)
        return jnp.where(lane < 16, out, 0.0)

    hi, lo = matrix(hi_row), matrix(lo_row)
    ratio = hi[3:4, 3:4] / hi[3:4, 2:3]
    start = jnp.sum(jnp.where(row == lane, hi, 0.0), axis=1, keepdims=True)
    live = jnp.ones((8, 128), F32)
    for k in range(order):
        col = tuple(jnp.broadcast_to(v[:, k : k + 1], (8, 128)) for v in (hi, lo))
        piv_row = tuple(jnp.broadcast_to(v[k : k + 1, :], (8, 128)) for v in (hi, lo))
        piv = tuple(jnp.broadcast_to(v[k : k + 1, k : k + 1], (8, 128)) for v in (hi, lo))
        good = piv[0] > 1e-11 * jnp.broadcast_to(start[k : k + 1, :], (8, 128))
        piv = (jnp.where(good, piv[0], 1.0), jnp.where(good, piv[1], 0.0))
        factor = pair_div(col, piv)
        new = pair_sub((hi, lo), pair_mul(factor, piv_row))
        change = good & (row != k)
        hi = jnp.where(change, new[0], hi)
        lo = jnp.where(change, new[1], lo)
        live = jnp.where((row == k) & ~good, 0.0, live)
    diag = jnp.sum(jnp.where(row == lane, hi, 0.0), axis=1, keepdims=True)
    diag = jnp.where((diag != 0.0) & (live[:, 0:1] > 0.0), diag, 1.0)
    y = jnp.broadcast_to(hi[:, 8:9] / diag, (8, 128)) * live
    y = jnp.where(row < order, y, 0.0)
    return y, jnp.broadcast_to(ratio, (8, 128))


def pack_body(rhs, surface, east, north, neast, nwest, land, out):
    for k, ref in enumerate((rhs, surface, east, north, neast, nwest)):
        out[k] = ref[...].T
    out[6] = land[...].astype(F32).T


def window_body(before, packed, after, out):
    for place in range(7):
        wide = jnp.concatenate([before[place], packed[place], after[place]], axis=0)
        for part in range(4):
            out[part, place] = wide[OWN * part : OWN * part + WIDE, :]


def select_body(shift, low, main, high, out):
    i = lax.broadcasted_iota(jnp.int32, (PAD, COLS + 2 * SIDE), 0)
    u = lax.broadcasted_iota(jnp.int32, (PAD, COLS + 2 * SIDE), 1)
    reach = shift[0] + GHOST + SIDE
    plain = jnp.where(u == reach - i, 1.0, 0.0).astype(jnp.bfloat16)
    moved = jnp.where(u == reach - 1 - i, 1.0, 0.0).astype(jnp.bfloat16)

    def pick(choice, values):
        return jnp.dot(choice, values, preferred_element_type=F32)

    for place, source in enumerate((0, 1, 2, 3, 5, 4, 6)):
        both = jnp.concatenate([low[source], main[source], high[source]], axis=0)
        top = both.astype(jnp.bfloat16)
        rest = both - top.astype(F32)
        middle = rest.astype(jnp.bfloat16)
        bottom = (rest - middle.astype(F32)).astype(jnp.bfloat16)
        choice = moved if source == 2 else plain
        facing = (pick(choice, top) + pick(choice, middle)) + pick(choice, bottom)
        for part in range(4):
            out[part, place] = facing[OWN * part : OWN * part + WIDE, :]


def east_of(v):
    return pltpu.roll(v, 127, v.ndim - 1)


def west_of(v):
    return pltpu.roll(v, 1, v.ndim - 1)


def facing_of(v):
    return pltpu.roll(v, 64, v.ndim - 1)


def row_before(v):
    s = lax.broadcasted_iota(jnp.int32, (8, 128), 0)
    return jnp.where(s == 0, 0.0, pltpu.roll(v, 1, 0))


def row_after(v):
    s = lax.broadcasted_iota(jnp.int32, (8, 128), 0)
    return jnp.where(s == 7, 0.0, pltpu.roll(v, 7, 0))


def line_solve(load, lines, below_mat, above_mat, y_buf, g_buf, finish):
    zero = jnp.zeros((8, 128), F32)

    carried = zero
    for start in range(0, STEPS, SPAN):
        local = zero
        before = carried
        for t in range(start, start + SPAN):
            local = load(t) + lines[MULT, t] * local if t > start else load(t)
            y = local + lines[RISE, t] * before
            y_buf[t] = y
        carried = y
    carried = zero
    for start in range(STEPS - 1, -1, -SPAN):
        local = zero
        after = carried
        for t in range(start, start - SPAN, -1):
            scaled = y_buf[t] * lines[IPIV, t]
            local = scaled + lines[MULT, t + 1] * local if t < start else scaled
            x = local + lines[FALL, t] * after
            g_buf[t] = x
        carried = x
    first, last = g_buf[0], g_buf[STEPS - 1]
    below, above = zero, zero
    for k in range(8):
        for base, ends in ((0, first), (8, last)):
            end = jnp.broadcast_to(ends[k : k + 1, :], (8, 128))
            below = below + below_mat[base + k] * end
            above = above + above_mat[base + k] * end

    def combine(c, _):
        t0 = c * 8
        g = g_buf[pl.ds(t0, 8)] + lines[LOWER, pl.ds(t0, 8)] * below + lines[UPPER, pl.ds(t0, 8)] * above
        finish(t0, g)
        return 0

    lax.fori_loop(0, STEPS // 8, combine, 0, unroll=4)


def operate(v_ref, place, w_ref, coef, fold, vp, ve, vw):
    for t, v in ((0, row_before(v_ref[place, STEPS - 1])), (STEPS + 1, row_after(v_ref[place, 0]))):
        vp[t] = v
        ve[t] = east_of(v)
        vw[t] = west_of(v)

    def step(c, _):
        t = c * 4
        here, up, down = pl.ds(t + 1, 4), pl.ds(t + 2, 4), pl.ds(t, 4)
        at = pl.ds(t, 4)
        out = coef[DIAG, at] * vp[here]
        side = coef[E, at] * ve[here] + coef[W, at] * vw[here]
        north = coef[N, at] * vp[up] + coef[NE, at] * ve[up] + coef[NW, at] * vw[up]
        south = coef[S, at] * vp[down] + coef[SW, at] * vw[down] + coef[SE, at] * ve[down]
        w_ref[place, at] = out - (side + north + south)
        return 0

    lax.fori_loop(0, STEPS // 4, step, 0, unroll=4)
    w_ref[place, STEPS - 1] = w_ref[place, STEPS - 1] - fold[...] * facing_of(v_ref[place, STEPS - 1])


def store_field(v_ref, place, vp, ve, vw):
    def finish_with(value_of):
        def finish(t0, g):
            v = value_of(t0, g)
            v_ref[place, pl.ds(t0, 8)] = v
            vp[pl.ds(t0 + 1, 8)] = v
            ve[pl.ds(t0 + 1, 8)] = east_of(v)
            vw[pl.ds(t0 + 1, 8)] = west_of(v)

        return finish

    return finish_with


def pack_own(sources, packed):
    lane = lax.broadcasted_iota(jnp.int32, (8, 128), 1)

    def step(c, _):
        for k, source in enumerate(sources):
            out = pltpu.roll(source(4 * c), 128 - GHOST, 1)
            for part in range(1, 4):
                moved = pltpu.roll(source(4 * c + part), OWN * part - GHOST, 1)
                out = jnp.where(lane >= OWN * part, moved, out)
            packed[k, c] = out
        return 0

    lax.fori_loop(0, STEPS // 4, step, 0, unroll=2)


def gram_row(lefts, rights, pairs, exact, columns, highs, lows, out):
    highs[...] = jnp.zeros(highs.shape, F32)
    lows[...] = jnp.zeros(lows.shape, F32)
    start = 0
    while start < len(pairs):
        end = start
        while end < len(pairs) and (pairs[end][0] == pairs[start][0] or end - start < 12) and end - start < 17:
            end += 1
        part = pairs[start:end]
        start = end

        def add(t, sums, part=part):
            left = {i: lefts[i](t) for i in sorted({i for i, _, _ in part})}
            right = {j: rights[j](t) for j in sorted({j for _, j, _ in part})}
            if not exact:
                return tuple((s + left[i] * right[j], e) for (s, e), (i, j, _) in zip(sums, part))
            left_halves = {i: split(v) for i, v in left.items()}
            right_halves = {j: split(v) for j, v in right.items()}
            out = []
            for (s, e), (i, j, _) in zip(sums, part):
                ah, al = left_halves[i]
                bh, bl = right_halves[j]
                s, err = two_sum(s, ah * bh)
                out.append((s, e + (err + (ah * bl + al * right[j]))))
            return tuple(out)

        zero = jnp.zeros((8, 128), F32)
        sums = lax.fori_loop(0, STEPS // 4 if exact else STEPS, add, tuple((zero, zero) for _ in part), unroll=1 if exact else 2)
        for (s, e), (_, _, lanes) in zip(sums, part):
            for lane in lanes:
                highs[pl.ds(lane, 8, stride=SLAB), :] = s
                lows[pl.ds(lane, 8, stride=SLAB), :] = e
    s, e = highs[0:128], lows[0:128]
    for k in range(1, 8):
        s, err = two_sum(s, highs[SLAB * k : SLAB * k + 128])
        e = e + (err + lows[SLAB * k : SLAB * k + 128])
    s, e = s.T, e.T
    hi, lo = sum_rows(jnp.concatenate([s[columns], e[columns]], axis=0))
    row = lax.broadcasted_iota(jnp.int32, (8, 128), 0)
    both = jnp.broadcast_to(hi, (8, 128))
    if exact:
        both = jnp.where((row & 1) == 0, both, jnp.broadcast_to(lo, (8, 128)))
    out[...] = jnp.concatenate([both] * (out.shape[0] // 8), axis=0)


def gram_pairs(count):
    out = []
    for i in range(count):
        out += [(i, j, sorted({16 * i + j, 16 * j + i})) for j in range(i, count)]
        out.append((i, count, [16 * i + 8]))
    return out


def at(ref, *index):
    return lambda t: ref[(*index, t)]


def first_body(own, facing, coef, lines, below_mat, above_mat, fold, r0, v_ref, w_ref, gram, raw, grid, y_buf, g_buf, vp, ve, vw, highs, lows):
    s_id = lax.broadcasted_iota(jnp.int32, (8, 128), 0)
    zero = jnp.zeros((8, 128), F32)
    gap = jnp.zeros((64 - WIDE, 128), F32)
    for place in range(7):
        for source in range(4):
            full = jnp.concatenate([own[source, place], gap, facing[source, place], gap], axis=0)
            full = full.T
            for part in range(2):
                row = LINE * (2 * source + part)
                raw[place, row : row + STEPS, :] = full[STEPS * part : STEPS * part + STEPS]
        for t in range(STEPS):
            grid[place, t + 1] = raw[place, pl.ds(t, 8, stride=LINE), :]
    top_north = grid[3, STEPS]
    top_ocean = grid[6, STEPS]
    last = s_id == 7
    fold_open = jnp.where(last, 0.5 * (top_north + facing_of(top_north)), 0.0)
    fold[...] = fold_open * top_ocean * facing_of(top_ocean)
    for place in (3, 4, 5):
        grid[place, STEPS] = jnp.where(last, 0.0, grid[place, STEPS])
    for place in (3, 4, 5, 6):
        grid[place, 0] = row_before(grid[place, STEPS])
        grid[place, STEPS + 1] = row_after(grid[place, 1])

    def weigh(t, _):
        o, o_up, o_down = grid[6, t + 1], grid[6, t + 2], grid[6, t]
        east = grid[2, t + 1]
        north, neast, nwest = grid[3, t + 1], grid[4, t + 1], grid[5, t + 1]
        south, s_neast, s_nwest = grid[3, t], grid[4, t], grid[5, t]
        open_sum = zero
        parts = (
            (E, east, east_of(o)),
            (W, west_of(east), west_of(o)),
            (N, north, o_up),
            (S, south, o_down),
            (NE, neast, east_of(o_up)),
            (SW, west_of(s_neast), west_of(o_down)),
            (NW, nwest, west_of(o_up)),
            (SE, east_of(s_nwest), east_of(o_down)),
        )
        for place, edge, other in parts:
            coef[place, t] = edge * o * other
            open_sum = open_sum + edge
        surface = grid[1, t + 1]
        coef[DIAG, t] = o * (surface + open_sum) + (1.0 - o)
        r0[t] = o * grid[0, t + 1]
        vw[t] = o * (surface + coef[N, t] + coef[S, t]) + (1.0 - o)
        return 0

    lax.fori_loop(0, STEPS, weigh, 0, unroll=4)
    o = top_ocean
    coef[DIAG, STEPS - 1] = coef[DIAG, STEPS - 1] + o * fold_open

    def eliminate(t, carry):
        ratio, beyond = carry
        north = coef[N, t]
        pivot = vw[t] - jnp.maximum(coef[S, t] * ratio, 0.0)
        more, err = two_sum(pivot, -north)
        more = more + err
        y_buf[t] = more - ratio * beyond
        inverse = 1.0 / pivot
        guess = north * inverse
        prod, err = two_prod(guess, pivot)
        return guess + ((north - prod) - err) * inverse, more

    ends = lax.fori_loop(0, STEPS, eliminate, (zero, zero), unroll=2)
    lax.fori_loop(0, STEPS, eliminate, tuple(row_before(v) for v in ends), unroll=2)

    def pivots(t, carry):
        before, beyond, response, source = carry
        rest = y_buf[t]
        mult = jnp.where(t == 0, zero, coef[S, t] * before)
        beyond = rest + jnp.where(t == 0, coef[S, 0], mult * beyond)
        inverse = 1.0 / (coef[N, t] + beyond)
        lines[MULT, t] = mult
        lines[IPIV, t] = inverse
        response = jnp.where(t == 0, coef[S, 0], mult * response)
        source = rest + mult * source
        g_buf[t] = response
        vp[t] = source
        return inverse, beyond, response, source

    lax.fori_loop(0, STEPS, pivots, (zero,) * 4, unroll=4)
    for t in range(STEPS, lines.shape[1]):
        lines[MULT, t] = zero
    for start in range(0, STEPS, SPAN):
        rise = lines[MULT, start]
        fall = lines[MULT, start + SPAN]
        for k in range(SPAN):
            lines[RISE, start + k] = rise
            lines[FALL, start + SPAN - 1 - k] = fall
            rise = rise * lines[MULT, start + k + 1]
            fall = fall * lines[MULT, start + SPAN - 1 - k]

    def respond(k, carry):
        low, up, source = carry
        t = STEPS - 1 - k
        factor = lines[MULT, t + 1]
        inverse = lines[IPIV, t]
        low = g_buf[t] * inverse + factor * low
        up = jnp.where(k == 0, coef[N, STEPS - 1] * inverse, factor * up)
        source = vp[t] * inverse + factor * source
        lines[LOWER, t] = low
        lines[UPPER, t] = up
        ve[t] = source
        return low, up, source

    lax.fori_loop(0, STEPS, respond, (zero,) * 3, unroll=4)
    unit = lax.broadcasted_iota(jnp.int32, (16, 128), 0)
    low_first, low_last = lines[LOWER, 0], lines[LOWER, STEPS - 1]
    up_first, up_last = lines[UPPER, 0], lines[UPPER, STEPS - 1]

    def spread(v, s):
        return jnp.broadcast_to(v[s : s + 1, :], (16, 128))

    source_first, source_last = ve[0], ve[STEPS - 1]
    alphas, betas, dens = [jnp.zeros((16, 128), F32)], [jnp.zeros((16, 128), F32)], []
    short = jnp.ones((16, 128), F32)
    for s in range(8):
        alpha, beta = alphas[-1], betas[-1]
        g_first = jnp.where(unit == s, 1.0, 0.0)
        g_last = jnp.where(unit == 8 + s, 1.0, 0.0)
        lf, ll, uf, ul = (spread(v, s) for v in (low_first, low_last, up_first, up_last))
        sf, sl = spread(source_first, s), spread(source_last, s)
        den = 1.0 / (sf + uf + short * lf)
        dens.append(den)
        alphas.append(g_last + ll * (alpha + beta * den * (g_first + lf * alpha)))
        betas.append(ul + ll * beta * den * uf)
        short = sl + ll * (short + beta * den * (sf + lf * short))
    above = jnp.zeros((16, 128), F32)
    for s in range(7, -1, -1):
        alpha, beta = alphas[s], betas[s]
        above_mat[:, s, :] = above
        lf, uf = spread(low_first, s), spread(up_first, s)
        g_first = jnp.where(unit == s, 1.0, 0.0)
        above = dens[s] * (g_first + lf * alpha + uf * above)
        below_mat[:, s, :] = alpha + beta * above
    finish_with = functools.partial(store_field, v_ref)
    for i in range(HALF):
        load = (lambda t: r0[t]) if i == 0 else (lambda t, i=i: w_ref[i - 1, t])
        value = (lambda t0, g: g) if i == 0 else (lambda t0, g: g * SCALE)
        line_solve(load, lines, below_mat, above_mat, y_buf, g_buf, finish_with(i, vp, ve, vw)(value))
        operate(v_ref, i, w_ref, coef, fold, vp, ve, vw)
    lefts = [at(v_ref, i) for i in range(HALF)]
    rights = [at(w_ref, j) for j in range(HALF)] + [at(r0)]
    gram_row(lefts, rights, gram_pairs(HALF), False, slice(GHOST, GHOST + OWN), highs, lows, gram)


def second_body(sums, coef, lines, below_mat, above_mat, fold, r0, v1, w1, r_ref, y_out, v_ref, w_ref, gram, packed, y_buf, g_buf, vp, ve, vw, highs, lows):
    y, ratio = small_solve(*sum_rows(sums[...]), HALF)
    y_out[...] = y
    bound = ratio * (2.0 / SCALE)
    step = 2.0 / bound
    weights = [jnp.broadcast_to(y[i : i + 1, :], (8, 128)) for i in range(HALF)]

    def renew(t, _):
        r = r0[t]
        for i in range(HALF):
            r = r - weights[i] * w1[i, t]
        r_ref[t] = r
        return 0

    lax.fori_loop(0, STEPS, renew, 0, unroll=4)
    finish_with = functools.partial(store_field, v_ref)
    for i in range(HALF):
        load = (lambda t: r_ref[t]) if i == 0 else (lambda t, i=i: w_ref[i - 1, t])
        if i == 0:
            value = lambda t0, g: g
        elif i == 1:
            value = lambda t0, g: v_ref[0, pl.ds(t0, 8)] - step * g
        else:
            value = lambda t0, g, i=i: 2.0 * (v_ref[i - 1, pl.ds(t0, 8)] - step * g) - v_ref[i - 2, pl.ds(t0, 8)]
        line_solve(load, lines, below_mat, above_mat, y_buf, g_buf, finish_with(i, vp, ve, vw)(value))
        operate(v_ref, i, w_ref, coef, fold, vp, ve, vw)
    vectors = [at(ref, i) for ref in (v1, v_ref, w1, w_ref) for i in range(HALF)] + [at(r_ref)]
    pack_own(vectors, packed)
    lefts = [at(packed, i) for i in range(TOTAL)]
    rights = [at(packed, TOTAL + j) for j in range(TOTAL + 1)]
    gram_row(lefts, rights, gram_pairs(TOTAL), True, slice(0, 128), highs, lows, gram)


def last_body(sums, y1, r_ref, v1, w1, v2, w2, out, x_rows, r_rows):
    y, _ = small_solve(*sum_rows(sums[...]), TOTAL)
    w_weights = [jnp.broadcast_to(y[i : i + 1, :], (8, 128)) for i in range(TOTAL)]
    v_weights = [w + (y1[i : i + 1, :] if i < HALF else 0.0) for i, w in enumerate(w_weights)]
    for t in range(STEPS):
        x = jnp.zeros((8, 128), F32)
        r = r_ref[t]
        for i in range(HALF):
            x = x + v_weights[i] * v1[i, t]
            r = r - w_weights[i] * w1[i, t]
        for i in range(HALF):
            x = x + v_weights[HALF + i] * v2[i, t]
            r = r - w_weights[HALF + i] * w2[i, t]
        x_rows[pl.ds(t, 8, stride=LINE), :] = x
        r_rows[pl.ds(t, 8, stride=LINE), :] = r
    for place, rows in enumerate((x_rows, r_rows)):
        for part in range(4):
            low, high = (rows[LINE * k : LINE * k + STEPS, :] for k in (2 * part, 2 * part + 1))
            out[part, place] = jnp.concatenate([low, high], axis=0).T[GHOST : GHOST + OWN, :]


def unpack_body(recv, x, r):
    for place, ref in enumerate((x, r)):
        ref[...] = jnp.concatenate([recv[part, place] for part in range(4)], axis=0).T


def shape(*dims):
    return jax.ShapeDtypeStruct(dims, F32)


def vmem(*dims):
    return pltpu.VMEM(dims, F32)


FIELD = (STEPS, 8, 128)
SCRATCH = [vmem(*FIELD), vmem(*FIELD), vmem(STEPS + 2, 8, 128), vmem(STEPS + 2, 8, 128), vmem(STEPS + 2, 8, 128), vmem(8 * SLAB, 128), vmem(8 * SLAB, 128)]


def all_sums(gram):
    return lax.all_to_all(gram, ("lat", *LON), split_axis=0, concat_axis=0, tiled=True)


def ring(block, step):
    return lax.ppermute(block, LON, [(d, (d + step) % 64) for d in range(64)])


def reflect(block, half):
    def branch(q):
        return lambda b: lax.ppermute(b, LON, [(d, (2 * q - d) % 64) for d in range(64)])

    return lax.switch(half, [branch(q) for q in range(32)], block)


def strips(block, odd):
    def even_branch(b):
        return ring(b[:, COLS - SIDE :], -1), b, ring(b[:, :SIDE], 1)

    def odd_branch(b):
        return b[:, COLS - SIDE :], ring(b, 1), ring(b[:, :SIDE], 2)

    return lax.cond(odd == 0, even_branch, odd_branch, block)


def swap_lat(pieces):
    return lax.all_to_all(pieces, "lat", split_axis=0, concat_axis=0, tiled=True)


def shards(right_side, surface_term, east, north, neast, nwest, land_sea, fold_map):
    offset = (fold_map[0] + COLS * lax.axis_index(LON)) % NLON
    centre = ((offset - COLS // 2) % NLON) // COLS
    shift = (offset - COLS // 2) % COLS + COLS // 2
    smem = pl.BlockSpec(memory_space=pltpu.SMEM)
    whole = pl.BlockSpec(memory_space=pltpu.VMEM)
    packed = pl.pallas_call(pack_body, out_shape=shape(7, COLS, 128), name="pack")(
        right_side, surface_term, east, north, neast, nwest, land_sea
    )
    before = ring(packed[:, COLS - GHOST :], 1)
    after = ring(packed[:, :GHOST], -1)
    block = reflect(packed, centre // 2)
    own = pl.pallas_call(window_body, out_shape=shape(4, 7, WIDE, 128), name="window", compiler_params=params())(
        before, packed, after
    )
    own = swap_lat(own)
    low, main, high = strips(block, centre % 2)
    windows = pl.pallas_call(
        select_body,
        in_specs=[smem] + [whole] * 3,
        out_shape=shape(4, 7, WIDE, 128),
        name="select",
        compiler_params=params(),
    )(shift.reshape(1), low, main, high)
    facing = swap_lat(windows)
    coef, lines, below_mat, above_mat, fold, r0, v1, w1, gram = pl.pallas_call(
        first_body,
        out_shape=(
            shape(9, *FIELD),
            shape(6, STEPS + 8, 8, 128),
            shape(16, 8, 128),
            shape(16, 8, 128),
            shape(8, 128),
            shape(*FIELD),
            shape(HALF, *FIELD),
            shape(HALF, *FIELD),
            shape(256, 128),
        ),
        scratch_shapes=[vmem(7, 8 * LINE, 128), vmem(7, STEPS + 2, 8, 128), *SCRATCH],
        name="phase_one",
        compiler_params=params(),
    )(own, facing)
    sums = all_sums(gram)
    r4, y1, v2, w2, gram = pl.pallas_call(
        second_body,
        out_shape=(
            shape(*FIELD),
            shape(8, 128),
            shape(HALF, *FIELD),
            shape(HALF, *FIELD),
            shape(512, 128),
        ),
        scratch_shapes=[vmem(2 * TOTAL + 1, STEPS // 4, 8, 128), *SCRATCH],
        name="phase_two",
        compiler_params=params(),
    )(sums, coef, lines, below_mat, above_mat, fold, r0, v1, w1)
    sums = all_sums(gram)
    pieces = pl.pallas_call(
        last_body,
        out_shape=shape(4, 2, OWN, 128),
        scratch_shapes=[vmem(8 * LINE, 128), vmem(8 * LINE, 128)],
        name="combine",
        compiler_params=params(),
    )(sums, y1, r4, v1, w1, v2, w2)
    columns = swap_lat(pieces)
    return pl.pallas_call(unpack_body, out_shape=(shape(128, COLS), shape(128, COLS)), name="unpack")(columns)


def solution(mesh):
    finer = Mesh(mesh.devices.reshape(mesh.shape["lat"], 4, 8, 2), ("lat", *LON))
    field = P("lat", LON)
    return jax.shard_map(
        shards,
        mesh=finer,
        in_specs=(field,) * 7 + (P(LON),),
        out_specs=(field, field),
        check_vma=False,
    )
```
